32 devices in a mesh: ctx: 16 (over z, x, core), fsdp: 2 (over y).
Axes of the slice: x: 2, y: 2, z: 4, core: 2. Of those that a mesh axis runs over, the one named last changes fastest.
Arguments:
- tokens: bfloat16 [2, 2048, 1024], P('fsdp', 'ctx'), may hold values from -6 to 6
- cotangent: bfloat16 [2, 2048, 1024], P('fsdp', 'ctx'), may hold values from -6 to 6
- gain_attn: float32 [1024], replicated, may hold values from 0.5 to 1.5
- gain_mlp: float32 [1024], replicated, may hold values from 0.5 to 1.5
- qkv_weight: bfloat16 [3072, 1024], P('fsdp'), may hold values from -2 to 2
- out_weight: bfloat16 [1024, 1024], P('fsdp'), may hold values from -0.625 to 0.625
- in_weight: bfloat16 [5248, 1024], P('fsdp'), may hold values from -0.1875 to 0.1875
- down_weight: bfloat16 [1024, 2624], P('fsdp'), may hold values from -0.125 to 0.125
Outputs:
- output: float32 [2, 2048, 1024], P('fsdp', 'ctx')
- grad_input: float32 [2, 2048, 1024], P('fsdp', 'ctx')
- grad_qkv: float32 [3072, 1024], P(('ctx', 'fsdp'))
- grad_out_proj: float32 [1024, 1024], P(('ctx', 'fsdp'))
- grad_in_proj: float32 [5248, 1024], P(('ctx', 'fsdp'))
- grad_down: float32 [1024, 2624], P(('ctx', 'fsdp'))
- grad_gain_attn: float32 [1024], P(('ctx', 'fsdp'))
- grad_gain_mlp: float32 [1024], P(('ctx', 'fsdp'))
The draws below stay inside these ranges and needn't reach their ends.
All inputs are finite; a program needn't handle non-finite values.
Results may differ from the reference program's by a relative error of at most 0.015.
Values may be sent and summed in bfloat16 or wider, within the bound.
A program may use at most 256 MiB of HBM per device.

```python
import jax
import jax.numpy as jnp
from jax import lax

D = 1024
HEADS = 16
HEAD_DIM = 64
FF = 2624
SEQ = 2048
BATCH = 2


def draw_qkv_weight(key, part):
    base = jnp.clip(jax.random.normal(key, (3 * D, D), jnp.float32), -6.0, 6.0) * D ** (-0.5)
    base = jnp.clip(base, -2.0, 2.0)
    return base.astype(jnp.bfloat16)


def steps_of(own_key, extent, shards, least, largest):
    def one(position, shards_of):
        draws = jax.random.uniform(jax.random.fold_in(jax.random.fold_in(own_key, 6), position), (shards_of,), jnp.float32, least / len(shards), largest / len(shards))
        return jnp.repeat(jnp.exp(draws), extent[position] // shards_of).reshape((-1,) + (1,) * (len(extent) - position - 1))

    factor_of = one(*shards[0])
    for cut in shards[1:]:
        factor_of = factor_of * one(*cut)
    return factor_of


def noise(key, dims, deviation, limit, pieces=(), held_as=jnp.bfloat16):
    factor_of = steps_of(key, dims, pieces, -0.22, 0.18) if pieces else 1.0
    result = jax.random.normal(key, dims, jnp.float32) * deviation * factor_of
    return jnp.minimum(jnp.maximum(result, -limit), limit).astype(held_as)


def setup_inputs(seed: int = 0) -> dict:
    splits = jax.random.split(jax.random.key(seed), 9)
    return {
        "tokens": noise(splits[0], (BATCH, SEQ, D), 1.0, 6.0, ((0, 2), (1, 16))),
        "cotangent": noise(splits[1], (BATCH, SEQ, D), 1.0, 6.0, ((0, 2), (1, 16))),
        "gain_attn": jnp.clip(1.0 + 0.1 * jax.random.normal(splits[2], (D,), jnp.float32), 0.5, 1.5),
        "gain_mlp": jnp.clip(1.0 + 0.1 * jax.random.normal(splits[3], (D,), jnp.float32), 0.5, 1.5),
        "qkv_weight": draw_qkv_weight(jax.random.fold_in(splits[8], 71), 0),
        "out_weight": noise(splits[5], (D, D), ((SEQ // D) ** 0.5 / D ** 0.5), 0.625, ((0, 2),)),
        "in_weight": noise(splits[6], (2 * FF, D), D ** -0.5, 0.1875, ((0, 2),)),
        "down_weight": noise(splits[7], (D, FF), FF ** -0.5, 0.125, ((0, 2),)),
    }


EPSILON = 1e-05
ROPE_BASE = 160000.0

def to_bf(tensor):
    return lax.optimization_barrier(tensor.astype(jnp.bfloat16))

def normalize(tensor):
    centred = tensor - lax.optimization_barrier(jnp.mean(tensor, axis=-1, keepdims=True))
    inv_std = lax.rsqrt(lax.optimization_barrier(jnp.mean(centred * centred, axis=-1, keepdims=True)) + EPSILON)
    return (centred * inv_std, inv_std)

def norm_back(grad_norm, normed, inv_std):
    return inv_std * (grad_norm - lax.optimization_barrier(jnp.mean(grad_norm, axis=-1, keepdims=True)) - normed * lax.optimization_barrier(jnp.mean(grad_norm * normed, axis=-1, keepdims=True)))

def gelu_pair(tensor):
    cumul = 0.5 * (1.0 + jax.scipy.special.erf(tensor * 0.7071067811865476))
    density = jnp.exp(-0.5 * tensor * tensor) * 0.3989422804014327
    return (tensor * cumul, cumul + tensor * density)

def rope_tables(offset, length, head_size):
    positions = (offset + jnp.arange(length, dtype=jnp.int32)).astype(jnp.float32)
    inverse = ROPE_BASE ** (-jnp.arange(0, head_size, 2, dtype=jnp.int32).astype(jnp.float32) / head_size)
    angles = positions[:, None] * inverse[None, :]
    angles = jnp.concatenate([angles, angles], axis=-1)
    return (jnp.cos(angles)[:, None, :], jnp.sin(angles)[:, None, :])

def rotate(tensor, cos_table, sine_table):
    middle = tensor.shape[-1] // 2
    turned = jnp.concatenate([-tensor[..., middle:], tensor[..., :middle]], axis=-1)
    return tensor * cos_table + turned * sine_table

def rotate_back(gradient, cos_table, sine_table):
    middle = gradient.shape[-1] // 2
    scaled = gradient * sine_table
    turned = jnp.concatenate([scaled[..., middle:], -scaled[..., :middle]], axis=-1)
    return gradient * cos_table + turned

def reference(tokens, cotangent, gain_attn, gain_mlp, qkv_weight, out_weight, in_weight, down_weight):
    seq_len = tokens.shape[1]
    scale = HEAD_DIM ** (-0.5)
    q_block = min(512, seq_len)
    block_count = seq_len // q_block
    cos_table, sine_table = rope_tables(0, seq_len, HEAD_DIM)
    f32 = jnp.float32
    bf16 = jnp.bfloat16

    def one_sequence(pair):
        inputs, cot = pair
        resid = inputs.astype(f32)
        normed_a, inv_a = normalize(resid)
        act_a = (normed_a * gain_attn).astype(bf16)
        packed = jnp.dot(act_a, qkv_weight.T, preferred_element_type=f32)
        query = to_bf(rotate(packed[:, :D].reshape(seq_len, HEADS, HEAD_DIM), cos_table, sine_table)).astype(f32)
        keys = to_bf(rotate(packed[:, D:2 * D].reshape(seq_len, HEADS, HEAD_DIM), cos_table, sine_table)).astype(f32)
        values = to_bf(packed[:, 2 * D:].reshape(seq_len, HEADS, HEAD_DIM)).astype(f32)
        query_blocks = query.reshape(block_count, q_block, HEADS, HEAD_DIM)

        def forward_block(query_part):
            scores = jnp.einsum('qhd,khd->hqk', query_part, keys) * scale
            row_max = lax.optimization_barrier(jnp.max(scores, axis=-1))
            row_sum = lax.optimization_barrier(jnp.sum(jnp.exp(scores - row_max[..., None]), axis=-1))
            log_sum = row_max + jnp.log(row_sum)
            weights = to_bf(jnp.exp(scores - log_sum[..., None])).astype(f32)
            return (jnp.einsum('hqk,khd->qhd', weights, values), log_sum)
        mixed_blocks, log_sums = lax.map(forward_block, query_blocks)
        mixed = mixed_blocks.reshape(seq_len, D).astype(bf16)
        middle = resid + jnp.dot(mixed, out_weight.T, preferred_element_type=f32)
        normed_m, inv_m = normalize(middle)
        act_m = (normed_m * gain_mlp).astype(bf16)
        inner = jnp.dot(act_m, in_weight.T, preferred_element_type=f32)
        gelu_val, gelu_slope = gelu_pair(inner[:, :FF])
        gated = (gelu_val * inner[:, FF:]).astype(bf16)
        output = middle + jnp.dot(gated, down_weight.T, preferred_element_type=f32)
        grad_down = jnp.dot(cot.T, gated, preferred_element_type=f32)
        grad_gated = jnp.dot(cot, down_weight, preferred_element_type=f32)
        grad_inner = jnp.concatenate([grad_gated * inner[:, FF:] * gelu_slope, grad_gated * gelu_val], axis=1).astype(bf16)
        grad_in = jnp.dot(grad_inner.T, act_m, preferred_element_type=f32)
        grad_act_m = jnp.dot(grad_inner, in_weight, preferred_element_type=f32)
        grad_gain_m = lax.optimization_barrier(jnp.sum(grad_act_m * normed_m, axis=0))
        grad_middle = cot.astype(f32) + norm_back(grad_act_m * gain_mlp, normed_m, inv_m)
        grad_mid_bf = grad_middle.astype(bf16)
        grad_out = jnp.dot(grad_mid_bf.T, mixed, preferred_element_type=f32)
        grad_mixed = to_bf(jnp.dot(grad_mid_bf, out_weight, preferred_element_type=f32)).astype(f32).reshape(seq_len, HEADS, HEAD_DIM)
        mixed_heads = mixed.astype(f32).reshape(seq_len, HEADS, HEAD_DIM)
        delta = lax.optimization_barrier(jnp.sum(grad_mixed * mixed_heads, axis=-1))
        delta_blocks = delta.reshape(block_count, q_block, HEADS).transpose(0, 2, 1)
        grad_blocks = grad_mixed.reshape(block_count, q_block, HEADS, HEAD_DIM)

        def backward_block(carried, item):
            grad_keys, grad_values = carried
            query_part, grad_part, log_part, delta_part = item
            scores = jnp.einsum('qhd,khd->hqk', query_part, keys) * scale
            probs = jnp.exp(scores - log_part[..., None])
            grad_values = grad_values + jnp.einsum('hqk,qhd->khd', to_bf(probs).astype(f32), grad_part)
            grad_probs = jnp.einsum('qhd,khd->hqk', grad_part, values)
            grad_scores = to_bf(probs * (grad_probs - delta_part[..., None])).astype(f32)
            grad_query = jnp.einsum('hqk,khd->qhd', grad_scores, keys) * scale
            grad_keys = grad_keys + jnp.einsum('hqk,qhd->khd', grad_scores, query_part) * scale
            return ((grad_keys, grad_values), grad_query)
        zeros_kv = jnp.zeros((seq_len, HEADS, HEAD_DIM), f32)
        (grad_keys, grad_values), grad_query = lax.scan(backward_block, (zeros_kv, zeros_kv), (query_blocks, grad_blocks, log_sums, delta_blocks))
        grad_query = rotate_back(grad_query.reshape(seq_len, HEADS, HEAD_DIM), cos_table, sine_table)
        grad_keys = rotate_back(grad_keys, cos_table, sine_table)
        grad_packed = jnp.concatenate([grad_query.reshape(seq_len, D), grad_keys.reshape(seq_len, D), grad_values.reshape(seq_len, D)], axis=1).astype(bf16)
        grad_qkv = jnp.dot(grad_packed.T, act_a, preferred_element_type=f32)
        grad_act_a = jnp.dot(grad_packed, qkv_weight, preferred_element_type=f32)
        grad_gain_a = lax.optimization_barrier(jnp.sum(grad_act_a * normed_a, axis=0))
        grad_input = grad_middle + norm_back(grad_act_a * gain_attn, normed_a, inv_a)
        return (output, grad_input, grad_qkv, grad_out, grad_in, grad_down, grad_gain_a, grad_gain_m)
    results = lax.map(one_sequence, (tokens, cotangent))
    output, grad_input = (results[0], results[1])
    summed = [lax.optimization_barrier(jnp.sum(item, axis=0)) for item in results[2:]]
    return (output, grad_input, summed[0], summed[1], summed[2], summed[3], summed[4], summed[5])
```

```python
import functools
import math

import jax
import jax.numpy as jnp
from jax import lax
from jax.experimental import pallas as pl
from jax.experimental.pallas import tpu as pltpu
from jax.sharding import PartitionSpec as P

HEAD_DIM = 64


EPSILON = 1e-05
ROPE_BASE = 160000.0


def normalize(tensor):
    centred = tensor - jnp.mean(tensor, axis=-1, keepdims=True)
    inv_std = lax.rsqrt(jnp.mean(centred * centred, axis=-1, keepdims=True) + EPSILON)
    return (centred * inv_std, inv_std)


def norm_back(grad_norm, normed, inv_std):
    return inv_std * (
        grad_norm
        - jnp.mean(grad_norm, axis=-1, keepdims=True)
        - normed * jnp.mean(grad_norm * normed, axis=-1, keepdims=True)
    )


def gelu_pair(tensor):
    cumul = 0.5 * (1.0 + jax.scipy.special.erf(tensor * 0.7071067811865476))
    density = jnp.exp(-0.5 * tensor * tensor) * 0.3989422804014327
    return (tensor * cumul, cumul + tensor * density)


def rope_tables(offset, length, head_size):
    positions = (offset + jnp.arange(length, dtype=jnp.int32)).astype(jnp.float32)
    inverse = ROPE_BASE ** (
        -jnp.arange(0, head_size, 2, dtype=jnp.int32).astype(jnp.float32) / head_size
    )
    angles = positions[:, None] * inverse[None, :]
    angles = jnp.concatenate([angles, angles], axis=-1)
    return (jnp.cos(angles)[:, None, :], jnp.sin(angles)[:, None, :])


def rotate(tensor, cos_table, sine_table):
    middle = tensor.shape[-1] // 2
    turned = jnp.concatenate([-tensor[..., middle:], tensor[..., :middle]], axis=-1)
    return tensor * cos_table + turned * sine_table


def rotate_back(gradient, cos_table, sine_table):
    middle = gradient.shape[-1] // 2
    scaled = gradient * sine_table
    turned = jnp.concatenate([scaled[..., middle:], -scaled[..., :middle]], axis=-1)
    return gradient * cos_table + turned


def rows_product(left, right):
    return lax.dot_general(
        left, right, (((1,), (1,)), ((), ())), preferred_element_type=jnp.float32
    )


def rows_contract(left, right):
    return lax.dot_general(
        left, right, (((0,), (0,)), ((), ())), preferred_element_type=jnp.float32
    )


def gathered_layer(
    tokens, cotangent, gain_attn, gain_mlp, qkv_weight, out_weight, in_weight, down_weight
):
    f32 = jnp.float32
    bf16 = jnp.bfloat16
    qkv_full, out_full, in_full, down_full = (
        lax.all_gather(qkv_weight, "fsdp", axis=0, tiled=True),
        lax.all_gather(out_weight, "fsdp", axis=0, tiled=True),
        lax.all_gather(in_weight, "fsdp", axis=0, tiled=True),
        lax.all_gather(down_weight, "fsdp", axis=0, tiled=True),
    )
    tok_rows = tokens.shape[1]
    width = tokens.shape[2]
    hidden = down_full.shape[1]
    head_size = HEAD_DIM
    head_count = width // head_size
    scale = head_size ** (-0.5)
    offset = lax.axis_index("ctx") * tok_rows
    cos_table, sine_table = rope_tables(offset, tok_rows, head_size)
    resid = tokens[0].astype(f32)
    normed_a, inv_a = normalize(resid)
    act_a = (normed_a * gain_attn).astype(bf16)
    packed = rows_product(act_a, qkv_full)
    query_heads = rotate(
        packed[:, :width].reshape(tok_rows, head_count, head_size), cos_table, sine_table
    ).astype(bf16)
    key_heads = rotate(
        packed[:, width : 2 * width].reshape(tok_rows, head_count, head_size), cos_table, sine_table
    ).astype(bf16)
    value_send = packed[:, 2 * width :].astype(bf16)
    key_send = key_heads.reshape(tok_rows, width)
    value_heads = value_send.reshape(tok_rows, head_count, head_size)
    start_state = (
        jnp.zeros((tok_rows, head_count, head_size), f32),
        jnp.full((head_count, tok_rows), -1e30, f32),
        jnp.zeros((head_count, tok_rows), f32),
    )
    key_piece = lax.all_gather(key_send, "ctx", axis=0, tiled=True)
    value_piece = lax.all_gather(value_send, "ctx", axis=0, tiled=True)
    length = key_piece.shape[0]
    step_len = math.gcd(length, 1024)

    def attend_block(block_num, running):
        weighted, row_max, row_sum = running
        key_blk = lax.dynamic_slice_in_dim(key_piece, block_num * step_len, step_len, 0).reshape(
            step_len, head_count, head_size
        )
        value_blk = lax.dynamic_slice_in_dim(
            value_piece, block_num * step_len, step_len, 0
        ).reshape(step_len, head_count, head_size)
        scores = (
            jnp.einsum("qhd,khd->hqk", query_heads, key_blk, preferred_element_type=f32) * scale
        )
        new_max = jnp.maximum(row_max, jnp.max(scores, axis=-1))
        shrink = jnp.exp(row_max - new_max)
        weights = jnp.exp(scores - new_max[..., None])
        row_sum = row_sum * shrink + jnp.sum(weights, axis=-1)
        weighted = weighted * shrink.T[:, :, None] + jnp.einsum(
            "hqk,khd->qhd", weights.astype(bf16), value_blk, preferred_element_type=f32
        )
        return (weighted, new_max, row_sum)

    weighted, row_max, row_sum = lax.fori_loop(0, length // step_len, attend_block, start_state)
    log_sum = row_max + jnp.log(row_sum)
    mixed = (weighted / row_sum.T[:, :, None]).reshape(tok_rows, width).astype(bf16)
    middle = resid + rows_product(mixed, out_full)
    normed_m, inv_m = normalize(middle)
    act_m = (normed_m * gain_mlp).astype(bf16)
    inner = rows_product(act_m, in_full)
    gelu_val, gelu_slope = gelu_pair(inner[:, :hidden])
    gated = (gelu_val * inner[:, hidden:]).astype(bf16)
    output = middle + rows_product(gated, down_full)
    cot_rows = cotangent[0]
    grad_down = rows_contract(cot_rows, gated)
    grad_gated = jnp.dot(cot_rows, down_full, preferred_element_type=f32)
    grad_inner = jnp.concatenate(
        [grad_gated * inner[:, hidden:] * gelu_slope, grad_gated * gelu_val], axis=1
    ).astype(bf16)
    grad_in = rows_contract(grad_inner, act_m)
    grad_act_m = jnp.dot(grad_inner, in_full, preferred_element_type=f32)
    grad_gain_m = jnp.sum(grad_act_m * normed_m, axis=0)
    grad_middle = cot_rows.astype(f32) + norm_back(grad_act_m * gain_mlp, normed_m, inv_m)
    grad_mid_bf = grad_middle.astype(bf16)
    grad_out = rows_contract(grad_mid_bf, mixed)
    grad_mixed = jnp.dot(grad_mid_bf, out_full, preferred_element_type=f32).astype(bf16)
    grad_heads = grad_mixed.reshape(tok_rows, head_count, head_size)
    delta_rows = jnp.sum(
        grad_heads.astype(f32) * mixed.reshape(tok_rows, head_count, head_size).astype(f32), axis=-1
    )
    delta = delta_rows.T
    zeros_heads = jnp.zeros((tok_rows, head_count, head_size), f32)
    query_key_piece = lax.all_gather(key_send, "ctx", axis=0, tiled=True)
    query_value_piece = lax.all_gather(value_send, "ctx", axis=0, tiled=True)
    length = query_key_piece.shape[0]
    query_step_len = math.gcd(length, 1024)

    def query_grad_block(block_num, grad_query):
        key_blk = lax.dynamic_slice_in_dim(
            query_key_piece, block_num * query_step_len, query_step_len, 0
        ).reshape(query_step_len, head_count, head_size)
        value_blk = lax.dynamic_slice_in_dim(
            query_value_piece, block_num * query_step_len, query_step_len, 0
        ).reshape(query_step_len, head_count, head_size)
        scores = (
            jnp.einsum("qhd,khd->hqk", query_heads, key_blk, preferred_element_type=f32) * scale
        )
        probs = jnp.exp(scores - log_sum[..., None])
        grad_probs = jnp.einsum("qhd,khd->hqk", grad_heads, value_blk, preferred_element_type=f32)
        grad_scores = (probs * (grad_probs - delta[..., None])).astype(bf16)
        return (
            grad_query
            + jnp.einsum("hqk,khd->qhd", grad_scores, key_blk, preferred_element_type=f32) * scale
        )

    grad_query = lax.fori_loop(0, length // query_step_len, query_grad_block, zeros_heads)
    query_send = query_heads.reshape(tok_rows, width).astype(f32)
    grad_send = grad_mixed.astype(f32)
    query_piece = lax.all_gather(query_send, "ctx", axis=0, tiled=True)
    grad_piece = lax.all_gather(grad_send, "ctx", axis=0, tiled=True)
    log_piece = lax.all_gather(log_sum.T, "ctx", axis=0, tiled=True)
    delta_piece = lax.all_gather(delta_rows, "ctx", axis=0, tiled=True)
    length = query_piece.shape[0]
    key_step_len = math.gcd(length, 1024)

    def key_grad_block(block_num, running):
        grad_keys, grad_values = running
        query_blk = (
            lax.dynamic_slice_in_dim(query_piece, block_num * key_step_len, key_step_len, 0)
            .astype(bf16)
            .reshape(key_step_len, head_count, head_size)
        )
        grad_blk = (
            lax.dynamic_slice_in_dim(grad_piece, block_num * key_step_len, key_step_len, 0)
            .astype(bf16)
            .reshape(key_step_len, head_count, head_size)
        )
        log_blk = lax.dynamic_slice_in_dim(log_piece, block_num * key_step_len, key_step_len, 0).T
        delta_blk = lax.dynamic_slice_in_dim(
            delta_piece, block_num * key_step_len, key_step_len, 0
        ).T
        scores = (
            jnp.einsum("qhd,khd->hqk", query_blk, key_heads, preferred_element_type=f32) * scale
        )
        probs = jnp.exp(scores - log_blk[..., None])
        grad_values = grad_values + jnp.einsum(
            "hqk,qhd->khd", probs.astype(bf16), grad_blk, preferred_element_type=f32
        )
        grad_probs = jnp.einsum("qhd,khd->hqk", grad_blk, value_heads, preferred_element_type=f32)
        grad_scores = (probs * (grad_probs - delta_blk[..., None])).astype(bf16)
        grad_keys = (
            grad_keys
            + jnp.einsum("hqk,qhd->khd", grad_scores, query_blk, preferred_element_type=f32) * scale
        )
        return (grad_keys, grad_values)

    grad_keys, grad_values = lax.fori_loop(
        0, length // key_step_len, key_grad_block, (zeros_heads, zeros_heads)
    )
    grad_query = rotate_back(grad_query, cos_table, sine_table)
    grad_keys = rotate_back(grad_keys, cos_table, sine_table)
    grad_packed = jnp.concatenate(
        [
            grad_query.reshape(tok_rows, width),
            grad_keys.reshape(tok_rows, width),
            grad_values.reshape(tok_rows, width),
        ],
        axis=1,
    ).astype(bf16)
    grad_qkv = rows_contract(grad_packed, act_a)
    grad_act_a = jnp.dot(grad_packed, qkv_full, preferred_element_type=f32)
    grad_gain_a = jnp.sum(grad_act_a * normed_a, axis=0)
    grad_input = grad_middle + norm_back(grad_act_a * gain_attn, normed_a, inv_a)
    owned = (
        lax.psum_scatter(grad_qkv, ("ctx", "fsdp"), scatter_dimension=0, tiled=True),
        lax.psum_scatter(grad_out, ("ctx", "fsdp"), scatter_dimension=0, tiled=True),
        lax.psum_scatter(grad_in, ("ctx", "fsdp"), scatter_dimension=0, tiled=True),
        lax.psum_scatter(grad_down, ("ctx", "fsdp"), scatter_dimension=0, tiled=True),
        lax.psum_scatter(grad_gain_a, ("ctx", "fsdp"), scatter_dimension=0, tiled=True),
        lax.psum_scatter(grad_gain_m, ("ctx", "fsdp"), scatter_dimension=0, tiled=True),
    )
    return (
        output[None],
        grad_input[None],
        owned[0],
        owned[1],
        owned[2],
        owned[3],
        owned[4],
        owned[5],
    )


MESH = pl.DeviceIdType.MESH
VMEM_LIMIT = 60 * 1024 * 1024


def matmul(left, right, left_dim, right_dim):
    return lax.dot_general(
        left, right, (((left_dim,), (right_dim,)), ((), ())), preferred_element_type=jnp.float32
    )


class Place:
    def __init__(self, count):
        self.count, self.line = count, count // 4
        self.me = lax.axis_index("ctx")
        self.z, self.x, self.core = self.me // 4, self.me // 2 % 2, self.me % 2

    def slot(self, z, x, core):
        return z * 4 + x * 2 + core

    def far(self, step):
        last = self.line - 1
        low = 2 * self.z < self.line
        own = jnp.where(low, self.z, last - self.z)
        at = jnp.where(
            step < last - own, last - step, jnp.where(step == last, own, step - (last - own))
        )
        return jnp.where(low, at, last - at)

    def near(self, step):
        return self.far(self.line - 1 - step)

    def meet(self):
        barrier = pltpu.get_barrier_semaphore()

        @pl.loop(1, self.count)
        def _(shift):
            pl.semaphore_signal(
                barrier, inc=1, device_id={"ctx": (self.me + shift) % self.count}, device_id_type=MESH
            )

        pl.semaphore_wait(barrier, self.count - 1)

    def copy(self, src, dst, send, recv, to):
        return pltpu.make_async_remote_copy(
            src_ref=src, dst_ref=dst, send_sem=send, recv_sem=recv,
            device_id={"ctx": to}, device_id_type=MESH,
        )


class Gather:
    def __init__(self, place, buf, sems):
        self.p, self.buf = place, buf
        self.up_s, self.up_r, self.dn_s, self.dn_r, self.x_s, self.x_r, self.c_s, self.c_r = sems

    @staticmethod
    def sems(line):
        return [pltpu.SemaphoreType.DMA((line,))] * 6 + [pltpu.SemaphoreType.DMA((2 * line,))] * 2

    def over(self, z, x, core, send, recv, to):
        at = self.buf.at[self.p.slot(z, x, core)]
        return self.p.copy(at, at, send, recv, to)

    def up(self, z):
        p = self.p
        return self.over(z, p.x, p.core, self.up_s.at[z], self.up_r.at[z], (p.me + 4) % p.count)

    def down(self, z):
        p = self.p
        return self.over(z, p.x, p.core, self.dn_s.at[z], self.dn_r.at[z], (p.me + p.count - 4) % p.count)

    def across(self, z):
        p = self.p
        return self.over(z, p.x, p.core, self.x_s.at[z], self.x_r.at[z], p.slot(p.z, 1 - p.x, p.core))

    def beside(self, z, x):
        p = self.p
        at = z * 2 + x
        return self.over(z, x, p.core, self.c_s.at[at], self.c_r.at[at], p.slot(p.z, p.x, 1 - p.core))

    def arrive(self, z):
        p = self.p

        @pl.when(z < p.z)
        def _():
            self.up(z).wait_recv()

        @pl.when(z > p.z)
        def _():
            self.down(z).wait_recv()

        @pl.when((z <= p.z) & (p.z < p.line - 1))
        def _():
            self.up(z).start()

        @pl.when((z >= p.z) & (p.z > 0))
        def _():
            self.down(z).start()

        self.across(z).start()
        self.beside(z, p.x).start()

    def arrive_across(self, z):
        self.across(z).wait_recv()
        self.beside(z, 1 - self.p.x).start()

    def part(self, turn, use=None):
        p = self.p
        step, part = turn // 4, turn % 4
        z = jnp.where(part == 0, p.near(step), p.near(step - 1))

        @pl.when(jnp.where(part == 0, step < p.line, step > 0))
        def _():
            @pl.when(part == 0)
            def _():
                self.arrive(z)

            @pl.when(part == 1)
            def _():
                self.arrive_across(z)

            x = jnp.where(part % 2 == 0, p.x, 1 - p.x)

            @pl.when(part >= 2)
            def _():
                self.beside(z, x).wait_recv()

            if use is not None:
                use(z, x, jnp.where(part < 2, p.core, 1 - p.core))

    def sent(self):
        p = self.p

        @pl.loop(0, p.line)
        def _(z):
            @pl.when((z <= p.z) & (p.z < p.line - 1))
            def _():
                self.up(z).wait_send()

            @pl.when((z >= p.z) & (p.z > 0))
            def _():
                self.down(z).wait_send()

            self.across(z).wait_send()
            self.beside(z, 0).wait_send()
            self.beside(z, 1).wait_send()


class Halve:
    def __init__(self, place, whole, got, sums, sems):
        self.p, self.whole, self.got, self.sums = place, whole, got, sums
        self.c_s, self.c_r = sems

    @staticmethod
    def sems(line):
        return [pltpu.SemaphoreType.DMA((2 * line,))] * 2

    def beside(self, z, x):
        p, at = self.p, z * 2 + x
        return p.copy(
            self.whole.at[p.slot(z, x, 1 - p.core)], self.got.at[at], self.c_s.at[at], self.c_r.at[at],
            p.slot(p.z, p.x, 1 - p.core),
        )

    def add(self, z):
        p = self.p
        for x in range(2):
            at = z * 2 + x
            self.beside(z, x).wait_recv()
            self.sums[at] = (
                self.whole[p.slot(z, x, p.core)].astype(jnp.float32) + self.got[at].astype(jnp.float32)
            ).astype(self.sums.dtype)

    def sent(self):
        @pl.loop(0, 2 * self.p.line)
        def _(at):
            self.beside(at // 2, at % 2).wait_send()


class Settle:
    def __init__(self, place, sums, bufs, sems):
        self.p, self.sums = place, sums
        self.got, self.total, self.low, self.high = bufs
        self.x_s, self.x_r, self.up_s, self.up_r, self.dn_s, self.dn_r = sems

    @staticmethod
    def sems(line):
        return [pltpu.SemaphoreType.DMA((line,))] * 6

    @staticmethod
    def bufs(line, block):
        return [pltpu.VMEM((line,) + block, jnp.bfloat16)] * 4

    def across(self, z):
        p = self.p
        return p.copy(
            self.sums.at[z * 2 + 1 - p.x], self.got.at[z], self.x_s.at[z], self.x_r.at[z],
            p.slot(p.z, 1 - p.x, p.core),
        )

    def up(self, z):
        p = self.p
        return p.copy(self.total.at[z], self.low.at[z], self.up_s.at[z], self.up_r.at[z], (p.me + 4) % p.count)

    def down(self, z):
        p = self.p
        return p.copy(
            self.total.at[z], self.high.at[z], self.dn_s.at[z], self.dn_r.at[z], (p.me + p.count - 4) % p.count
        )

    def pass_on(self, z):
        p, f32 = self.p, jnp.float32
        self.across(z).wait_recv()
        self.total[z] = (
            self.sums[z * 2 + p.x].astype(f32) + self.got[z].astype(f32)
        ).astype(self.total.dtype)

        @pl.when(z > p.z)
        def _():
            @pl.when(p.z > 0)
            def _():
                self.up(z).wait_recv()
                self.total[z] = (self.total[z].astype(f32) + self.low[z].astype(f32)).astype(self.total.dtype)

            self.up(z).start()

        @pl.when(z < p.z)
        def _():
            @pl.when(p.z < p.line - 1)
            def _():
                self.down(z).wait_recv()
                self.total[z] = (self.total[z].astype(f32) + self.high[z].astype(f32)).astype(self.total.dtype)

            self.down(z).start()

    def finish(self, out):
        p, f32 = self.p, jnp.float32
        out[...] = self.total[p.z].astype(f32)

        @pl.when(p.z > 0)
        def _():
            self.up(p.z).wait_recv()
            out[...] += self.low[p.z].astype(f32)

        @pl.when(p.z < p.line - 1)
        def _():
            self.down(p.z).wait_recv()
            out[...] += self.high[p.z].astype(f32)

    def sent(self):
        p = self.p

        @pl.loop(0, p.line)
        def _(z):
            self.across(z).wait_send()

            @pl.when(z > p.z)
            def _():
                self.up(z).wait_send()

            @pl.when(z < p.z)
            def _():
                self.down(z).wait_send()


class Exchange:
    def __init__(self, place, src, dst, sems):
        self.p, self.src, self.dst = place, src, dst
        self.s, self.r = sems

    @staticmethod
    def sems(count):
        return [pltpu.SemaphoreType.DMA((count,))] * 2

    def to(self, j):
        return self.p.copy(self.src.at[j], self.dst.at[self.p.me], self.s.at[j], self.r.at[self.p.me], j)

    def send(self, j):
        @pl.when(j != self.p.me)
        def _():
            self.to(j).start()

        @pl.when(j == self.p.me)
        def _():
            self.dst[j] = self.src[j]

    def arrived(self):
        p = self.p

        @pl.loop(1, p.count)
        def _(shift):
            j = (p.me + shift) % p.count
            p.copy(self.src.at[j], self.dst.at[j], self.s.at[j], self.r.at[j], j).wait_recv()

    def sent(self):
        p = self.p

        @pl.loop(1, p.count)
        def _(shift):
            self.to((p.me + shift) % p.count).wait_send()


def turn(value):
    half = value.shape[0] // 2
    return jnp.concatenate([-value[half:], value[:half]], axis=0)


def turn_back(value):
    half = value.shape[0] // 2
    return jnp.concatenate([value[half:], -value[:half]], axis=0)


def attend_kernel(
    count, act, cot, weight, cos, sine,
    act_all, cot_all, query_t, keys_t, keys, values, mixed_own, log_sum, mixed,
    values_t, load_sem, *sems
):
    f32, bf16 = jnp.float32, jnp.bfloat16
    p = Place(count)
    rows, head = act.shape[0], keys_t.shape[0]
    n = 8
    first = Gather(p, act_all, sems[:n])
    second = Gather(p, cot_all, sems[n : 2 * n])
    trade = Exchange(p, mixed_own, mixed, sems[2 * n :])
    loads = [
        pltpu.make_async_copy(act, act_all.at[p.me], load_sem.at[0]),
        pltpu.make_async_copy(cot, cot_all.at[p.me], load_sem.at[1]),
    ]
    for load in loads:
        load.start()
    p.meet()
    for load in loads:
        load.wait()

    def project(z, x, core):
        at = p.slot(z, x, core)
        lanes = pl.ds(pl.multiple_of(at * rows, rows), rows)
        packed = matmul(weight[...], act_all[at], 1, 1)
        c, s = cos[:, lanes], sine[:, lanes]
        query, key = packed[:head], packed[head : 2 * head]
        query_t[:, lanes] = (query * c + turn(query) * s).astype(bf16)
        key = key * c + turn(key) * s
        keys_t[:, lanes] = key.astype(bf16)
        values_t[:, lanes] = packed[2 * head :].astype(bf16)
        keys[lanes, :] = key.T.astype(bf16)
        values[lanes, :] = packed[2 * head :].T.astype(bf16)

    @pl.loop(0, 4 * p.line + 4)
    def _(at):
        first.part(at, project)

    def gather_more(step):
        for part in range(4):
            second.part(step * 4 + part)

    gather_more(0)
    wide = 2 * rows
    blocks = count // 2
    scale = head ** (-0.5)

    def attend(i):
        block = (p.me // 2 + i) % blocks
        lanes = pl.ds(pl.multiple_of(block * wide, wide), wide)
        scores = matmul(keys[...], query_t[:, lanes], 1, 0) * scale
        top = jnp.max(scores, axis=0, keepdims=True)
        weights = jnp.exp(scores - top)
        total = jnp.sum(weights, axis=0, keepdims=True)
        log_sum[:, lanes] = top + jnp.log(total)
        out = (matmul(values_t[...], weights.astype(bf16), 1, 0) / total).astype(bf16)
        mixed_own[2 * block] = out[:, :rows]
        mixed_own[2 * block + 1] = out[:, rows:]
        trade.send(2 * block)
        trade.send(2 * block + 1)

    @pl.loop(0, blocks // 2)
    def _(i):
        attend(i)

    gather_more(1)

    @pl.loop(blocks // 2, blocks)
    def _(i):
        attend(i)

    for step in range(2, p.line):
        gather_more(step)
    trade.arrived()
    gather_more(p.line)
    first.sent()
    second.sent()
    trade.sent()


def feed_kernel(
    count, act, cot_all, weight, down,
    grad_act, out_sums, grad_weight, grad_down,
    act_all, gated, inner_grad, grad_part, out_part, grad_got, grad_sums, out_got, load_sem, *rest
):
    f32, bf16 = jnp.float32, jnp.bfloat16
    p = Place(count)
    rows, group = act.shape[0], down.shape[1]
    bufs, sems = rest[:4], rest[4:]
    gather = Gather(p, act_all, sems[:8])
    halve = Halve(p, grad_part, grad_got, grad_sums, sems[8:10])
    settle = Settle(p, grad_sums, bufs, sems[10:16])
    halve_out = Halve(p, out_part, out_got, out_sums, sems[16:18])
    load = pltpu.make_async_copy(act, act_all.at[p.me], load_sem)
    load.start()
    p.meet()
    load.wait()

    def feed(z, x, core):
        at = p.slot(z, x, core)
        inner = matmul(act_all[at], weight[...], 1, 1)
        grad_gated = matmul(cot_all[at], down[...], 1, 0)
        value, gate = inner[:, :group], inner[:, group:]
        gelu_val, gelu_slope = gelu_pair(value)
        token = pl.ds(pl.multiple_of(at * rows, rows), rows)
        out = (gelu_val * gate).astype(bf16)
        gated[token, :] = out
        grads = jnp.concatenate(
            [grad_gated * gate * gelu_slope, grad_gated * gelu_val], axis=1
        ).astype(bf16)
        inner_grad[token, :] = grads
        grad_part[at] = matmul(grads, weight[...], 1, 0).astype(bf16)

        @pl.when(core != p.core)
        def _():
            halve.beside(z, x).start()

        out_part[at] = matmul(out, down[...], 1, 1).astype(bf16)

        @pl.when(core != p.core)
        def _():
            halve_out.beside(z, x).start()

    @pl.loop(0, 4 * p.line + 4)
    def _(at):
        gather.part(at, feed)

    @pl.loop(0, p.line)
    def _(step):
        z = p.far(step)
        halve.add(z)
        settle.across(z).start()

    def grad_chunk(step):
        token = pl.ds(pl.multiple_of(step * 4 * rows, 4 * rows), 4 * rows)
        acts = jnp.concatenate([act_all[4 * step + i] for i in range(4)], axis=0)
        cots = jnp.concatenate([cot_all[4 * step + i] for i in range(4)], axis=0)
        return matmul(inner_grad[token, :], acts, 0, 0), matmul(cots, gated[token, :], 0, 0)

    grad_weight[...], grad_down[...] = grad_chunk(0)

    @pl.loop(0, p.line)
    def _(step):
        settle.pass_on(p.far(step))

        @pl.when(step > 0)
        def _():
            more = grad_chunk(step)
            grad_weight[...] += more[0]
            grad_down[...] += more[1]

        halve_out.add(step)

    settle.finish(grad_act)
    gather.sent()
    halve.sent()
    halve_out.sent()
    settle.sent()


def attend_back_kernel(
    count, grad_mixed, out_sums, query_t, keys_t, keys, values, mixed_own, log_sum, act_all, weight, cos, sine,
    grad_act, out_total, grad_weight,
    grad_own, grad_keys, grad_values, grad_packed, grad_part, grad_got, grad_sums, *rest
):
    f32, bf16 = jnp.float32, jnp.bfloat16
    p = Place(count)
    rows, head = grad_mixed.shape[2], keys_t.shape[0]
    bufs, out_bufs, sems = rest[:4], rest[4:8], rest[8:]
    trade = Exchange(p, grad_mixed, grad_own, sems[:2])
    halve = Halve(p, grad_part, grad_got, grad_sums, sems[2:4])
    settle = Settle(p, grad_sums, bufs, sems[4:10])
    settle_out = Settle(p, out_sums, out_bufs, sems[10:16])
    p.meet()

    @pl.loop(0, count)
    def _(shift):
        trade.send((p.me + shift) % count)

    @pl.loop(0, p.line)
    def _(step):
        settle_out.across(p.far(step)).start()

    grad_keys[...] = jnp.zeros_like(grad_keys)
    grad_values[...] = jnp.zeros_like(grad_values)
    trade.arrived()
    wide = 2 * rows
    scale = head ** (-0.5)

    def back(i):
        lanes = pl.ds(pl.multiple_of(i * wide, wide), wide)
        query = query_t[:, lanes]
        grad = jnp.concatenate([grad_own[2 * i], grad_own[2 * i + 1]], axis=1)
        own = jnp.concatenate([mixed_own[2 * i], mixed_own[2 * i + 1]], axis=1)
        delta = jnp.sum(grad.astype(f32) * own.astype(f32), axis=0, keepdims=True)
        scores = matmul(keys[...], query, 1, 0) * scale
        probs = jnp.exp(scores - log_sum[:, lanes])
        grad_values[...] += matmul(probs.astype(bf16), grad, 1, 1)
        grad_probs = matmul(values[...], grad, 1, 0)
        grad_scores = (probs * (grad_probs - delta)).astype(bf16)
        grad_keys[...] += matmul(grad_scores, query, 1, 1)
        grad_query = matmul(keys_t[...], grad_scores, 1, 0) * scale
        back_query = grad_query * cos[:, lanes] + turn_back(grad_query * sine[:, lanes])
        grad_packed[:head, lanes] = back_query.astype(bf16)

    @pl.loop(0, count // 2)
    def _(i):
        back(i)

    @pl.loop(0, p.line)
    def _(step):
        settle_out.pass_on(p.far(step))

    grad_key = grad_keys[...].T * scale
    grad_packed[head : 2 * head, :] = (grad_key * cos[...] + turn_back(grad_key * sine[...])).astype(bf16)
    grad_packed[2 * head :, :] = grad_values[...].T.astype(bf16)

    @pl.loop(0, p.line)
    def _(step):
        z = p.far(step)
        for at in range(4):
            lanes = pl.ds(pl.multiple_of((z * 4 + at) * rows, rows), rows)
            grad_part[z * 4 + at] = matmul(grad_packed[:, lanes], weight[...], 0, 0).astype(bf16)
        halve.beside(z, 0).start()
        halve.beside(z, 1).start()

    @pl.loop(0, p.line)
    def _(step):
        z = p.far(step)
        halve.add(z)
        settle.across(z).start()

    def grad_chunk(step):
        lanes = pl.ds(pl.multiple_of(step * 4 * rows, 4 * rows), 4 * rows)
        acts = jnp.concatenate([act_all[4 * step + i] for i in range(4)], axis=0)
        return matmul(grad_packed[:, lanes], acts, 1, 0)

    grad_weight[...] = grad_chunk(0)

    @pl.loop(0, p.line)
    def _(step):
        settle.pass_on(p.far(step))

        @pl.when(step > 0)
        def _():
            grad_weight[...] += grad_chunk(step)

    settle_out.finish(out_total)
    settle.finish(grad_act)
    trade.sent()
    halve.sent()
    settle.sent()
    settle_out.sent()


def run_kernel(body, outs, scratch, collective, flops, args):
    vmem = pl.BlockSpec(memory_space=pltpu.VMEM)
    return pl.pallas_call(
        body,
        out_shape=outs,
        in_specs=[vmem] * len(args),
        out_specs=[vmem] * len(outs),
        scratch_shapes=scratch,
        compiler_params=pltpu.CompilerParams(
            collective_id=collective, has_side_effects=True, vmem_limit_bytes=VMEM_LIMIT
        ),
        cost_estimate=pl.CostEstimate(flops=flops, bytes_accessed=20_000_000, transcendentals=0),
        name=body.func.__name__,
    )(*args)


def shaped(shape, kind):
    return jax.ShapeDtypeStruct(shape, kind)


def attend(count, act, cot, weight, cos, sine):
    bf16, f32 = jnp.bfloat16, jnp.float32
    rows, width = act.shape
    head, length, line = weight.shape[0] // 3, rows * count, count // 4
    blocks = shaped((count, rows, width), bf16)
    tall, flat = shaped((head, length), bf16), shaped((length, head), bf16)
    heads = shaped((count, head, rows), bf16)
    return run_kernel(
        functools.partial(attend_kernel, count),
        [blocks, blocks, tall, tall, flat, flat, heads, shaped((1, length), f32), heads],
        [pltpu.VMEM((head, length), bf16), pltpu.SemaphoreType.DMA((2,))]
        + Gather.sems(line) * 2 + Exchange.sems(count),
        0, 10_000_000_000, [act, cot, weight, cos, sine],
    )


def feed(count, act, cot_all, weight, down):
    bf16, f32 = jnp.bfloat16, jnp.float32
    rows, width = act.shape
    group, length, line = down.shape[1], rows * count, count // 4
    block = (rows, width)
    whole, half = pltpu.VMEM((count,) + block, bf16), pltpu.VMEM((2 * line,) + block, bf16)
    return run_kernel(
        functools.partial(feed_kernel, count),
        [shaped(block, f32), shaped((2 * line,) + block, bf16), shaped(weight.shape, f32), shaped(down.shape, f32)],
        [whole, pltpu.VMEM((length, group), bf16), pltpu.VMEM((length, 2 * group), bf16), whole, whole,
         half, half, half, pltpu.SemaphoreType.DMA]
        + Settle.bufs(line, block)
        + Gather.sems(line) + Halve.sems(line) + Settle.sems(line) + Halve.sems(line),
        1, 20_000_000_000, [act, cot_all, weight, down],
    )


def attend_back(count, grad_mixed, out_sums, kept, act_all, weight, cos, sine):
    bf16, f32 = jnp.bfloat16, jnp.float32
    rows, width = act_all.shape[1:]
    head, length, line = weight.shape[0] // 3, rows * count, count // 4
    block = (rows, width)
    whole, half = pltpu.VMEM((count,) + block, bf16), pltpu.VMEM((2 * line,) + block, bf16)
    flat = pltpu.VMEM((length, head), f32)
    return run_kernel(
        functools.partial(attend_back_kernel, count),
        [shaped(block, f32), shaped(block, f32), shaped(weight.shape, f32)],
        [pltpu.VMEM((count, head, rows), bf16), flat, flat, pltpu.VMEM((3 * head, length), bf16), whole, half, half]
        + Settle.bufs(line, block) * 2
        + Exchange.sems(count) + Halve.sems(line) + Settle.sems(line) * 2,
        2, 20_000_000_000, [grad_mixed, out_sums, *kept, act_all, weight, cos, sine],
    )


def swap_perm(count, stride):
    return [(i, i + stride if (i // stride) % 2 == 0 else i - stride) for i in range(count)]


def line_perm(count, stride, shift):
    return [(i, (i + shift * stride) % count) for i in range(count)]


def pick(cond, first, second):
    return jnp.where(cond, first, second)


def scatter_sum(partial):
    count = lax.axis_size("ctx")
    index = lax.axis_index("ctx")
    line = count // 4
    line_pos = index // 4
    f32 = jnp.float32
    rest = partial.reshape((line, 2, 2) + partial.shape[1:])
    for stride in (1, 2):
        axis = 2 if stride == 1 else 1
        mine = lax.rem(index // stride, 2)
        keep = lax.dynamic_index_in_dim(rest, mine, axis, keepdims=False)
        send = lax.dynamic_index_in_dim(rest, 1 - mine, axis, keepdims=False)
        got = lax.ppermute(send, "ctx", swap_perm(count, stride))
        rest = (keep.astype(f32) + got.astype(f32)).astype(partial.dtype)
    total = lax.dynamic_index_in_dim(rest, line_pos, 0, keepdims=False).astype(f32)
    for shift in range(1, line):
        send = lax.dynamic_index_in_dim(rest, lax.rem(line_pos + shift, line), 0, keepdims=False)
        total = total + lax.ppermute(send, "ctx", line_perm(count, 4, shift)).astype(f32)
    return total


def pair_halves(low, high):
    second = lax.axis_index("fsdp") == 1
    send = pick(second, low, high)
    keep = pick(second, high, low)
    return keep + lax.ppermute(send, "fsdp", [(0, 1), (1, 0)])


def pair_rows(mine):
    other = lax.ppermute(mine, "fsdp", [(0, 1), (1, 0)])
    second = lax.axis_index("fsdp") == 1
    return pick(second, other, mine), pick(second, mine, other)


def tensor_layer(
    tokens, cotangent, gain_attn, gain_mlp, qkv_weight, out_weight, in_weight, down_weight
):
    f32 = jnp.float32
    bf16 = jnp.bfloat16
    count = lax.axis_size("ctx")
    devices = count * lax.axis_size("fsdp")
    index = lax.axis_index("ctx")
    pair = lax.axis_index("fsdp")
    place = index * 2 + pair
    rows, width = tokens.shape[1], tokens.shape[2]
    length = rows * count
    head_size = width // count
    hidden = in_weight.shape[0]
    group = hidden // count
    padding = -group % 128
    unit = width // devices

    half_rows = qkv_weight.shape[0]

    def head_rows(part):
        start = part * width + index * head_size
        owner = start // half_rows
        own = lax.dynamic_slice_in_dim(qkv_weight, start - owner * half_rows, head_size, 0)
        return owner == pair, own

    owned = [head_rows(part) for part in range(3)]
    got = lax.ppermute(jnp.stack([own for _, own in owned]), "fsdp", [(0, 1), (1, 0)])
    qkv_head = jnp.concatenate([jnp.where(here, own, got[i]) for i, (here, own) in enumerate(owned)], axis=0)
    in_mine = lax.dynamic_slice_in_dim(in_weight, index * group, group, 0)
    in_both = jnp.concatenate([jnp.pad(part, ((0, padding), (0, 0))) for part in pair_rows(in_mine)], axis=0)
    down_mine = lax.dynamic_slice_in_dim(down_weight, index * group, group, 1)
    down_cols = jnp.concatenate([jnp.pad(part, ((0, 0), (0, padding))) for part in pair_rows(down_mine)], axis=0)
    out_full = jnp.concatenate(pair_rows(out_weight), axis=0)

    cos_table, sine_table = rope_tables(0, length, head_size)
    cos_table, sine_table = cos_table[:, 0].T, sine_table[:, 0].T
    resid = tokens[0].astype(f32)
    normed_a, inv_a = normalize(resid)
    act_a = (normed_a * gain_attn).astype(bf16)
    cot_rows = cotangent[0]
    act_all, cot_all, *kept, mixed = attend(count, act_a, cot_rows, qkv_head, cos_table, sine_table)
    mixed = mixed.reshape(width, rows)
    middle = resid + matmul(mixed, out_full, 0, 1)
    normed_m, inv_m = normalize(middle)
    act_m = (normed_m * gain_mlp).astype(bf16)
    grad_act_m, out_sums, grad_in_both, grad_down_cols = feed(count, act_m, cot_all, in_both, down_cols)

    grad_middle = cot_rows.astype(f32) + norm_back(grad_act_m * gain_mlp, normed_m, inv_m)
    grad_mid_bf = grad_middle.astype(bf16)
    grad_mixed = matmul(out_full, grad_mid_bf, 0, 1).astype(bf16).reshape(count, head_size, rows)

    padded = group + padding
    grad_in_half = pair_halves(grad_in_both[:group], grad_in_both[padded : padded + group])
    grad_in = lax.ppermute(
        grad_in_half,
        ("ctx", "fsdp"),
        [(c * 2 + y, y * count + c) for c in range(count) for y in range(2)],
    )
    grad_down_cols = grad_down_cols[:, :group].reshape(count, 2, unit, group)
    grad_down_half = pair_halves(grad_down_cols[:, 0], grad_down_cols[:, 1])
    grad_down = lax.all_to_all(grad_down_half, "ctx", 0, 0).transpose(1, 0, 2).reshape(unit, hidden)
    grad_out_part = matmul(grad_mid_bf, mixed, 0, 1).reshape(count, 2, unit, width)
    grad_out = scatter_sum(pair_halves(grad_out_part[:, 0], grad_out_part[:, 1]).astype(bf16))

    grad_act_a, out_total, grad_qkv_head = attend_back(
        count, grad_mixed, out_sums, kept, act_all, qkv_head, cos_table, sine_table
    )
    output = middle + out_total
    grad_qkv_head = grad_qkv_head.reshape(3, 2, unit, width)
    grad_units = pair_halves(grad_qkv_head[:, 0], grad_qkv_head[:, 1])
    inverse = pow(3, -1, devices)
    slots = []
    for slot in range(3):
        owner = lax.rem((place - slot + devices) * inverse, devices)
        piece = lax.dynamic_index_in_dim(grad_units, (3 * owner + slot) // devices, 0, keepdims=False)
        slots.append(
            lax.ppermute(
                piece, ("ctx", "fsdp"), [((3 * o + slot) % devices, o) for o in range(devices)]
            )
        )
    grad_qkv = jnp.concatenate(slots, axis=0)
    grad_gain_m = jnp.sum(grad_act_m * normed_m, axis=0)
    grad_gain_a = jnp.sum(grad_act_a * normed_a, axis=0)
    grad_input = grad_middle + norm_back(grad_act_a * gain_attn, normed_a, inv_a)
    gains = jnp.stack([grad_gain_a, grad_gain_m]).reshape(2, devices, unit).transpose(1, 0, 2)
    gains = jnp.sum(lax.all_to_all(gains, ("ctx", "fsdp"), 0, 0), axis=0)
    return (output[None], grad_input[None], grad_qkv, grad_out, grad_in, grad_down, gains[0], gains[1])


def solution(mesh):

    def layer(*arrays):
        one_head_each = arrays[0].shape[2] == HEAD_DIM * mesh.shape["ctx"]
        if one_head_each and mesh.shape["fsdp"] == 2 and mesh.shape["ctx"] % 4 == 0:
            return tensor_layer(*arrays)
        return gathered_layer(*arrays)

    return jax.shard_map(
        layer,
        mesh=mesh,
        in_specs=(
            P("fsdp", "ctx", None),
            P("fsdp", "ctx", None),
            P(),
            P(),
            P("fsdp", None),
            P("fsdp", None),
            P("fsdp", None),
            P("fsdp", None),
        ),
        out_specs=(
            P("fsdp", "ctx", None),
            P("fsdp", "ctx", None),
            P(("ctx", "fsdp"), None),
            P(("ctx", "fsdp"), None),
            P(("ctx", "fsdp"), None),
            P(("ctx", "fsdp"), None),
            P(("ctx", "fsdp")),
            P(("ctx", "fsdp")),
        ),
        check_vma=False,
    )
```

```python
import functools
import math

import jax
import jax.numpy as jnp
from jax import lax
from jax.experimental import pallas as pl
from jax.experimental.pallas import tpu as pltpu
from jax.sharding import PartitionSpec as P

HEAD_DIM = 64


EPSILON = 1e-05
ROPE_BASE = 160000.0


def normalize(tensor):
    centred = tensor - jnp.mean(tensor, axis=-1, keepdims=True)
    inv_std = lax.rsqrt(jnp.mean(centred * centred, axis=-1, keepdims=True) + EPSILON)
    return (centred * inv_std, inv_std)


def norm_back(grad_norm, normed, inv_std):
    return inv_std * (
        grad_norm
        - jnp.mean(grad_norm, axis=-1, keepdims=True)
        - normed * jnp.mean(grad_norm * normed, axis=-1, keepdims=True)
    )


def gelu_pair(tensor):
    cumul = 0.5 * (1.0 + jax.scipy.special.erf(tensor * 0.7071067811865476))
    density = jnp.exp(-0.5 * tensor * tensor) * 0.3989422804014327
    return (tensor * cumul, cumul + tensor * density)


def rope_tables(offset, length, head_size):
    positions = (offset + jnp.arange(length, dtype=jnp.int32)).astype(jnp.float32)
    inverse = ROPE_BASE ** (
        -jnp.arange(0, head_size, 2, dtype=jnp.int32).astype(jnp.float32) / head_size
    )
    angles = positions[:, None] * inverse[None, :]
    angles = jnp.concatenate([angles, angles], axis=-1)
    return (jnp.cos(angles)[:, None, :], jnp.sin(angles)[:, None, :])


def rotate(tensor, cos_table, sine_table):
    middle = tensor.shape[-1] // 2
    turned = jnp.concatenate([-tensor[..., middle:], tensor[..., :middle]], axis=-1)
    return tensor * cos_table + turned * sine_table


def rotate_back(gradient, cos_table, sine_table):
    middle = gradient.shape[-1] // 2
    scaled = gradient * sine_table
    turned = jnp.concatenate([scaled[..., middle:], -scaled[..., :middle]], axis=-1)
    return gradient * cos_table + turned


def rows_product(left, right):
    return lax.dot_general(
        left, right, (((1,), (1,)), ((), ())), preferred_element_type=jnp.float32
    )


def rows_contract(left, right):
    return lax.dot_general(
        left, right, (((0,), (0,)), ((), ())), preferred_element_type=jnp.float32
    )


def gathered_layer(
    tokens, cotangent, gain_attn, gain_mlp, qkv_weight, out_weight, in_weight, down_weight
):
    f32 = jnp.float32
    bf16 = jnp.bfloat16
    qkv_full, out_full, in_full, down_full = (
        lax.all_gather(qkv_weight, "fsdp", axis=0, tiled=True),
        lax.all_gather(out_weight, "fsdp", axis=0, tiled=True),
        lax.all_gather(in_weight, "fsdp", axis=0, tiled=True),
        lax.all_gather(down_weight, "fsdp", axis=0, tiled=True),
    )
    tok_rows = tokens.shape[1]
    width = tokens.shape[2]
    hidden = down_full.shape[1]
    head_size = HEAD_DIM
    head_count = width // head_size
    scale = head_size ** (-0.5)
    offset = lax.axis_index("ctx") * tok_rows
    cos_table, sine_table = rope_tables(offset, tok_rows, head_size)
    resid = tokens[0].astype(f32)
    normed_a, inv_a = normalize(resid)
    act_a = (normed_a * gain_attn).astype(bf16)
    packed = rows_product(act_a, qkv_full)
    query_heads = rotate(
        packed[:, :width].reshape(tok_rows, head_count, head_size), cos_table, sine_table
    ).astype(bf16)
    key_heads = rotate(
        packed[:, width : 2 * width].reshape(tok_rows, head_count, head_size), cos_table, sine_table
    ).astype(bf16)
    value_send = packed[:, 2 * width :].astype(bf16)
    key_send = key_heads.reshape(tok_rows, width)
    value_heads = value_send.reshape(tok_rows, head_count, head_size)
    start_state = (
        jnp.zeros((tok_rows, head_count, head_size), f32),
        jnp.full((head_count, tok_rows), -1e30, f32),
        jnp.zeros((head_count, tok_rows), f32),
    )
    key_piece = lax.all_gather(key_send, "ctx", axis=0, tiled=True)
    value_piece = lax.all_gather(value_send, "ctx", axis=0, tiled=True)
    length = key_piece.shape[0]
    step_len = math.gcd(length, 1024)

    def attend_block(block_num, running):
        weighted, row_max, row_sum = running
        key_blk = lax.dynamic_slice_in_dim(key_piece, block_num * step_len, step_len, 0).reshape(
            step_len, head_count, head_size
        )
        value_blk = lax.dynamic_slice_in_dim(
            value_piece, block_num * step_len, step_len, 0
        ).reshape(step_len, head_count, head_size)
        scores = (
            jnp.einsum("qhd,khd->hqk", query_heads, key_blk, preferred_element_type=f32) * scale
        )
        new_max = jnp.maximum(row_max, jnp.max(scores, axis=-1))
        shrink = jnp.exp(row_max - new_max)
        weights = jnp.exp(scores - new_max[..., None])
        row_sum = row_sum * shrink + jnp.sum(weights, axis=-1)
        weighted = weighted * shrink.T[:, :, None] + jnp.einsum(
            "hqk,khd->qhd", weights.astype(bf16), value_blk, preferred_element_type=f32
        )
        return (weighted, new_max, row_sum)

    weighted, row_max, row_sum = lax.fori_loop(0, length // step_len, attend_block, start_state)
    log_sum = row_max + jnp.log(row_sum)
    mixed = (weighted / row_sum.T[:, :, None]).reshape(tok_rows, width).astype(bf16)
    middle = resid + rows_product(mixed, out_full)
    normed_m, inv_m = normalize(middle)
    act_m = (normed_m * gain_mlp).astype(bf16)
    inner = rows_product(act_m, in_full)
    gelu_val, gelu_slope = gelu_pair(inner[:, :hidden])
    gated = (gelu_val * inner[:, hidden:]).astype(bf16)
    output = middle + rows_product(gated, down_full)
    cot_rows = cotangent[0]
    grad_down = rows_contract(cot_rows, gated)
    grad_gated = jnp.dot(cot_rows, down_full, preferred_element_type=f32)
    grad_inner = jnp.concatenate(
        [grad_gated * inner[:, hidden:] * gelu_slope, grad_gated * gelu_val], axis=1
    ).astype(bf16)
    grad_in = rows_contract(grad_inner, act_m)
    grad_act_m = jnp.dot(grad_inner, in_full, preferred_element_type=f32)
    grad_gain_m = jnp.sum(grad_act_m * normed_m, axis=0)
    grad_middle = cot_rows.astype(f32) + norm_back(grad_act_m * gain_mlp, normed_m, inv_m)
    grad_mid_bf = grad_middle.astype(bf16)
    grad_out = rows_contract(grad_mid_bf, mixed)
    grad_mixed = jnp.dot(grad_mid_bf, out_full, preferred_element_type=f32).astype(bf16)
    grad_heads = grad_mixed.reshape(tok_rows, head_count, head_size)
    delta_rows = jnp.sum(
        grad_heads.astype(f32) * mixed.reshape(tok_rows, head_count, head_size).astype(f32), axis=-1
    )
    delta = delta_rows.T
    zeros_heads = jnp.zeros((tok_rows, head_count, head_size), f32)
    query_key_piece = lax.all_gather(key_send, "ctx", axis=0, tiled=True)
    query_value_piece = lax.all_gather(value_send, "ctx", axis=0, tiled=True)
    length = query_key_piece.shape[0]
    query_step_len = math.gcd(length, 1024)

    def query_grad_block(block_num, grad_query):
        key_blk = lax.dynamic_slice_in_dim(
            query_key_piece, block_num * query_step_len, query_step_len, 0
        ).reshape(query_step_len, head_count, head_size)
        value_blk = lax.dynamic_slice_in_dim(
            query_value_piece, block_num * query_step_len, query_step_len, 0
        ).reshape(query_step_len, head_count, head_size)
        scores = (
            jnp.einsum("qhd,khd->hqk", query_heads, key_blk, preferred_element_type=f32) * scale
        )
        probs = jnp.exp(scores - log_sum[..., None])
        grad_probs = jnp.einsum("qhd,khd->hqk", grad_heads, value_blk, preferred_element_type=f32)
        grad_scores = (probs * (grad_probs - delta[..., None])).astype(bf16)
        return (
            grad_query
            + jnp.einsum("hqk,khd->qhd", grad_scores, key_blk, preferred_element_type=f32) * scale
        )

    grad_query = lax.fori_loop(0, length // query_step_len, query_grad_block, zeros_heads)
    query_send = query_heads.reshape(tok_rows, width).astype(f32)
    grad_send = grad_mixed.astype(f32)
    query_piece = lax.all_gather(query_send, "ctx", axis=0, tiled=True)
    grad_piece = lax.all_gather(grad_send, "ctx", axis=0, tiled=True)
    log_piece = lax.all_gather(log_sum.T, "ctx", axis=0, tiled=True)
    delta_piece = lax.all_gather(delta_rows, "ctx", axis=0, tiled=True)
    length = query_piece.shape[0]
    key_step_len = math.gcd(length, 1024)

    def key_grad_block(block_num, running):
        grad_keys, grad_values = running
        query_blk = (
            lax.dynamic_slice_in_dim(query_piece, block_num * key_step_len, key_step_len, 0)
            .astype(bf16)
            .reshape(key_step_len, head_count, head_size)
        )
        grad_blk = (
            lax.dynamic_slice_in_dim(grad_piece, block_num * key_step_len, key_step_len, 0)
            .astype(bf16)
            .reshape(key_step_len, head_count, head_size)
        )
        log_blk = lax.dynamic_slice_in_dim(log_piece, block_num * key_step_len, key_step_len, 0).T
        delta_blk = lax.dynamic_slice_in_dim(
            delta_piece, block_num * key_step_len, key_step_len, 0
        ).T
        scores = (
            jnp.einsum("qhd,khd->hqk", query_blk, key_heads, preferred_element_type=f32) * scale
        )
        probs = jnp.exp(scores - log_blk[..., None])
        grad_values = grad_values + jnp.einsum(
            "hqk,qhd->khd", probs.astype(bf16), grad_blk, preferred_element_type=f32
        )
        grad_probs = jnp.einsum("qhd,khd->hqk", grad_blk, value_heads, preferred_element_type=f32)
        grad_scores = (probs * (grad_probs - delta_blk[..., None])).astype(bf16)
        grad_keys = (
            grad_keys
            + jnp.einsum("hqk,qhd->khd", grad_scores, query_blk, preferred_element_type=f32) * scale
        )
        return (grad_keys, grad_values)

    grad_keys, grad_values = lax.fori_loop(
        0, length // key_step_len, key_grad_block, (zeros_heads, zeros_heads)
    )
    grad_query = rotate_back(grad_query, cos_table, sine_table)
    grad_keys = rotate_back(grad_keys, cos_table, sine_table)
    grad_packed = jnp.concatenate(
        [
            grad_query.reshape(tok_rows, width),
            grad_keys.reshape(tok_rows, width),
            grad_values.reshape(tok_rows, width),
        ],
        axis=1,
    ).astype(bf16)
    grad_qkv = rows_contract(grad_packed, act_a)
    grad_act_a = jnp.dot(grad_packed, qkv_full, preferred_element_type=f32)
    grad_gain_a = jnp.sum(grad_act_a * normed_a, axis=0)
    grad_input = grad_middle + norm_back(grad_act_a * gain_attn, normed_a, inv_a)
    owned = (
        lax.psum_scatter(grad_qkv, ("ctx", "fsdp"), scatter_dimension=0, tiled=True),
        lax.psum_scatter(grad_out, ("ctx", "fsdp"), scatter_dimension=0, tiled=True),
        lax.psum_scatter(grad_in, ("ctx", "fsdp"), scatter_dimension=0, tiled=True),
        lax.psum_scatter(grad_down, ("ctx", "fsdp"), scatter_dimension=0, tiled=True),
        lax.psum_scatter(grad_gain_a, ("ctx", "fsdp"), scatter_dimension=0, tiled=True),
        lax.psum_scatter(grad_gain_m, ("ctx", "fsdp"), scatter_dimension=0, tiled=True),
    )
    return (
        output[None],
        grad_input[None],
        owned[0],
        owned[1],
        owned[2],
        owned[3],
        owned[4],
        owned[5],
    )


MESH = pl.DeviceIdType.MESH
VMEM_LIMIT = 60 * 1024 * 1024


def matmul(left, right, left_dim, right_dim):
    return lax.dot_general(
        left, right, (((left_dim,), (right_dim,)), ((), ())), preferred_element_type=jnp.float32
    )


class Place:
    def __init__(self, count):
        self.count, self.line = count, count // 4
        self.me, self.pair = lax.axis_index("ctx"), lax.axis_index("fsdp")
        self.owner = self.me * 2 + self.pair
        self.z, self.x, self.core = self.me // 4, self.me // 2 % 2, self.me % 2

    def slot(self, z, x, core):
        return z * 4 + x * 2 + core

    def far(self, step):
        last = self.line - 1
        low = 2 * self.z < self.line
        own = jnp.where(low, self.z, last - self.z)
        at = jnp.where(
            step < last - own, last - step, jnp.where(step == last, own, step - (last - own))
        )
        return jnp.where(low, at, last - at)

    def near(self, step):
        return self.far(self.line - 1 - step)

    def meet(self, everyone=False):
        barrier = pltpu.get_barrier_semaphore()

        @pl.loop(1, self.count)
        def _(shift):
            pl.semaphore_signal(
                barrier, inc=1, device_id={"ctx": (self.me + shift) % self.count}, device_id_type=MESH
            )

        if everyone:
            @pl.loop(0, self.count)
            def _(to):
                pl.semaphore_signal(
                    barrier, inc=1, device_id={"ctx": to, "fsdp": 1 - self.pair}, device_id_type=MESH
                )

            pl.semaphore_wait(barrier, 2 * self.count - 1)
        else:
            pl.semaphore_signal(barrier, inc=1, device_id={"fsdp": 1 - self.pair}, device_id_type=MESH)
            pl.semaphore_wait(barrier, self.count)

    def over_pair(self, src, dst, send, recv):
        return pltpu.make_async_remote_copy(
            src_ref=src, dst_ref=dst, send_sem=send, recv_sem=recv,
            device_id={"fsdp": 1 - self.pair}, device_id_type=MESH,
        )

    def to_owner(self, src, dst, send, recv, owner):
        return pltpu.make_async_remote_copy(
            src_ref=src, dst_ref=dst, send_sem=send, recv_sem=recv,
            device_id={"ctx": owner // 2, "fsdp": owner % 2}, device_id_type=MESH,
        )

    def copy(self, src, dst, send, recv, to):
        return pltpu.make_async_remote_copy(
            src_ref=src, dst_ref=dst, send_sem=send, recv_sem=recv,
            device_id={"ctx": to}, device_id_type=MESH,
        )


class Gather:
    def __init__(self, place, buf, sems):
        self.p, self.buf = place, buf
        self.up_s, self.up_r, self.dn_s, self.dn_r, self.x_s, self.x_r, self.c_s, self.c_r = sems

    @staticmethod
    def sems(line):
        return [pltpu.SemaphoreType.DMA((line,))] * 6 + [pltpu.SemaphoreType.DMA((2 * line,))] * 2

    def over(self, z, x, core, send, recv, to):
        at = self.buf.at[self.p.slot(z, x, core)]
        return self.p.copy(at, at, send, recv, to)

    def up(self, z):
        p = self.p
        return self.over(z, p.x, p.core, self.up_s.at[z], self.up_r.at[z], (p.me + 4) % p.count)

    def down(self, z):
        p = self.p
        return self.over(z, p.x, p.core, self.dn_s.at[z], self.dn_r.at[z], (p.me + p.count - 4) % p.count)

    def across(self, z):
        p = self.p
        return self.over(z, p.x, p.core, self.x_s.at[z], self.x_r.at[z], p.slot(p.z, 1 - p.x, p.core))

    def beside(self, z, x):
        p = self.p
        at = z * 2 + x
        return self.over(z, x, p.core, self.c_s.at[at], self.c_r.at[at], p.slot(p.z, p.x, 1 - p.core))

    def arrive(self, z):
        p = self.p

        @pl.when(z < p.z)
        def _():
            self.up(z).wait_recv()

        @pl.when(z > p.z)
        def _():
            self.down(z).wait_recv()

        @pl.when((z <= p.z) & (p.z < p.line - 1))
        def _():
            self.up(z).start()

        @pl.when((z >= p.z) & (p.z > 0))
        def _():
            self.down(z).start()

        self.across(z).start()
        self.beside(z, p.x).start()

    def arrive_across(self, z):
        self.across(z).wait_recv()
        self.beside(z, 1 - self.p.x).start()

    def part(self, turn, use=None):
        p = self.p
        step, part = turn // 4, turn % 4
        z = jnp.where(part == 0, p.near(step), p.near(step - 1))

        @pl.when(jnp.where(part == 0, step < p.line, step > 0))
        def _():
            @pl.when(part == 0)
            def _():
                self.arrive(z)

            @pl.when(part == 1)
            def _():
                self.arrive_across(z)

            x = jnp.where(part % 2 == 0, p.x, 1 - p.x)

            @pl.when(part >= 2)
            def _():
                self.beside(z, x).wait_recv()

            if use is not None:
                use(z, x, jnp.where(part < 2, p.core, 1 - p.core))

    def sent(self):
        p = self.p

        @pl.loop(0, p.line)
        def _(z):
            @pl.when((z <= p.z) & (p.z < p.line - 1))
            def _():
                self.up(z).wait_send()

            @pl.when((z >= p.z) & (p.z > 0))
            def _():
                self.down(z).wait_send()

            self.across(z).wait_send()
            self.beside(z, 0).wait_send()
            self.beside(z, 1).wait_send()


class Halve:
    def __init__(self, place, whole, got, sums, sems):
        self.p, self.whole, self.got, self.sums = place, whole, got, sums
        self.c_s, self.c_r = sems

    @staticmethod
    def sems(line):
        return [pltpu.SemaphoreType.DMA((2 * line,))] * 2

    def beside(self, z, x):
        p, at = self.p, z * 2 + x
        return p.copy(
            self.whole.at[p.slot(z, x, 1 - p.core)], self.got.at[at], self.c_s.at[at], self.c_r.at[at],
            p.slot(p.z, p.x, 1 - p.core),
        )

    def add(self, z):
        p = self.p
        for x in range(2):
            at = z * 2 + x
            self.beside(z, x).wait_recv()
            self.sums[at] = (
                self.whole[p.slot(z, x, p.core)].astype(jnp.float32) + self.got[at].astype(jnp.float32)
            ).astype(self.sums.dtype)

    def sent(self):
        @pl.loop(0, 2 * self.p.line)
        def _(at):
            self.beside(at // 2, at % 2).wait_send()


class Settle:
    def __init__(self, place, sums, bufs, sems):
        self.p, self.sums = place, sums
        self.got, self.total, self.low, self.high = bufs
        self.x_s, self.x_r, self.up_s, self.up_r, self.dn_s, self.dn_r = sems

    @staticmethod
    def sems(line):
        return [pltpu.SemaphoreType.DMA((line,))] * 6

    @staticmethod
    def bufs(line, block):
        return [pltpu.VMEM((line,) + block, jnp.bfloat16)] * 4

    def across(self, z):
        p = self.p
        return p.copy(
            self.sums.at[z * 2 + 1 - p.x], self.got.at[z], self.x_s.at[z], self.x_r.at[z],
            p.slot(p.z, 1 - p.x, p.core),
        )

    def up(self, z):
        p = self.p
        return p.copy(self.total.at[z], self.low.at[z], self.up_s.at[z], self.up_r.at[z], (p.me + 4) % p.count)

    def down(self, z):
        p = self.p
        return p.copy(
            self.total.at[z], self.high.at[z], self.dn_s.at[z], self.dn_r.at[z], (p.me + p.count - 4) % p.count
        )

    def pass_on(self, z):
        p, f32 = self.p, jnp.float32
        self.across(z).wait_recv()
        self.total[z] = (
            self.sums[z * 2 + p.x].astype(f32) + self.got[z].astype(f32)
        ).astype(self.total.dtype)

        @pl.when(z > p.z)
        def _():
            @pl.when(p.z > 0)
            def _():
                self.up(z).wait_recv()
                self.total[z] = (self.total[z].astype(f32) + self.low[z].astype(f32)).astype(self.total.dtype)

            self.up(z).start()

        @pl.when(z < p.z)
        def _():
            @pl.when(p.z < p.line - 1)
            def _():
                self.down(z).wait_recv()
                self.total[z] = (self.total[z].astype(f32) + self.high[z].astype(f32)).astype(self.total.dtype)

            self.down(z).start()

    def finish(self, out):
        p, f32 = self.p, jnp.float32
        out[...] = self.total[p.z].astype(f32)

        @pl.when(p.z > 0)
        def _():
            self.up(p.z).wait_recv()
            out[...] += self.low[p.z].astype(f32)

        @pl.when(p.z < p.line - 1)
        def _():
            self.down(p.z).wait_recv()
            out[...] += self.high[p.z].astype(f32)

    def sent(self):
        p = self.p

        @pl.loop(0, p.line)
        def _(z):
            self.across(z).wait_send()

            @pl.when(z > p.z)
            def _():
                self.up(z).wait_send()

            @pl.when(z < p.z)
            def _():
                self.down(z).wait_send()


class Exchange:
    def __init__(self, place, src, dst, sems):
        self.p, self.src, self.dst = place, src, dst
        self.s, self.r = sems

    @staticmethod
    def sems(count):
        return [pltpu.SemaphoreType.DMA((count,))] * 2

    def to(self, j):
        return self.p.copy(self.src.at[j], self.dst.at[self.p.me], self.s.at[j], self.r.at[self.p.me], j)

    def send(self, j):
        @pl.when(j != self.p.me)
        def _():
            self.to(j).start()

        @pl.when(j == self.p.me)
        def _():
            self.dst[j] = self.src[j]

    def arrived(self):
        p = self.p

        @pl.loop(1, p.count)
        def _(shift):
            j = (p.me + shift) % p.count
            p.copy(self.src.at[j], self.dst.at[j], self.s.at[j], self.r.at[j], j).wait_recv()

    def sent(self):
        p = self.p

        @pl.loop(1, p.count)
        def _(shift):
            self.to((p.me + shift) % p.count).wait_send()


class Spread:
    def __init__(self, place, src, dst, sems):
        self.p, self.src, self.dst = place, src, dst
        self.s, self.r = sems

    @staticmethod
    def sems(count):
        return [pltpu.SemaphoreType.DMA((2 * count,))] * 2

    def to(self, j):
        p = self.p
        return p.to_owner(self.src.at[j], self.dst.at[p.owner], self.s.at[j], self.r.at[p.owner], j)

    def send(self):
        p = self.p
        self.dst[p.owner] = self.src[p.owner]

        @pl.loop(1, 2 * p.count)
        def _(shift):
            self.to((p.owner + shift) % (2 * p.count)).start()

    def arrived(self):
        p = self.p

        @pl.loop(1, 2 * p.count)
        def _(shift):
            j = (p.owner + shift) % (2 * p.count)
            p.to_owner(self.src.at[j], self.dst.at[j], self.s.at[j], self.r.at[j], j).wait_recv()

    def sent(self):
        p = self.p

        @pl.loop(1, 2 * p.count)
        def _(shift):
            self.to((p.owner + shift) % (2 * p.count)).wait_send()


class Deliver:
    def __init__(self, place, src, dst, sems):
        self.p, self.src, self.dst = place, src, dst
        self.s, self.r = sems

    def away(self, piece, owner, slot):
        return self.p.to_owner(self.src.at[piece], self.dst.at[slot], self.s.at[piece], self.r.at[slot], owner)

    def send(self, piece, owner, slot):
        @pl.when(owner != self.p.owner)
        def _():
            self.away(piece, owner, slot).start()

        @pl.when(owner == self.p.owner)
        def _():
            self.dst[slot] = self.src[piece]

    def sent(self, piece, owner, slot):
        @pl.when(owner != self.p.owner)
        def _():
            self.away(piece, owner, slot).wait_send()

    def arrived(self, slot, source):
        p = self.p

        @pl.when(source != p.owner)
        def _():
            p.to_owner(self.src.at[0], self.dst.at[slot], self.s.at[0], self.r.at[slot], source).wait_recv()


def turn(value):
    half = value.shape[0] // 2
    return jnp.concatenate([-value[half:], value[:half]], axis=0)


def turn_back(value):
    half = value.shape[0] // 2
    return jnp.concatenate([value[half:], -value[:half]], axis=0)


def attend_kernel(
    count, act, cot, qkv_weight, in_mine, down_mine, out_mine, cos, sine,
    act_all, cot_all, query_t, keys_t, keys, values, mixed_own, log_sum, mixed, weight, in_pair, down_pair, out_pair,
    values_t, load_sem, part_sem, part_got, piece_sem, piece_got, *sems
):
    f32, bf16 = jnp.float32, jnp.bfloat16
    p = Place(count)
    rows, head = act.shape[0], keys_t.shape[0]
    width = count * head
    n = 8
    first = Gather(p, act_all, sems[:n])
    second = Gather(p, cot_all, sems[n : 2 * n])
    trade = Exchange(p, mixed_own, mixed, sems[2 * n :])
    pieces = [(in_mine, in_pair), (down_mine, down_pair), (out_mine, out_pair)]
    loads = [(act, act_all.at[p.me]), (cot, cot_all.at[p.me])] + [(src, dst.at[p.pair]) for src, dst in pieces]
    loads = [pltpu.make_async_copy(src, dst, load_sem.at[i]) for i, (src, dst) in enumerate(loads)]
    for load in loads:
        load.start()

    def part_rows(part):
        start = part * width + p.me * head
        holder = start // qkv_weight.shape[0]
        at = pl.ds(pl.multiple_of(start - holder * qkv_weight.shape[0], head), head)
        return holder == p.pair, qkv_weight.at[at]

    def part_copies(part):
        here, src = part_rows(part)
        return (
            here,
            pltpu.make_async_copy(src, weight.at[part], load_sem.at[5 + part]),
            p.over_pair(src, weight.at[part], part_sem.at[part], part_got.at[part]),
        )

    swaps = [
        p.over_pair(src, dst.at[p.pair], piece_sem.at[i], piece_got.at[i]) for i, (src, dst) in enumerate(pieces)
    ]
    for part in range(3):
        here, own, away = part_copies(part)

        @pl.when(here)
        def _():
            own.start()

    p.meet()
    for part in range(3):
        here, own, away = part_copies(part)

        @pl.when(here)
        def _():
            away.start()

    for swap in swaps:
        swap.start()
    for load in loads:
        load.wait()

    first.part(0)
    for part in range(3):
        here, own, away = part_copies(part)

        @pl.when(here)
        def _():
            own.wait()

        @pl.when(jnp.logical_not(here))
        def _():
            away.wait_recv()

    head_weight = weight[...].reshape(3 * head, act.shape[1])

    def project(z, x, core):
        at = p.slot(z, x, core)
        lanes = pl.ds(pl.multiple_of(at * rows, rows), rows)
        packed = matmul(head_weight, act_all[at], 1, 1)
        c, s = cos[:, lanes], sine[:, lanes]
        query, key = packed[:head], packed[head : 2 * head]
        query_t[:, lanes] = (query * c + turn(query) * s).astype(bf16)
        key = key * c + turn(key) * s
        keys_t[:, lanes] = key.astype(bf16)
        values_t[:, lanes] = packed[2 * head :].astype(bf16)
        keys[lanes, :] = key.T.astype(bf16)
        values[lanes, :] = packed[2 * head :].T.astype(bf16)

    project(p.z, p.x, p.core)

    @pl.loop(4, 4 * p.line + 4)
    def _(at):
        first.part(at, project)

    def gather_more(step):
        for part in range(4):
            second.part(step * 4 + part)

    gather_more(0)
    wide = 2 * rows
    blocks = count // 2
    scale = head ** (-0.5)

    def attend(i):
        block = (p.me // 2 + i) % blocks
        lanes = pl.ds(pl.multiple_of(block * wide, wide), wide)
        scores = matmul(keys[...], query_t[:, lanes], 1, 0) * scale
        top = jnp.max(scores, axis=0, keepdims=True)
        weights = jnp.exp(scores - top)
        total = jnp.sum(weights, axis=0, keepdims=True)
        log_sum[:, lanes] = top + jnp.log(total)
        out = (matmul(values_t[...], weights.astype(bf16), 1, 0) / total).astype(bf16)
        mixed_own[2 * block] = out[:, :rows]
        mixed_own[2 * block + 1] = out[:, rows:]
        trade.send(2 * block)
        trade.send(2 * block + 1)

    @pl.loop(0, blocks // 2)
    def _(i):
        attend(i)

    gather_more(1)

    @pl.loop(blocks // 2, blocks)
    def _(i):
        attend(i)

    for step in range(2, p.line):
        gather_more(step)
    trade.arrived()
    gather_more(p.line)
    first.sent()
    second.sent()
    trade.sent()
    for part in range(3):
        here, own, away = part_copies(part)

        @pl.when(here)
        def _():
            away.wait_send()

    for swap in swaps:
        swap.wait()


def feed_kernel(
    count, act, cot_all, in_pair, down_pair, gain,
    grad_act, out_sums, in_grad, down_grad,
    weight, down, grad_weight, grad_down,
    act_all, gated, inner_grad, grad_part, out_part, grad_got, grad_sums, out_got, load_sem, *rest
):
    f32, bf16 = jnp.float32, jnp.bfloat16
    p = Place(count)
    rows, group = act.shape[0], down.shape[1]
    bufs, sems = rest[:4], rest[4:]
    gather = Gather(p, act_all, sems[:8])
    halve = Halve(p, grad_part, grad_got, grad_sums, sems[8:10])
    settle = Settle(p, grad_sums, bufs, sems[10:16])
    halve_out = Halve(p, out_part, out_got, out_sums, sems[16:18])
    load = pltpu.make_async_copy(act, act_all.at[p.me], load_sem)
    load.start()
    units, half = in_pair.shape[1], down_pair.shape[1]
    weight[...] = jnp.zeros_like(weight)
    down[...] = jnp.zeros_like(down)
    for at in range(2):
        weight[at * group : at * group + units, :] = in_pair[at]
        down[at * half : (at + 1) * half, :units] = down_pair[at]
    p.meet()
    load.wait()

    def feed(z, x, core):
        at = p.slot(z, x, core)
        inner = matmul(act_all[at], weight[...], 1, 1)
        grad_gated = matmul(cot_all[at], down[...], 1, 0)
        value, gate = inner[:, :group], inner[:, group:]
        gelu_val, gelu_slope = gelu_pair(value)
        token = pl.ds(pl.multiple_of(at * rows, rows), rows)
        out = (gelu_val * gate).astype(bf16)
        gated[token, :] = out
        grads = jnp.concatenate(
            [grad_gated * gate * gelu_slope, grad_gated * gelu_val], axis=1
        ).astype(bf16)
        inner_grad[token, :] = grads
        grad_part[at] = matmul(grads, weight[...], 1, 0).astype(bf16)

        @pl.when(core != p.core)
        def _():
            halve.beside(z, x).start()

        out_part[at] = matmul(out, down[...], 1, 1).astype(bf16)

        @pl.when(core != p.core)
        def _():
            halve_out.beside(z, x).start()

    @pl.loop(0, 4 * p.line + 4)
    def _(at):
        gather.part(at, feed)

    @pl.loop(0, p.line)
    def _(step):
        z = p.far(step)
        halve.add(z)
        settle.across(z).start()

    def grad_chunk(step):
        token = pl.ds(pl.multiple_of(step * 4 * rows, 4 * rows), 4 * rows)
        acts = jnp.concatenate([act_all[4 * step + i] for i in range(4)], axis=0)
        cots = jnp.concatenate([cot_all[4 * step + i] for i in range(4)], axis=0)
        return matmul(inner_grad[token, :], acts, 0, 0), matmul(cots, gated[token, :], 0, 0)

    grad_weight[...], grad_down[...] = grad_chunk(0)

    @pl.loop(0, p.line)
    def _(step):
        settle.pass_on(p.far(step))

        @pl.when(step > 0)
        def _():
            more = grad_chunk(step)
            grad_weight[...] += more[0]
            grad_down[...] += more[1]

        halve_out.add(step)

    for at in range(2):
        in_grad[at] = grad_weight[at * group : at * group + units, :].astype(bf16)
    gain_row = jnp.sum(grad_weight[...] * weight[...].astype(f32), axis=0, keepdims=True) / gain[...]
    lane = lax.broadcasted_iota(jnp.int32, grad_down.shape, 1)
    column = jnp.broadcast_to(gain_row, (8, gain_row.shape[1])).T[:, :1]
    down_grad[...] = jnp.where(lane == units, column, grad_down[...]).astype(bf16).reshape(down_grad.shape)
    settle.finish(grad_act)
    gather.sent()
    halve.sent()
    halve_out.sent()
    settle.sent()


def attend_back_kernel(
    count, grad_mixed, grad_mid, mixed, out_sums, query_t, keys_t, keys, values, mixed_own, log_sum,
    act_all, weight, cos, sine, in_grad, down_grad, gain,
    grad_act, out_total, qkv_out, out_out, in_out, down_out, gain_m_out, gain_a_out,
    grad_own, grad_keys, grad_values, grad_packed, grad_part, grad_got, grad_sums, grad_weight,
    pair_part, pair_got, proj_part, proj_got, proj_sums, in_got, down_got, qkv_part, qkv_got, gain_part, gain_got,
    pair_s, pair_r, in_s, in_r, qkv_s, qkv_r, *rest
):
    f32, bf16 = jnp.float32, jnp.bfloat16
    p = Place(count)
    rows, head = grad_mixed.shape[2], keys_t.shape[0]
    width, unit = count * head, head // 2
    bufs, out_bufs, proj_bufs, sems = rest[:4], rest[4:8], rest[8:12], rest[12:]
    trade = Exchange(p, grad_mixed, grad_own, sems[:2])
    halve = Halve(p, grad_part, grad_got, grad_sums, sems[2:4])
    settle = Settle(p, grad_sums, bufs, sems[4:10])
    settle_out = Settle(p, out_sums, out_bufs, sems[10:16])
    halve_proj = Halve(p, proj_part, proj_got, proj_sums, sems[16:18])
    settle_proj = Settle(p, proj_sums, proj_bufs, sems[18:24])
    spread_down = Spread(p, down_grad, down_got, sems[24:26])
    spread_gain = Spread(p, gain_part, gain_got, sems[26:28])
    give_in = Deliver(p, in_grad, in_got, (in_s, in_r))
    give_qkv = Deliver(p, qkv_part, qkv_got, (qkv_s, qkv_r))
    swap = p.over_pair(pair_part.at[1 - p.pair], pair_got, pair_s, pair_r)
    p.meet(True)

    @pl.loop(0, count)
    def _(shift):
        trade.send((p.me + shift) % count)

    @pl.loop(0, p.line)
    def _(step):
        settle_out.across(p.far(step)).start()

    for part in range(2):
        give_in.send(part, part * count + p.me, p.pair)
    spread_down.send()
    flat = mixed[...].reshape(width, rows)

    @pl.loop(0, count // 2)
    def _(i):
        lanes = pl.ds(pl.multiple_of(i * 4 * unit, 4 * unit), 4 * unit)
        piece = matmul(grad_mid[:, lanes], flat, 0, 1).astype(bf16)
        for at in range(4):
            pair_part[at % 2, 2 * i + at // 2] = piece[at * unit : (at + 1) * unit]

    swap.start()
    grad_keys[...] = jnp.zeros_like(grad_keys)
    grad_values[...] = jnp.zeros_like(grad_values)
    trade.arrived()
    wide = 2 * rows
    scale = head ** (-0.5)

    def back(i):
        lanes = pl.ds(pl.multiple_of(i * wide, wide), wide)
        query = query_t[:, lanes]
        grad = jnp.concatenate([grad_own[2 * i], grad_own[2 * i + 1]], axis=1)
        own = jnp.concatenate([mixed_own[2 * i], mixed_own[2 * i + 1]], axis=1)
        delta = jnp.sum(grad.astype(f32) * own.astype(f32), axis=0, keepdims=True)
        scores = matmul(keys[...], query, 1, 0) * scale
        probs = jnp.exp(scores - log_sum[:, lanes])
        grad_values[...] += matmul(probs.astype(bf16), grad, 1, 1)
        grad_probs = matmul(values[...], grad, 1, 0)
        grad_scores = (probs * (grad_probs - delta)).astype(bf16)
        grad_keys[...] += matmul(grad_scores, query, 1, 1)
        grad_query = matmul(keys_t[...], grad_scores, 1, 0) * scale
        back_query = grad_query * cos[:, lanes] + turn_back(grad_query * sine[:, lanes])
        grad_packed[:head, lanes] = back_query.astype(bf16)

    @pl.loop(0, count // 2)
    def _(i):
        back(i)

    @pl.loop(0, p.line)
    def _(step):
        settle_out.pass_on(p.far(step))

    swap.wait_recv()
    proj_part[...] = (pair_part[p.pair].astype(f32) + pair_got[...].astype(f32)).astype(bf16)
    grad_key = grad_keys[...].T * scale
    grad_packed[head : 2 * head, :] = (grad_key * cos[...] + turn_back(grad_key * sine[...])).astype(bf16)
    grad_packed[2 * head :, :] = grad_values[...].T.astype(bf16)

    @pl.loop(0, p.line)
    def _(step):
        z = p.far(step)
        for at in range(4):
            lanes = pl.ds(pl.multiple_of((z * 4 + at) * rows, rows), rows)
            grad_part[z * 4 + at] = matmul(grad_packed[:, lanes], weight[...], 0, 0).astype(bf16)
        halve.beside(z, 0).start()
        halve.beside(z, 1).start()

    @pl.loop(0, p.line)
    def _(step):
        z = p.far(step)
        halve_proj.beside(z, 0).start()
        halve_proj.beside(z, 1).start()
        halve.add(z)
        settle.across(z).start()

    def grad_chunk(step):
        lanes = pl.ds(pl.multiple_of(step * 4 * rows, 4 * rows), 4 * rows)
        acts = jnp.concatenate([act_all[4 * step + i] for i in range(4)], axis=0)
        return matmul(grad_packed[:, lanes], acts, 1, 0)

    grad_weight[...] = grad_chunk(0)

    @pl.loop(1, p.line)
    def _(step):
        grad_weight[...] += grad_chunk(step)

    for at in range(6):
        qkv_part[at] = grad_weight[at * unit : (at + 1) * unit, :].astype(bf16)
    gain_row = jnp.sum(grad_weight[...] * weight[...].astype(f32), axis=0, keepdims=True) / gain[...]
    gain_part[...] = jnp.broadcast_to(gain_row, (128, width)).T.astype(bf16).reshape(gain_part.shape)

    def unit_of(at):
        return (at // 2) * 2 * count + 2 * p.me + at % 2

    for at in range(6):
        give_qkv.send(at, unit_of(at) // 3, unit_of(at) % 3 * 2 + p.pair)
    spread_gain.send()

    @pl.loop(0, p.line)
    def _(step):
        z = p.far(step)
        halve_proj.add(z)
        settle_proj.across(z).start()

    @pl.loop(0, p.line)
    def _(step):
        z = p.far(step)
        settle.pass_on(z)
        settle_proj.pass_on(z)

    for side in range(2):
        give_in.arrived(side, p.owner % count * 2 + side)
    in_out[...] = in_got[0].astype(f32) + in_got[1].astype(f32)
    spread_down.arrived()
    units = in_out.shape[0]
    gain_m = jnp.zeros((unit, down_got.shape[2]), f32)
    for at in range(count):
        block = down_got[2 * at].astype(f32) + down_got[2 * at + 1].astype(f32)
        down_out[:, at * units : (at + 1) * units] = block[:, :units]
        gain_m += block
    gain_m_out[...] = gain_m[:, units : units + 1]
    settle_out.finish(out_total)
    for slot in range(3):
        source = (3 * p.owner + slot) % (2 * count) // 2 * 2
        for side in range(2):
            give_qkv.arrived(2 * slot + side, source + side)
        qkv_out[slot * unit : (slot + 1) * unit, :] = qkv_got[2 * slot].astype(f32) + qkv_got[2 * slot + 1].astype(f32)
    spread_gain.arrived()
    gain_a = jnp.zeros(gain_got.shape[1:], f32)
    for at in range(2 * count):
        gain_a += gain_got[at].astype(f32)
    gain_a_out[...] = gain_a[:, :1]
    settle_proj.finish(out_out)
    settle.finish(grad_act)
    trade.sent()
    halve.sent()
    settle.sent()
    settle_out.sent()
    halve_proj.sent()
    settle_proj.sent()
    spread_down.sent()
    spread_gain.sent()
    swap.wait_send()
    for part in range(2):
        give_in.sent(part, part * count + p.me, p.pair)
    for at in range(6):
        give_qkv.sent(at, unit_of(at) // 3, unit_of(at) % 3 * 2 + p.pair)


def run_kernel(body, outs, scratch, collective, flops, args, outside=()):
    vmem, anywhere = pl.BlockSpec(memory_space=pltpu.VMEM), pl.BlockSpec(memory_space=pl.ANY)
    return pl.pallas_call(
        body,
        out_shape=outs,
        in_specs=[anywhere if i in outside else vmem for i in range(len(args))],
        out_specs=[vmem] * len(outs),
        scratch_shapes=scratch,
        compiler_params=pltpu.CompilerParams(
            collective_id=collective, has_side_effects=True, vmem_limit_bytes=VMEM_LIMIT
        ),
        cost_estimate=pl.CostEstimate(flops=flops, bytes_accessed=20_000_000, transcendentals=0),
        name=body.func.__name__,
    )(*args)


def shaped(shape, kind):
    return jax.ShapeDtypeStruct(shape, kind)


def attend(count, head, act, cot, qkv_weight, in_mine, down_mine, out_mine, cos, sine):
    bf16, f32 = jnp.bfloat16, jnp.float32
    rows, width = act.shape
    length, line = rows * count, count // 4
    blocks = shaped((count, rows, width), bf16)
    tall, flat = shaped((head, length), bf16), shaped((length, head), bf16)
    heads = shaped((count, head, rows), bf16)
    pairs = [shaped((2,) + part.shape, bf16) for part in (in_mine, down_mine, out_mine)]
    three = pltpu.SemaphoreType.DMA((3,))
    return run_kernel(
        functools.partial(attend_kernel, count),
        [blocks, blocks, tall, tall, flat, flat, heads, shaped((1, length), f32), heads, shaped((3, head, width), bf16)]
        + pairs,
        [pltpu.VMEM((head, length), bf16), pltpu.SemaphoreType.DMA((8,))] + [three] * 4
        + Gather.sems(line) * 2 + Exchange.sems(count),
        0, 10_000_000_000, [act, cot, qkv_weight, in_mine, down_mine, out_mine, cos, sine], (2, 5),
    )


def feed(count, group, act, cot_all, in_pair, down_pair, gain):
    bf16, f32 = jnp.bfloat16, jnp.float32
    rows, width = act.shape
    length, line = rows * count, count // 4
    block = (rows, width)
    whole, half = pltpu.VMEM((count,) + block, bf16), pltpu.VMEM((2 * line,) + block, bf16)
    return run_kernel(
        functools.partial(feed_kernel, count),
        [shaped(block, f32), shaped((2 * line,) + block, bf16), shaped(in_pair.shape, bf16),
         shaped((2 * count, width // (2 * count), group), bf16)],
        [pltpu.VMEM((2 * group, width), bf16), pltpu.VMEM((width, group), bf16),
         pltpu.VMEM((2 * group, width), f32), pltpu.VMEM((width, group), f32),
         whole, pltpu.VMEM((length, group), bf16), pltpu.VMEM((length, 2 * group), bf16), whole, whole,
         half, half, half, pltpu.SemaphoreType.DMA]
        + Settle.bufs(line, block)
        + Gather.sems(line) + Halve.sems(line) + Settle.sems(line) + Halve.sems(line),
        1, 20_000_000_000, [act, cot_all, in_pair, down_pair, gain],
    )


def attend_back(count, grad_mixed, grad_mid, mixed, out_sums, kept, act_all, weight, cos, sine, in_grad, down_grad, gain):
    bf16, f32 = jnp.bfloat16, jnp.float32
    rows, width = act_all.shape[1:]
    head, length, line = weight.shape[0] // 3, rows * count, count // 4
    block, unit, units = (rows, width), head // 2, in_grad.shape[1]
    piece = (unit, width)

    def held(*shape):
        return pltpu.VMEM(shape, bf16)

    whole, half = held(count, *block), held(2 * line, *block)
    flat = pltpu.VMEM((length, head), f32)
    two, six, one = pltpu.SemaphoreType.DMA((2,)), pltpu.SemaphoreType.DMA((6,)), pltpu.SemaphoreType.DMA
    return run_kernel(
        functools.partial(attend_back_kernel, count),
        [shaped(block, f32), shaped(block, f32), shaped((3 * unit, width), f32), shaped(piece, f32),
         shaped((units, width), f32), shaped((unit, units * count), f32), shaped((unit, 1), f32), shaped((unit, 1), f32)],
        [held(count, head, rows), flat, flat, held(3 * head, length), whole, half, half,
         pltpu.VMEM((3 * head, width), f32),
         held(2, count, *piece), held(count, *piece), held(count, *piece), held(2 * line, *piece), held(2 * line, *piece),
         held(*in_grad.shape), held(*down_grad.shape), held(6, *piece), held(6, *piece),
         held(2 * count, unit, 128), held(2 * count, unit, 128),
         one, one, two, two, six, six]
        + Settle.bufs(line, block) * 2 + Settle.bufs(line, piece)
        + Exchange.sems(count) + Halve.sems(line) + Settle.sems(line) * 2
        + Halve.sems(line) + Settle.sems(line) + Spread.sems(count) * 2,
        2, 20_000_000_000,
        [grad_mixed, grad_mid, mixed, out_sums, *kept, act_all, weight, cos, sine, in_grad, down_grad, gain],
    )


def tensor_layer(
    tokens, cotangent, gain_attn, gain_mlp, qkv_weight, out_weight, in_weight, down_weight
):
    f32 = jnp.float32
    bf16 = jnp.bfloat16
    count = lax.axis_size("ctx")
    index = lax.axis_index("ctx")
    rows, width = tokens.shape[1], tokens.shape[2]
    length = rows * count
    head_size = width // count
    group = in_weight.shape[0] // count
    padded = (group // 128 + 1) * 128

    in_mine = lax.dynamic_slice_in_dim(in_weight, index * group, group, 0)
    down_mine = lax.dynamic_slice_in_dim(down_weight, index * group, group, 1)

    cos_table, sine_table = rope_tables(0, length, head_size)
    cos_table, sine_table = cos_table[:, 0].T, sine_table[:, 0].T
    resid = tokens[0].astype(f32)
    normed_a, inv_a = normalize(resid)
    act_a = (normed_a * gain_attn).astype(bf16)
    cot_rows = cotangent[0]
    act_all, cot_all, *kept, mixed, qkv_head, in_pair, down_pair, out_pair = attend(
        count, head_size, act_a, cot_rows, qkv_weight, in_mine, down_mine, out_weight, cos_table, sine_table
    )
    qkv_head = qkv_head.reshape(3 * head_size, width)
    out_full = out_pair.reshape(width, width)
    middle = resid + matmul(mixed.reshape(width, rows), out_full, 0, 1)
    normed_m, inv_m = normalize(middle)
    act_m = (normed_m * gain_mlp).astype(bf16)
    grad_act_m, out_sums, in_grad, down_grad = feed(count, padded, act_m, cot_all, in_pair, down_pair, gain_mlp[None])

    grad_middle = cot_rows.astype(f32) + norm_back(grad_act_m * gain_mlp, normed_m, inv_m)
    grad_mid_bf = grad_middle.astype(bf16)
    grad_mixed = matmul(out_full, grad_mid_bf, 0, 1).astype(bf16).reshape(count, head_size, rows)
    grad_act_a, out_total, grad_qkv, grad_out, grad_in, grad_down, grad_gain_m, grad_gain_a = attend_back(
        count, grad_mixed, grad_mid_bf, mixed, out_sums, kept, act_all, qkv_head, cos_table, sine_table,
        in_grad, down_grad, gain_attn[None],
    )
    output = middle + out_total
    grad_input = grad_middle + norm_back(grad_act_a * gain_attn, normed_a, inv_a)
    return (
        output[None], grad_input[None], grad_qkv, grad_out, grad_in, grad_down,
        grad_gain_a.reshape(-1), grad_gain_m.reshape(-1),
    )


def solution(mesh):

    def layer(*arrays):
        one_head_each = arrays[0].shape[2] == HEAD_DIM * mesh.shape["ctx"]
        if one_head_each and mesh.shape["fsdp"] == 2 and mesh.shape["ctx"] % 4 == 0:
            return tensor_layer(*arrays)
        return gathered_layer(*arrays)

    return jax.shard_map(
        layer,
        mesh=mesh,
        in_specs=(
            P("fsdp", "ctx", None),
            P("fsdp", "ctx", None),
            P(),
            P(),
            P("fsdp", None),
            P("fsdp", None),
            P("fsdp", None),
            P("fsdp", None),
        ),
        out_specs=(
            P("fsdp", "ctx", None),
            P("fsdp", "ctx", None),
            P(("ctx", "fsdp"), None),
            P(("ctx", "fsdp"), None),
            P(("ctx", "fsdp"), None),
            P(("ctx", "fsdp"), None),
            P(("ctx", "fsdp")),
            P(("ctx", "fsdp")),
        ),
        check_vma=False,
    )
```

```python
import functools
import math

import jax
import jax.numpy as jnp
from jax import lax
from jax.experimental import pallas as pl
from jax.experimental.pallas import tpu as pltpu
from jax.sharding import PartitionSpec as P

HEAD_DIM = 64


EPSILON = 1e-05
ROPE_BASE = 160000.0


def normalize(tensor):
    centred = tensor - jnp.mean(tensor, axis=-1, keepdims=True)
    inv_std = lax.rsqrt(jnp.mean(centred * centred, axis=-1, keepdims=True) + EPSILON)
    return (centred * inv_std, inv_std)


def norm_back(grad_norm, normed, inv_std):
    return inv_std * (
        grad_norm
        - jnp.mean(grad_norm, axis=-1, keepdims=True)
        - normed * jnp.mean(grad_norm * normed, axis=-1, keepdims=True)
    )


def gelu_pair(tensor):
    cumul = 0.5 * (1.0 + jax.scipy.special.erf(tensor * 0.7071067811865476))
    density = jnp.exp(-0.5 * tensor * tensor) * 0.3989422804014327
    return (tensor * cumul, cumul + tensor * density)


def rope_tables(offset, length, head_size):
    positions = (offset + jnp.arange(length, dtype=jnp.int32)).astype(jnp.float32)
    inverse = ROPE_BASE ** (
        -jnp.arange(0, head_size, 2, dtype=jnp.int32).astype(jnp.float32) / head_size
    )
    angles = positions[:, None] * inverse[None, :]
    angles = jnp.concatenate([angles, angles], axis=-1)
    return (jnp.cos(angles)[:, None, :], jnp.sin(angles)[:, None, :])


def rotate(tensor, cos_table, sine_table):
    middle = tensor.shape[-1] // 2
    turned = jnp.concatenate([-tensor[..., middle:], tensor[..., :middle]], axis=-1)
    return tensor * cos_table + turned * sine_table


def rotate_back(gradient, cos_table, sine_table):
    middle = gradient.shape[-1] // 2
    scaled = gradient * sine_table
    turned = jnp.concatenate([scaled[..., middle:], -scaled[..., :middle]], axis=-1)
    return gradient * cos_table + turned


def rows_product(left, right):
    return lax.dot_general(
        left, right, (((1,), (1,)), ((), ())), preferred_element_type=jnp.float32
    )


def rows_contract(left, right):
    return lax.dot_general(
        left, right, (((0,), (0,)), ((), ())), preferred_element_type=jnp.float32
    )


def gathered_layer(
    tokens, cotangent, gain_attn, gain_mlp, qkv_weight, out_weight, in_weight, down_weight
):
    f32 = jnp.float32
    bf16 = jnp.bfloat16
    qkv_full, out_full, in_full, down_full = (
        lax.all_gather(qkv_weight, "fsdp", axis=0, tiled=True),
        lax.all_gather(out_weight, "fsdp", axis=0, tiled=True),
        lax.all_gather(in_weight, "fsdp", axis=0, tiled=True),
        lax.all_gather(down_weight, "fsdp", axis=0, tiled=True),
    )
    tok_rows = tokens.shape[1]
    width = tokens.shape[2]
    hidden = down_full.shape[1]
    head_size = HEAD_DIM
    head_count = width // head_size
    scale = head_size ** (-0.5)
    offset = lax.axis_index("ctx") * tok_rows
    cos_table, sine_table = rope_tables(offset, tok_rows, head_size)
    resid = tokens[0].astype(f32)
    normed_a, inv_a = normalize(resid)
    act_a = (normed_a * gain_attn).astype(bf16)
    packed = rows_product(act_a, qkv_full)
    query_heads = rotate(
        packed[:, :width].reshape(tok_rows, head_count, head_size), cos_table, sine_table
    ).astype(bf16)
    key_heads = rotate(
        packed[:, width : 2 * width].reshape(tok_rows, head_count, head_size), cos_table, sine_table
    ).astype(bf16)
    value_send = packed[:, 2 * width :].astype(bf16)
    key_send = key_heads.reshape(tok_rows, width)
    value_heads = value_send.reshape(tok_rows, head_count, head_size)
    start_state = (
        jnp.zeros((tok_rows, head_count, head_size), f32),
        jnp.full((head_count, tok_rows), -1e30, f32),
        jnp.zeros((head_count, tok_rows), f32),
    )
    key_piece = lax.all_gather(key_send, "ctx", axis=0, tiled=True)
    value_piece = lax.all_gather(value_send, "ctx", axis=0, tiled=True)
    length = key_piece.shape[0]
    step_len = math.gcd(length, 1024)

    def attend_block(block_num, running):
        weighted, row_max, row_sum = running
        key_blk = lax.dynamic_slice_in_dim(key_piece, block_num * step_len, step_len, 0).reshape(
            step_len, head_count, head_size
        )
        value_blk = lax.dynamic_slice_in_dim(
            value_piece, block_num * step_len, step_len, 0
        ).reshape(step_len, head_count, head_size)
        scores = (
            jnp.einsum("qhd,khd->hqk", query_heads, key_blk, preferred_element_type=f32) * scale
        )
        new_max = jnp.maximum(row_max, jnp.max(scores, axis=-1))
        shrink = jnp.exp(row_max - new_max)
        weights = jnp.exp(scores - new_max[..., None])
        row_sum = row_sum * shrink + jnp.sum(weights, axis=-1)
        weighted = weighted * shrink.T[:, :, None] + jnp.einsum(
            "hqk,khd->qhd", weights.astype(bf16), value_blk, preferred_element_type=f32
        )
        return (weighted, new_max, row_sum)

    weighted, row_max, row_sum = lax.fori_loop(0, length // step_len, attend_block, start_state)
    log_sum = row_max + jnp.log(row_sum)
    mixed = (weighted / row_sum.T[:, :, None]).reshape(tok_rows, width).astype(bf16)
    middle = resid + rows_product(mixed, out_full)
    normed_m, inv_m = normalize(middle)
    act_m = (normed_m * gain_mlp).astype(bf16)
    inner = rows_product(act_m, in_full)
    gelu_val, gelu_slope = gelu_pair(inner[:, :hidden])
    gated = (gelu_val * inner[:, hidden:]).astype(bf16)
    output = middle + rows_product(gated, down_full)
    cot_rows = cotangent[0]
    grad_down = rows_contract(cot_rows, gated)
    grad_gated = jnp.dot(cot_rows, down_full, preferred_element_type=f32)
    grad_inner = jnp.concatenate(
        [grad_gated * inner[:, hidden:] * gelu_slope, grad_gated * gelu_val], axis=1
    ).astype(bf16)
    grad_in = rows_contract(grad_inner, act_m)
    grad_act_m = jnp.dot(grad_inner, in_full, preferred_element_type=f32)
    grad_gain_m = jnp.sum(grad_act_m * normed_m, axis=0)
    grad_middle = cot_rows.astype(f32) + norm_back(grad_act_m * gain_mlp, normed_m, inv_m)
    grad_mid_bf = grad_middle.astype(bf16)
    grad_out = rows_contract(grad_mid_bf, mixed)
    grad_mixed = jnp.dot(grad_mid_bf, out_full, preferred_element_type=f32).astype(bf16)
    grad_heads = grad_mixed.reshape(tok_rows, head_count, head_size)
    delta_rows = jnp.sum(
        grad_heads.astype(f32) * mixed.reshape(tok_rows, head_count, head_size).astype(f32), axis=-1
    )
    delta = delta_rows.T
    zeros_heads = jnp.zeros((tok_rows, head_count, head_size), f32)
    query_key_piece = lax.all_gather(key_send, "ctx", axis=0, tiled=True)
    query_value_piece = lax.all_gather(value_send, "ctx", axis=0, tiled=True)
    length = query_key_piece.shape[0]
    query_step_len = math.gcd(length, 1024)

    def query_grad_block(block_num, grad_query):
        key_blk = lax.dynamic_slice_in_dim(
            query_key_piece, block_num * query_step_len, query_step_len, 0
        ).reshape(query_step_len, head_count, head_size)
        value_blk = lax.dynamic_slice_in_dim(
            query_value_piece, block_num * query_step_len, query_step_len, 0
        ).reshape(query_step_len, head_count, head_size)
        scores = (
            jnp.einsum("qhd,khd->hqk", query_heads, key_blk, preferred_element_type=f32) * scale
        )
        probs = jnp.exp(scores - log_sum[..., None])
        grad_probs = jnp.einsum("qhd,khd->hqk", grad_heads, value_blk, preferred_element_type=f32)
        grad_scores = (probs * (grad_probs - delta[..., None])).astype(bf16)
        return (
            grad_query
            + jnp.einsum("hqk,khd->qhd", grad_scores, key_blk, preferred_element_type=f32) * scale
        )

    grad_query = lax.fori_loop(0, length // query_step_len, query_grad_block, zeros_heads)
    query_send = query_heads.reshape(tok_rows, width).astype(f32)
    grad_send = grad_mixed.astype(f32)
    query_piece = lax.all_gather(query_send, "ctx", axis=0, tiled=True)
    grad_piece = lax.all_gather(grad_send, "ctx", axis=0, tiled=True)
    log_piece = lax.all_gather(log_sum.T, "ctx", axis=0, tiled=True)
    delta_piece = lax.all_gather(delta_rows, "ctx", axis=0, tiled=True)
    length = query_piece.shape[0]
    key_step_len = math.gcd(length, 1024)

    def key_grad_block(block_num, running):
        grad_keys, grad_values = running
        query_blk = (
            lax.dynamic_slice_in_dim(query_piece, block_num * key_step_len, key_step_len, 0)
            .astype(bf16)
            .reshape(key_step_len, head_count, head_size)
        )
        grad_blk = (
            lax.dynamic_slice_in_dim(grad_piece, block_num * key_step_len, key_step_len, 0)
            .astype(bf16)
            .reshape(key_step_len, head_count, head_size)
        )
        log_blk = lax.dynamic_slice_in_dim(log_piece, block_num * key_step_len, key_step_len, 0).T
        delta_blk = lax.dynamic_slice_in_dim(
            delta_piece, block_num * key_step_len, key_step_len, 0
        ).T
        scores = (
            jnp.einsum("qhd,khd->hqk", query_blk, key_heads, preferred_element_type=f32) * scale
        )
        probs = jnp.exp(scores - log_blk[..., None])
        grad_values = grad_values + jnp.einsum(
            "hqk,qhd->khd", probs.astype(bf16), grad_blk, preferred_element_type=f32
        )
        grad_probs = jnp.einsum("qhd,khd->hqk", grad_blk, value_heads, preferred_element_type=f32)
        grad_scores = (probs * (grad_probs - delta_blk[..., None])).astype(bf16)
        grad_keys = (
            grad_keys
            + jnp.einsum("hqk,qhd->khd", grad_scores, query_blk, preferred_element_type=f32) * scale
        )
        return (grad_keys, grad_values)

    grad_keys, grad_values = lax.fori_loop(
        0, length // key_step_len, key_grad_block, (zeros_heads, zeros_heads)
    )
    grad_query = rotate_back(grad_query, cos_table, sine_table)
    grad_keys = rotate_back(grad_keys, cos_table, sine_table)
    grad_packed = jnp.concatenate(
        [
            grad_query.reshape(tok_rows, width),
            grad_keys.reshape(tok_rows, width),
            grad_values.reshape(tok_rows, width),
        ],
        axis=1,
    ).astype(bf16)
    grad_qkv = rows_contract(grad_packed, act_a)
    grad_act_a = jnp.dot(grad_packed, qkv_full, preferred_element_type=f32)
    grad_gain_a = jnp.sum(grad_act_a * normed_a, axis=0)
    grad_input = grad_middle + norm_back(grad_act_a * gain_attn, normed_a, inv_a)
    owned = (
        lax.psum_scatter(grad_qkv, ("ctx", "fsdp"), scatter_dimension=0, tiled=True),
        lax.psum_scatter(grad_out, ("ctx", "fsdp"), scatter_dimension=0, tiled=True),
        lax.psum_scatter(grad_in, ("ctx", "fsdp"), scatter_dimension=0, tiled=True),
        lax.psum_scatter(grad_down, ("ctx", "fsdp"), scatter_dimension=0, tiled=True),
        lax.psum_scatter(grad_gain_a, ("ctx", "fsdp"), scatter_dimension=0, tiled=True),
        lax.psum_scatter(grad_gain_m, ("ctx", "fsdp"), scatter_dimension=0, tiled=True),
    )
    return (
        output[None],
        grad_input[None],
        owned[0],
        owned[1],
        owned[2],
        owned[3],
        owned[4],
        owned[5],
    )


MESH = pl.DeviceIdType.MESH
VMEM_LIMIT = 60 * 1024 * 1024


def matmul(left, right, left_dim, right_dim):
    return lax.dot_general(
        left, right, (((left_dim,), (right_dim,)), ((), ())), preferred_element_type=jnp.float32
    )


class Place:
    def __init__(self, count):
        self.count, self.line = count, count // 4
        self.me, self.pair = lax.axis_index("ctx"), lax.axis_index("fsdp")
        self.owner = self.me * 2 + self.pair
        self.z, self.x, self.core = self.me // 4, self.me // 2 % 2, self.me % 2

    def slot(self, z, x, core):
        return z * 4 + x * 2 + core

    def far(self, step):
        last = self.line - 1
        low = 2 * self.z < self.line
        own = jnp.where(low, self.z, last - self.z)
        at = jnp.where(
            step < last - own, last - step, jnp.where(step == last, own, step - (last - own))
        )
        return jnp.where(low, at, last - at)

    def near(self, step):
        return self.far(self.line - 1 - step)

    def meet(self, everyone=False):
        barrier = pltpu.get_barrier_semaphore()

        @pl.loop(1, self.count)
        def _(shift):
            pl.semaphore_signal(
                barrier, inc=1, device_id={"ctx": (self.me + shift) % self.count}, device_id_type=MESH
            )

        if everyone:
            @pl.loop(0, self.count)
            def _(to):
                pl.semaphore_signal(
                    barrier, inc=1, device_id={"ctx": to, "fsdp": 1 - self.pair}, device_id_type=MESH
                )

            pl.semaphore_wait(barrier, 2 * self.count - 1)
        else:
            pl.semaphore_signal(barrier, inc=1, device_id={"fsdp": 1 - self.pair}, device_id_type=MESH)
            pl.semaphore_wait(barrier, self.count)

    def over_pair(self, src, dst, send, recv):
        return pltpu.make_async_remote_copy(
            src_ref=src, dst_ref=dst, send_sem=send, recv_sem=recv,
            device_id={"fsdp": 1 - self.pair}, device_id_type=MESH,
        )

    def to_owner(self, src, dst, send, recv, owner):
        return pltpu.make_async_remote_copy(
            src_ref=src, dst_ref=dst, send_sem=send, recv_sem=recv,
            device_id={"ctx": owner // 2, "fsdp": owner % 2}, device_id_type=MESH,
        )

    def copy(self, src, dst, send, recv, to):
        return pltpu.make_async_remote_copy(
            src_ref=src, dst_ref=dst, send_sem=send, recv_sem=recv,
            device_id={"ctx": to}, device_id_type=MESH,
        )


class Gather:
    def __init__(self, place, buf, sems):
        self.p, self.buf = place, buf
        self.up_s, self.up_r, self.dn_s, self.dn_r, self.x_s, self.x_r, self.c_s, self.c_r = sems

    @staticmethod
    def sems(line):
        return [pltpu.SemaphoreType.DMA((line,))] * 6 + [pltpu.SemaphoreType.DMA((2 * line,))] * 2

    def over(self, z, x, core, send, recv, to):
        at = self.buf.at[self.p.slot(z, x, core)]
        return self.p.copy(at, at, send, recv, to)

    def up(self, z):
        p = self.p
        return self.over(z, p.x, p.core, self.up_s.at[z], self.up_r.at[z], (p.me + 4) % p.count)

    def down(self, z):
        p = self.p
        return self.over(z, p.x, p.core, self.dn_s.at[z], self.dn_r.at[z], (p.me + p.count - 4) % p.count)

    def across(self, z):
        p = self.p
        return self.over(z, p.x, p.core, self.x_s.at[z], self.x_r.at[z], p.slot(p.z, 1 - p.x, p.core))

    def beside(self, z, x):
        p = self.p
        at = z * 2 + x
        return self.over(z, x, p.core, self.c_s.at[at], self.c_r.at[at], p.slot(p.z, p.x, 1 - p.core))

    def arrive(self, z):
        p = self.p

        @pl.when(z < p.z)
        def _():
            self.up(z).wait_recv()

        @pl.when(z > p.z)
        def _():
            self.down(z).wait_recv()

        @pl.when((z <= p.z) & (p.z < p.line - 1))
        def _():
            self.up(z).start()

        @pl.when((z >= p.z) & (p.z > 0))
        def _():
            self.down(z).start()

        self.across(z).start()
        self.beside(z, p.x).start()

    def arrive_across(self, z):
        self.across(z).wait_recv()
        self.beside(z, 1 - self.p.x).start()

    def part(self, turn, use=None):
        p = self.p
        step, part = turn // 4, turn % 4
        z = jnp.where(part == 0, p.near(step), p.near(step - 1))

        @pl.when(jnp.where(part == 0, step < p.line, step > 0))
        def _():
            @pl.when(part == 0)
            def _():
                self.arrive(z)

            @pl.when(part == 1)
            def _():
                self.arrive_across(z)

            x = jnp.where(part % 2 == 0, p.x, 1 - p.x)

            @pl.when(part >= 2)
            def _():
                self.beside(z, x).wait_recv()

            if use is not None:
                use(z, x, jnp.where(part < 2, p.core, 1 - p.core))

    def sent(self):
        p = self.p

        @pl.loop(0, p.line)
        def _(z):
            @pl.when((z <= p.z) & (p.z < p.line - 1))
            def _():
                self.up(z).wait_send()

            @pl.when((z >= p.z) & (p.z > 0))
            def _():
                self.down(z).wait_send()

            self.across(z).wait_send()
            self.beside(z, 0).wait_send()
            self.beside(z, 1).wait_send()


class Halve:
    def __init__(self, place, whole, got, sums, sems):
        self.p, self.whole, self.got, self.sums = place, whole, got, sums
        self.c_s, self.c_r = sems

    @staticmethod
    def sems(line):
        return [pltpu.SemaphoreType.DMA((2 * line,))] * 2

    def beside(self, z, x):
        p, at = self.p, z * 2 + x
        return p.copy(
            self.whole.at[p.slot(z, x, 1 - p.core)], self.got.at[at], self.c_s.at[at], self.c_r.at[at],
            p.slot(p.z, p.x, 1 - p.core),
        )

    def add(self, z):
        p = self.p
        for x in range(2):
            at = z * 2 + x
            self.beside(z, x).wait_recv()
            self.sums[at] = (
                self.whole[p.slot(z, x, p.core)].astype(jnp.float32) + self.got[at].astype(jnp.float32)
            ).astype(self.sums.dtype)

    def sent(self):
        @pl.loop(0, 2 * self.p.line)
        def _(at):
            self.beside(at // 2, at % 2).wait_send()


class Quad:
    def __init__(self, place, buf, sems):
        self.p, self.buf = place, buf
        self.s, self.r = sems

    @staticmethod
    def sems():
        return [pltpu.SemaphoreType.DMA((3,))] * 2

    def over(self, x, to, at):
        piece = self.buf.at[x * 2 + self.p.core]
        return self.p.copy(piece, piece, self.s.at[at], self.r.at[at], to)

    def across(self):
        p = self.p
        return self.over(p.x, p.slot(p.z, 1 - p.x, p.core), 0)

    def beside(self):
        p = self.p
        return self.over(p.x, p.slot(p.z, p.x, 1 - p.core), 1)

    def beside_next(self):
        p = self.p
        return self.over(1 - p.x, p.slot(p.z, p.x, 1 - p.core), 2)

    def start(self):
        self.across().start()
        self.beside().start()

    def relay(self):
        self.across().wait_recv()
        self.beside_next().start()

    def sent(self):
        self.across().wait_send()
        self.beside().wait_send()
        self.beside_next().wait_send()


class QuadSum:
    def __init__(self, place, whole, bufs, sems):
        self.p, self.whole = place, whole
        self.got, self.sums, self.far = bufs
        self.s, self.r = sems

    @staticmethod
    def sems():
        return [pltpu.SemaphoreType.DMA((3,))] * 2

    @staticmethod
    def bufs(block):
        return [pltpu.VMEM((2,) + block, jnp.bfloat16)] * 2 + [pltpu.VMEM(block, jnp.bfloat16)]

    def beside(self, x):
        p = self.p
        return p.copy(
            self.whole.at[x * 2 + 1 - p.core], self.got.at[x], self.s.at[x], self.r.at[x],
            p.slot(p.z, p.x, 1 - p.core),
        )

    def across(self):
        p = self.p
        return p.copy(
            self.sums.at[1 - p.x], self.far, self.s.at[2], self.r.at[2], p.slot(p.z, 1 - p.x, p.core)
        )

    def add(self, x):
        f32 = jnp.float32
        self.beside(x).wait_recv()
        self.sums[x] = (
            self.whole[x * 2 + self.p.core].astype(f32) + self.got[x].astype(f32)
        ).astype(self.sums.dtype)

    def finish(self, out):
        f32 = jnp.float32
        self.across().wait_recv()
        out[...] = self.sums[self.p.x].astype(f32) + self.far[...].astype(f32)

    def sent(self):
        self.beside(0).wait_send()
        self.beside(1).wait_send()
        self.across().wait_send()


class Settle:
    def __init__(self, place, sums, bufs, sems, pairwise=False):
        self.p, self.sums, self.pairwise = place, sums, pairwise
        self.got, self.total, self.low, self.high = bufs
        self.x_s, self.x_r, self.up_s, self.up_r, self.dn_s, self.dn_r = sems

    @staticmethod
    def sems(line):
        return [pltpu.SemaphoreType.DMA((line,))] * 6

    @staticmethod
    def bufs(line, block):
        return [pltpu.VMEM((line,) + block, jnp.bfloat16)] * 4

    def kept(self, z):
        p = self.p
        return p.pair * p.line + z if self.pairwise else z * 2 + p.x

    def across(self, z):
        p = self.p
        if self.pairwise:
            return p.over_pair(
                self.sums.at[(1 - p.pair) * p.line + z], self.got.at[z], self.x_s.at[z], self.x_r.at[z]
            )
        return p.copy(
            self.sums.at[z * 2 + 1 - p.x], self.got.at[z], self.x_s.at[z], self.x_r.at[z],
            p.slot(p.z, 1 - p.x, p.core),
        )

    def up(self, z):
        p = self.p
        return p.copy(self.total.at[z], self.low.at[z], self.up_s.at[z], self.up_r.at[z], (p.me + 4) % p.count)

    def down(self, z):
        p = self.p
        return p.copy(
            self.total.at[z], self.high.at[z], self.dn_s.at[z], self.dn_r.at[z], (p.me + p.count - 4) % p.count
        )

    def pass_on(self, z):
        p, f32 = self.p, jnp.float32
        self.across(z).wait_recv()
        self.total[z] = (
            self.sums[self.kept(z)].astype(f32) + self.got[z].astype(f32)
        ).astype(self.total.dtype)

        @pl.when(z > p.z)
        def _():
            @pl.when(p.z > 0)
            def _():
                self.up(z).wait_recv()
                self.total[z] = (self.total[z].astype(f32) + self.low[z].astype(f32)).astype(self.total.dtype)

            self.up(z).start()

        @pl.when(z < p.z)
        def _():
            @pl.when(p.z < p.line - 1)
            def _():
                self.down(z).wait_recv()
                self.total[z] = (self.total[z].astype(f32) + self.high[z].astype(f32)).astype(self.total.dtype)

            self.down(z).start()

    def finish(self, out):
        p, f32 = self.p, jnp.float32
        @pl.when(p.z > 0)
        def _():
            self.up(p.z).wait_recv()

        @pl.when(p.z < p.line - 1)
        def _():
            self.down(p.z).wait_recv()

        total = self.total[p.z].astype(f32)
        total += jnp.where(p.z > 0, self.low[p.z].astype(f32), 0.0)
        total += jnp.where(p.z < p.line - 1, self.high[p.z].astype(f32), 0.0)
        out[...] = total.astype(out.dtype)

    def sent(self):
        p = self.p

        @pl.loop(0, p.line)
        def _(z):
            self.across(z).wait_send()

            @pl.when(z > p.z)
            def _():
                self.up(z).wait_send()

            @pl.when(z < p.z)
            def _():
                self.down(z).wait_send()


class Exchange:
    def __init__(self, place, src, dst, sems):
        self.p, self.src, self.dst = place, src, dst
        self.s, self.r = sems

    @staticmethod
    def sems(count):
        return [pltpu.SemaphoreType.DMA((count,))] * 2

    def to(self, j):
        return self.p.copy(self.src.at[j], self.dst.at[self.p.me], self.s.at[j], self.r.at[self.p.me], j)

    def send(self, j):
        @pl.when(j != self.p.me)
        def _():
            self.to(j).start()

        @pl.when(j == self.p.me)
        def _():
            self.dst[j] = self.src[j]

    def arrived(self):
        p = self.p

        @pl.loop(1, p.count)
        def _(shift):
            j = (p.me + shift) % p.count
            p.copy(self.src.at[j], self.dst.at[j], self.s.at[j], self.r.at[j], j).wait_recv()

    def sent(self):
        p = self.p

        @pl.loop(1, p.count)
        def _(shift):
            self.to((p.me + shift) % p.count).wait_send()


class Spread:
    def __init__(self, place, src, dst, sems):
        self.p, self.src, self.dst = place, src, dst
        self.s, self.r = sems

    @staticmethod
    def sems(count):
        return [pltpu.SemaphoreType.DMA((2 * count,))] * 2

    def to(self, j):
        p = self.p
        return p.to_owner(self.src.at[j], self.dst.at[p.owner], self.s.at[j], self.r.at[p.owner], j)

    def send(self):
        p = self.p
        self.dst[p.owner] = self.src[p.owner]

        @pl.loop(1, 2 * p.count)
        def _(shift):
            self.to((p.owner + shift) % (2 * p.count)).start()

    def arrived(self):
        p = self.p

        @pl.loop(1, 2 * p.count)
        def _(shift):
            j = (p.owner + shift) % (2 * p.count)
            p.to_owner(self.src.at[j], self.dst.at[j], self.s.at[j], self.r.at[j], j).wait_recv()

    def sent(self):
        p = self.p

        @pl.loop(1, 2 * p.count)
        def _(shift):
            self.to((p.owner + shift) % (2 * p.count)).wait_send()


class Deliver:
    def __init__(self, place, src, dst, sems):
        self.p, self.src, self.dst = place, src, dst
        self.s, self.r = sems

    def away(self, piece, owner, slot):
        return self.p.to_owner(self.src.at[piece], self.dst.at[slot], self.s.at[piece], self.r.at[slot], owner)

    def send(self, piece, owner, slot):
        @pl.when(owner != self.p.owner)
        def _():
            self.away(piece, owner, slot).start()

        @pl.when(owner == self.p.owner)
        def _():
            self.dst[slot] = self.src[piece]

    def sent(self, piece, owner, slot):
        @pl.when(owner != self.p.owner)
        def _():
            self.away(piece, owner, slot).wait_send()

    def arrived(self, slot, source):
        p = self.p

        @pl.when(source != p.owner)
        def _():
            p.to_owner(self.src.at[0], self.dst.at[slot], self.s.at[0], self.r.at[slot], source).wait_recv()


def rotate_rows(value, cos, sine):
    half = value.shape[0] // 2
    first, second = value[:half], value[half:]
    return jnp.concatenate([first * cos - second * sine, second * cos + first * sine], axis=0)


def rotate_rows_back(grad, cos, sine):
    half = grad.shape[0] // 2
    first, second = grad[:half], grad[half:]
    return jnp.concatenate([first * cos + second * sine, second * cos - first * sine], axis=0)


def attend_kernel(
    count, act, cot, qkv_weight, in_weight, down_mine, out_mine, cos, sine,
    act_all, cot_all, query_t, keys_t, keys, values, mixed_own, log_sum, mixed, weight, in_other, down_other, out_pair,
    values_t, load_sem, part_sem, part_got, piece_sem, piece_got, *sems
):
    f32, bf16 = jnp.float32, jnp.bfloat16
    p = Place(count)
    rows, head = act.shape[0], keys_t.shape[0]
    width = count * head
    n = 8
    first = Gather(p, act_all, sems[:n])
    second = Quad(p, cot_all, sems[n : n + 2])
    trade = Exchange(p, mixed_own, mixed, sems[n + 2 :])
    half = out_mine.shape[0] // 2
    part_half = pl.ds(pl.multiple_of(p.core * half, half), half)
    loads = [(act, act_all.at[p.me]), (cot, cot_all.at[p.x * 2 + p.core]), (out_mine, out_pair.at[p.pair])]
    loads = [pltpu.make_async_copy(src, dst, load_sem.at[i]) for i, (src, dst) in enumerate(loads)]
    for load in loads:
        load.start()

    def part_rows(part):
        start = part * width + p.me * head
        holder = start // qkv_weight.shape[0]
        at = pl.ds(pl.multiple_of(start - holder * qkv_weight.shape[0], head), head)
        return holder == p.pair, qkv_weight.at[at]

    def part_copies(part):
        here, src = part_rows(part)
        return (
            here,
            pltpu.make_async_copy(src, weight.at[part], load_sem.at[3 + part]),
            p.over_pair(src, weight.at[part], part_sem.at[part], part_got.at[part]),
        )

    units, columns, down_rows = in_other.shape[0], in_other.shape[1] // 2, down_other.shape[0] // 2
    in_rows = pl.ds(pl.multiple_of((p.x * 2 + p.core) * units, 16), units)
    in_cols = pl.ds(pl.multiple_of(p.z % 2 * columns, columns), columns)
    down_part = pl.ds(pl.multiple_of(p.z % 2 * down_rows, down_rows), down_rows)
    in_here, down_here = in_other.at[:, in_cols], down_other.at[down_part]
    swaps = [
        p.over_pair(out_mine.at[part_half], out_pair.at[p.pair, part_half], piece_sem.at[0], piece_got.at[0]),
        p.over_pair(in_weight.at[in_rows, in_cols], in_here, piece_sem.at[1], piece_got.at[1]),
        p.over_pair(down_mine.at[down_part], down_here, piece_sem.at[2], piece_got.at[2]),
    ]
    next_z = p.me + 4 - p.z % 2 * 8
    in_share = p.copy(in_here, in_here, piece_sem.at[4], piece_got.at[4], next_z)
    down_share = p.copy(down_here, down_here, piece_sem.at[5], piece_got.at[5], next_z)
    out_rest = out_pair.at[1 - p.pair, part_half]
    share = p.copy(out_rest, out_rest, piece_sem.at[3], piece_got.at[3], p.slot(p.z, p.x, 1 - p.core))
    for part in range(3):
        here, own, away = part_copies(part)

        @pl.when(here)
        def _():
            own.start()

    p.meet()
    for part in range(3):
        here, own, away = part_copies(part)

        @pl.when(here)
        def _():
            away.start()

    for swap in swaps:
        swap.start()
    for load in loads:
        load.wait()

    first.part(0)
    for part in range(3):
        here, own, away = part_copies(part)

        @pl.when(here)
        def _():
            own.wait()

        @pl.when(jnp.logical_not(here))
        def _():
            away.wait_recv()

    head_weight = weight[...].reshape(3 * head, act.shape[1])

    def project(z, x, core):
        at = p.slot(z, x, core)
        lanes = pl.ds(pl.multiple_of(at * rows, rows), rows)
        packed = matmul(head_weight, act_all[at], 1, 1)
        c, s = cos[:, lanes], sine[:, lanes]
        query, key = packed[:head], packed[head : 2 * head]
        query_t[:, lanes] = rotate_rows(query, c, s).astype(bf16)
        key = rotate_rows(key, c, s)
        keys_t[:, lanes] = key.astype(bf16)
        values_t[:, lanes] = packed[2 * head :].astype(bf16)
        keys[lanes, :] = key.T.astype(bf16)
        values[lanes, :] = packed[2 * head :].T.astype(bf16)

    project(p.z, p.x, p.core)

    @pl.loop(4, 4 * p.line + 4)
    def _(at):
        first.part(at, project)

    second.start()
    wide = 2 * rows
    blocks = count // 2
    scale = head ** (-0.5)

    def attend(i):
        block = (p.me // 2 + i) % blocks
        lanes = pl.ds(pl.multiple_of(block * wide, wide), wide)
        scores = matmul(keys[...], query_t[:, lanes], 1, 0) * scale
        top = jnp.max(scores, axis=0, keepdims=True)
        weights = jnp.exp(scores - top)
        total = jnp.sum(weights, axis=0, keepdims=True)
        log_sum[:, lanes] = top + jnp.log(total)
        out = (matmul(values_t[...], weights.astype(bf16), 1, 0) / total).astype(bf16)
        mixed_own[2 * block] = out[:, :rows]
        mixed_own[2 * block + 1] = out[:, rows:]
        trade.send(2 * block)
        trade.send(2 * block + 1)

    @pl.loop(0, blocks // 2)
    def _(i):
        attend(i)

    second.relay()
    swaps[0].wait_recv()
    share.start()

    @pl.loop(blocks // 2, blocks)
    def _(i):
        attend(i)

    swaps[1].wait_recv()
    in_share.start()
    trade.arrived()
    second.beside().wait_recv()
    second.beside_next().wait_recv()
    swaps[2].wait_recv()
    down_share.start()
    first.sent()
    second.sent()
    trade.sent()
    for part in range(3):
        here, own, away = part_copies(part)

        @pl.when(here)
        def _():
            away.wait_send()

    for swap in swaps:
        swap.wait_send()
    share.wait()
    in_share.wait()
    down_share.wait()


def feed_kernel(
    count, act, cot_all, in_weight, in_other, down_mine, down_other, gain,
    grad_act, out_total, in_grad, down_grad,
    weight, down, act_all, gated, inner_grad, grad_part, out_part, load_sem, *rest
):
    f32, bf16 = jnp.float32, jnp.bfloat16
    p = Place(count)
    rows, group = act.shape[0], down.shape[1]
    gather = Quad(p, act_all, rest[:2])
    grad_sum = QuadSum(p, grad_part, rest[2:5], rest[8:10])
    out_sum = QuadSum(p, out_part, rest[5:8], rest[10:12])
    units, half = in_other.shape[0], down_other.shape[0]
    in_rows = pl.ds(pl.multiple_of((p.x * 2 + p.core) * units, 16), units)
    own_at = pl.ds(pl.multiple_of(p.pair * group, group), units)
    other_at = pl.ds(pl.multiple_of((1 - p.pair) * group, group), units)
    load = pltpu.make_async_copy(act, act_all.at[p.x * 2 + p.core], load_sem.at[0])
    weights = [
        pltpu.make_async_copy(in_weight.at[in_rows], weight.at[own_at], load_sem.at[1]),
        pltpu.make_async_copy(in_other, weight.at[other_at], load_sem.at[2]),
    ]
    load.start()
    for copy in weights:
        copy.start()
    p.meet()
    load.wait()
    gather.start()
    down[...] = jnp.zeros_like(down)
    down[pl.ds(pl.multiple_of(p.pair * half, half), half), :units] = down_mine[...]
    down[pl.ds(pl.multiple_of((1 - p.pair) * half, half), half), :units] = down_other[...]
    for at in range(2):
        weight[at * group + units : (at + 1) * group, :] = jnp.zeros((group - units, weight.shape[1]), bf16)
    for copy in weights:
        copy.wait()
    gather.beside().wait_recv()

    @pl.loop(0, 2)
    def _(step):
        x = jnp.where(step == 0, p.x, 1 - p.x)

        @pl.when(step == 1)
        def _():
            gather.relay()
            gather.beside_next().wait_recv()

        acts = jnp.concatenate([act_all[2 * x], act_all[2 * x + 1]], axis=0)
        cots = jnp.concatenate([cot_all[2 * x], cot_all[2 * x + 1]], axis=0)
        inner = matmul(acts, weight[...], 1, 1)
        grad_gated = matmul(cots, down[...], 1, 0)
        value, gate = inner[:, :group], inner[:, group:]
        gelu_val, gelu_slope = gelu_pair(value)
        token = pl.ds(pl.multiple_of(x * 2 * rows, 2 * rows), 2 * rows)
        out = (gelu_val * gate).astype(bf16)
        gated[token, :] = out
        grads = jnp.concatenate(
            [grad_gated * gate * gelu_slope, grad_gated * gelu_val], axis=1
        ).astype(bf16)
        inner_grad[token, :] = grads
        part = matmul(grads, weight[...], 1, 0).astype(bf16)
        grad_part[2 * x], grad_part[2 * x + 1] = part[:rows], part[rows:]
        grad_sum.beside(x).start()
        part = matmul(out, down[...], 1, 1).astype(bf16)
        out_part[2 * x], out_part[2 * x + 1] = part[:rows], part[rows:]
        out_sum.beside(x).start()

    grad_sum.add(1 - p.x)
    grad_sum.across().start()
    grad_sum.add(p.x)
    out_sum.add(1 - p.x)
    out_sum.across().start()
    out_sum.add(p.x)
    acts = act_all[...].reshape(4 * rows, act.shape[1])
    cots = cot_all[...].reshape(4 * rows, act.shape[1])
    quarter = units // 4
    gain_row = jnp.zeros((1, act.shape[1]), f32)
    for at in range(2):
        piece = matmul(inner_grad[:, at * group : (at + 1) * group], acts, 0, 0)
        gain_row += jnp.sum(piece * weight[at * group : (at + 1) * group, :].astype(f32), axis=0, keepdims=True)
        for k in range(4):
            in_grad[k % 2 * p.line + at * 2 + k // 2] = piece[k * quarter : (k + 1) * quarter].astype(bf16)
    piece = matmul(cots, gated[...], 0, 0)
    lane = lax.broadcasted_iota(jnp.int32, piece.shape, 1)
    gain_row = gain_row / gain[...]
    column = jnp.broadcast_to(gain_row, (8, gain_row.shape[1])).T[:, :1]
    piece = jnp.where(lane == units, column, piece).astype(bf16)
    unit = act.shape[1] // (2 * count)
    for z in range(p.line):
        for r in range(4):
            for y in range(2):
                start = ((z * 4 + r) * 2 + y) * unit
                down_grad[y * p.line + z, r] = piece[start : start + unit]
    grad_sum.finish(grad_act)
    out_sum.finish(out_total)
    gather.sent()
    grad_sum.sent()
    out_sum.sent()


def attend_back_kernel(
    count, grad_mixed, grad_mid, mixed, query_t, keys_t, keys, values, mixed_own, log_sum,
    act_all, weight, cos, sine, in_grad, down_grad, gain,
    grad_act, qkv_out, out_out, in_out, down_out, gain_m_out, gain_a_out,
    grad_own, grad_keys, grad_values, grad_packed, grad_part, grad_got, grad_sums, grad_weight,
    pair_part, pair_core, pair_sums, pair_got, proj_sums, in_sum, in_got, down_sum, down_got,
    qkv_part, qkv_got, gain_part, gain_got,
    pair_s, pair_r, in_s, in_r, down_s, down_r, qkv_s, qkv_r, *rest
):
    f32, bf16 = jnp.float32, jnp.bfloat16
    p = Place(count)
    rows, head = grad_mixed.shape[2], keys_t.shape[0]
    width, unit = count * head, head // 2
    bufs, proj_bufs, in_bufs, down_bufs, sems = rest[:4], rest[4:8], rest[8:12], rest[12:16], rest[16:]
    trade = Exchange(p, grad_mixed, grad_own, sems[:2])
    halve = Halve(p, grad_part, grad_got, grad_sums, sems[2:4])
    settle = Settle(p, grad_sums, bufs, sems[4:10])
    halve_proj = Halve(p, pair_part, pair_core, pair_sums, sems[10:12])
    settle_proj = Settle(p, proj_sums, proj_bufs, sems[12:18])
    settle_in = Settle(p, in_grad, in_bufs, sems[18:24], True)
    settle_down = Settle(p, down_grad, down_bufs, sems[24:30], True)
    spread_gain = Spread(p, gain_part, gain_got, sems[30:32])
    give_in = Deliver(p, in_sum, in_got, (in_s, in_r))
    give_down = Deliver(p, down_sum, down_got, (down_s, down_r))
    give_qkv = Deliver(p, qkv_part, qkv_got, (qkv_s, qkv_r))

    def swap(at):
        return p.over_pair(pair_sums.at[at, 1 - p.pair], pair_got.at[at], pair_s.at[at], pair_r.at[at])

    p.meet(True)

    @pl.loop(0, count)
    def _(shift):
        trade.send((p.me + shift) % count)

    flat = mixed[...].reshape(width, rows)

    @pl.loop(0, count // 2)
    def _(i):
        lanes = pl.ds(pl.multiple_of(i * 4 * unit, 4 * unit), 4 * unit)
        piece = matmul(grad_mid[:, lanes], flat, 0, 1).astype(bf16)
        for at in range(4):
            pair_part[2 * i + at // 2, at % 2] = piece[at * unit : (at + 1) * unit]

    @pl.loop(0, 2 * p.line)
    def _(at):
        halve_proj.beside(at // 2, at % 2).start()

    @pl.loop(0, p.line)
    def _(step):
        z = p.far(step)
        halve_proj.add(z)
        swap(2 * z).start()
        swap(2 * z + 1).start()

    @pl.loop(0, p.line)
    def _(step):
        settle_in.across(p.far(step)).start()
        settle_down.across(p.far(step)).start()

    grad_keys[...] = jnp.zeros_like(grad_keys)
    grad_values[...] = jnp.zeros_like(grad_values)
    trade.arrived()
    wide = 2 * rows
    scale = head ** (-0.5)

    def back(i):
        lanes = pl.ds(pl.multiple_of(i * wide, wide), wide)
        query = query_t[:, lanes]
        grad = jnp.concatenate([grad_own[2 * i], grad_own[2 * i + 1]], axis=1)
        own = jnp.concatenate([mixed_own[2 * i], mixed_own[2 * i + 1]], axis=1)
        delta = jnp.sum(grad.astype(f32) * own.astype(f32), axis=0, keepdims=True)
        scores = matmul(keys[...], query, 1, 0) * scale
        probs = jnp.exp(scores - log_sum[:, lanes])
        grad_values[...] += matmul(probs.astype(bf16), grad, 1, 1)
        grad_probs = matmul(values[...], grad, 1, 0)
        grad_scores = (probs * (grad_probs - delta)).astype(bf16)
        grad_keys[...] += matmul(grad_scores, query, 1, 1)
        grad_query = matmul(keys_t[...], grad_scores, 1, 0) * scale
        back_query = rotate_rows_back(grad_query, cos[:, lanes], sine[:, lanes])
        grad_packed[:head, lanes] = back_query.astype(bf16)

    @pl.loop(0, count // 2)
    def _(i):
        back(i)

        @pl.when(i == count // 4)
        def _():
            settle_in.pass_on(p.far(0))
            settle_down.pass_on(p.far(0))

    @pl.loop(0, p.line)
    def _(step):
        z = p.far(step)
        for x in range(2):
            at = 2 * z + x
            swap(at).wait_recv()
            proj_sums[at] = (pair_sums[at, p.pair].astype(f32) + pair_got[at].astype(f32)).astype(bf16)
        settle_proj.across(z).start()

    settle_in.pass_on(p.far(1))
    settle_down.pass_on(p.far(1))
    grad_key = grad_keys[...].T * scale
    grad_packed[head : 2 * head, :] = rotate_rows_back(grad_key, cos[...], sine[...]).astype(bf16)
    grad_packed[2 * head :, :] = grad_values[...].T.astype(bf16)

    @pl.loop(0, p.line)
    def _(step):
        z = p.far(step)
        for at in range(4):
            lanes = pl.ds(pl.multiple_of((z * 4 + at) * rows, rows), rows)
            grad_part[z * 4 + at] = matmul(grad_packed[:, lanes], weight[...], 0, 0).astype(bf16)
        halve.beside(z, 0).start()
        halve.beside(z, 1).start()

    @pl.loop(0, p.line)
    def _(step):
        z = p.far(step)
        halve.add(z)
        settle.across(z).start()

    def grad_chunk(step):
        lanes = pl.ds(pl.multiple_of(step * 4 * rows, 4 * rows), 4 * rows)
        acts = jnp.concatenate([act_all[4 * step + i] for i in range(4)], axis=0)
        return matmul(grad_packed[:, lanes], acts, 1, 0)

    grad_weight[...] = grad_chunk(0)

    @pl.loop(1, p.line)
    def _(step):
        grad_weight[...] += grad_chunk(step)

    for at in range(6):
        qkv_part[at] = grad_weight[at * unit : (at + 1) * unit, :].astype(bf16)
    gain_row = jnp.sum(grad_weight[...] * weight[...].astype(f32), axis=0, keepdims=True) / gain[...]
    for at in range(2 * count):
        chunk = at * unit // 128 * 128
        gain_part[at] = gain_row[:, chunk : chunk + 128]

    def unit_of(at):
        return (at // 2) * 2 * count + 2 * p.me + at % 2

    for at in range(6):
        give_qkv.send(at, unit_of(at) // 3, unit_of(at) % 3 * 2 + p.pair)
    spread_gain.send()

    @pl.loop(0, p.line)
    def _(step):
        z = p.far(step)
        settle.pass_on(z)
        settle_proj.pass_on(z)

        @pl.when(step > 1)
        def _():
            settle_in.pass_on(z)
            settle_down.pass_on(z)

    units = in_out.shape[0]
    r = p.x * 2 + p.core
    piece_owner = p.z // 2 * count + r * 4 + p.z % 2 * 2 + p.pair
    settle_in.finish(in_sum.at[0])
    give_in.send(0, piece_owner, 0)
    settle_down.finish(down_sum)
    for at in range(4):
        give_down.send(at, (p.z * 4 + at) * 2 + p.pair, r)
    for slot in range(3):
        source = (3 * p.owner + slot) % (2 * count) // 2 * 2
        for side in range(2):
            give_qkv.arrived(2 * slot + side, source + side)
        qkv_out[slot * unit : (slot + 1) * unit, :] = qkv_got[2 * slot].astype(f32) + qkv_got[2 * slot + 1].astype(f32)
    spread_gain.arrived()
    gain_a = gain_got[0]
    for at in range(1, 2 * count):
        gain_a += gain_got[at]
    gain_a_out[...] = gain_a
    settle_proj.finish(out_out)
    settle.finish(grad_act)
    half, r_of, k_of = p.owner // count, p.owner % count // 4, p.owner % 4
    source_in = ((half * 2 + k_of // 2) * 4 + r_of) * 2 + k_of % 2
    give_in.arrived(0, source_in)
    in_out[...] = in_got[0].astype(f32)
    gain_m = jnp.zeros((unit, 1), f32)
    group = 4 * units
    for at in range(4):
        give_down.arrived(at, (p.z * 4 + at) * 2 + p.pair)
        block = down_got[at].astype(f32)
        down_out[:, at * group : (at + 1) * group] = block[:, :group]
        gain_m += block[:, group : group + 1]
    gain_m_out[...] = jnp.broadcast_to(gain_m, (unit, 128)).T[:1]
    trade.sent()
    halve.sent()
    settle.sent()
    halve_proj.sent()
    settle_proj.sent()
    settle_in.sent()
    settle_down.sent()
    spread_gain.sent()

    @pl.loop(0, 2 * p.line)
    def _(at):
        swap(at).wait_send()

    give_in.sent(0, piece_owner, 0)
    for at in range(4):
        give_down.sent(at, (p.z * 4 + at) * 2 + p.pair, r)
    for at in range(6):
        give_qkv.sent(at, unit_of(at) // 3, unit_of(at) % 3 * 2 + p.pair)


def run_kernel(body, outs, scratch, collective, flops, args, outside=(), outs_outside=()):
    vmem, anywhere = pl.BlockSpec(memory_space=pltpu.VMEM), pl.BlockSpec(memory_space=pl.ANY)
    return pl.pallas_call(
        body,
        out_shape=outs,
        in_specs=[anywhere if i in outside else vmem for i in range(len(args))],
        out_specs=[anywhere if i in outs_outside else vmem for i in range(len(outs))],
        scratch_shapes=scratch,
        compiler_params=pltpu.CompilerParams(
            collective_id=collective, has_side_effects=True, vmem_limit_bytes=VMEM_LIMIT
        ),
        cost_estimate=pl.CostEstimate(flops=flops, bytes_accessed=20_000_000, transcendentals=0),
        name=body.func.__name__,
    )(*args)


def shaped(shape, kind):
    return jax.ShapeDtypeStruct(shape, kind)


def attend(count, head, act, cot, qkv_weight, in_weight, down_mine, out_mine, cos, sine):
    bf16, f32 = jnp.bfloat16, jnp.float32
    rows, width = act.shape
    length, line = rows * count, count // 4
    blocks = shaped((count, rows, width), bf16)
    tall, flat = shaped((head, length), bf16), shaped((length, head), bf16)
    heads = shaped((count, head, rows), bf16)
    pairs = [shaped((in_weight.shape[0] // 4, width), bf16), shaped(down_mine.shape, bf16), shaped((2,) + out_mine.shape, bf16)]
    three, six = pltpu.SemaphoreType.DMA((3,)), pltpu.SemaphoreType.DMA((6,))
    return run_kernel(
        functools.partial(attend_kernel, count),
        [blocks, shaped((4, rows, width), bf16), tall, tall, flat, flat, heads, shaped((1, length), f32), heads, shaped((3, head, width), bf16)]
        + pairs,
        [pltpu.VMEM((head, length), bf16), pltpu.SemaphoreType.DMA((6,))] + [three, three, six, six]
        + Gather.sems(line) + Quad.sems() + Exchange.sems(count),
        0, 10_000_000_000, [act, cot, qkv_weight, in_weight, down_mine, out_mine, cos, sine], (2, 3, 4, 5), (10, 11),
    )


def feed(count, group, act, cot_all, in_weight, in_other, down_mine, down_other, gain):
    bf16, f32 = jnp.bfloat16, jnp.float32
    rows, width = act.shape
    block = (rows, width)
    units, line, unit = in_other.shape[0], count // 4, width // (2 * count)
    whole = pltpu.VMEM((4,) + block, bf16)
    return run_kernel(
        functools.partial(feed_kernel, count),
        [shaped(block, f32), shaped(block, f32), shaped((2 * line, units // 4, width), bf16),
         shaped((2 * line, 4, unit, group), bf16)],
        [pltpu.VMEM((2 * group, width), bf16), pltpu.VMEM((width, group), bf16),
         whole, pltpu.VMEM((4 * rows, group), bf16), pltpu.VMEM((4 * rows, 2 * group), bf16), whole, whole,
         pltpu.SemaphoreType.DMA((3,))]
        + Quad.sems() + QuadSum.bufs(block) * 2 + QuadSum.sems() * 2,
        1, 20_000_000_000, [act, cot_all, in_weight, in_other, down_mine, down_other, gain], (2, 3),
    )


def attend_back(count, grad_mixed, grad_mid, mixed, kept, act_all, weight, cos, sine, in_grad, down_grad, gain):
    bf16, f32 = jnp.bfloat16, jnp.float32
    rows, width = act_all.shape[1:]
    head, length, line = weight.shape[0] // 3, rows * count, count // 4
    block, unit, units = (rows, width), head // 2, in_grad.shape[1]
    down_block = down_grad.shape[1:]
    piece = (unit, width)

    def held(*shape):
        return pltpu.VMEM(shape, bf16)

    whole, half = held(count, *block), held(2 * line, *block)
    flat = pltpu.VMEM((length, head), f32)
    one, four, six, many = [pltpu.SemaphoreType.DMA((n,)) for n in (1, 4, 6, 2 * line)]
    return run_kernel(
        functools.partial(attend_back_kernel, count),
        [shaped(block, f32), shaped((3 * unit, width), f32), shaped(piece, f32),
         shaped((units, width), f32), shaped((unit, units * count), f32), shaped((1, unit), f32), shaped((1, 128), f32)],
        [held(count, head, rows), flat, flat, held(3 * head, length), whole, half, half,
         pltpu.VMEM((3 * head, width), f32),
         held(count, 2, *piece), held(2 * line, 2, *piece), held(2 * line, 2, *piece), held(2 * line, *piece),
         held(2 * line, *piece), held(1, units, width), held(1, units, width), held(*down_block), held(*down_block),
         held(6, *piece), held(6, *piece), pltpu.VMEM((2 * count, 1, 128), f32), pltpu.VMEM((2 * count, 1, 128), f32),
         many, many, one, one, four, four, six, six]
        + Settle.bufs(line, block) + Settle.bufs(line, piece)
        + Settle.bufs(line, (units, width)) + Settle.bufs(line, down_block)
        + Exchange.sems(count) + (Halve.sems(line) + Settle.sems(line)) * 2
        + Settle.sems(line) * 2 + Spread.sems(count),
        2, 20_000_000_000,
        [grad_mixed, grad_mid, mixed, *kept, act_all, weight, cos, sine, in_grad, down_grad, gain],
    )


def tensor_layer(
    tokens, cotangent, gain_attn, gain_mlp, qkv_weight, out_weight, in_weight, down_weight
):
    f32 = jnp.float32
    bf16 = jnp.bfloat16
    count = lax.axis_size("ctx")
    index = lax.axis_index("ctx")
    rows, width = tokens.shape[1], tokens.shape[2]
    length = rows * count
    head_size = width // count
    quad = lax.rem(index, 4)
    group = in_weight.shape[0] // 4
    padded = (group // 128 + 1) * 128

    down_mine = lax.dynamic_slice_in_dim(down_weight, quad * group, group, 1)

    cos_table, sine_table = rope_tables(0, length, head_size)
    cos_table, sine_table = cos_table[:, 0, : head_size // 2].T, sine_table[:, 0, : head_size // 2].T
    resid = tokens[0].astype(f32)
    normed_a, inv_a = normalize(resid)
    act_a = (normed_a * gain_attn).astype(bf16)
    cot_rows = cotangent[0]
    act_all, cot_all, *kept, mixed, qkv_head, in_other, down_other, out_pair = attend(
        count, head_size, act_a, cot_rows, qkv_weight, in_weight, down_mine, out_weight, cos_table, sine_table
    )
    qkv_head = qkv_head.reshape(3 * head_size, width)
    out_full = out_pair.reshape(width, width)
    middle = resid + matmul(mixed.reshape(width, rows), out_full, 0, 1)
    normed_m, inv_m = normalize(middle)
    act_m = (normed_m * gain_mlp).astype(bf16)
    grad_act_m, out_total, in_grad, down_grad = feed(
        count, padded, act_m, cot_all, in_weight, in_other, down_mine, down_other, gain_mlp[None]
    )

    grad_middle = cot_rows.astype(f32) + norm_back(grad_act_m * gain_mlp, normed_m, inv_m)
    grad_mid_bf = grad_middle.astype(bf16)
    grad_mixed = matmul(out_full, grad_mid_bf, 0, 1).astype(bf16).reshape(count, head_size, rows)
    grad_act_a, grad_qkv, grad_out, grad_in, grad_down, grad_gain_m, grad_gain_a = attend_back(
        count, grad_mixed, grad_mid_bf, mixed, kept, act_all, qkv_head, cos_table, sine_table,
        in_grad, down_grad, gain_attn[None],
    )
    unit = width // (2 * count)
    lane = lax.rem((index * 2 + lax.axis_index("fsdp")) * unit, 128)
    grad_gain_a = lax.dynamic_slice_in_dim(grad_gain_a[0], lane, unit)
    output = middle + out_total
    grad_input = grad_middle + norm_back(grad_act_a * gain_attn, normed_a, inv_a)
    return (
        output[None], grad_input[None], grad_qkv, grad_out, grad_in, grad_down,
        grad_gain_a, grad_gain_m[0],
    )


def solution(mesh):

    def layer(*arrays):
        one_head_each = arrays[0].shape[2] == HEAD_DIM * mesh.shape["ctx"]
        if one_head_each and mesh.shape["fsdp"] == 2 and mesh.shape["ctx"] % 4 == 0:
            return tensor_layer(*arrays)
        return gathered_layer(*arrays)

    return jax.shard_map(
        layer,
        mesh=mesh,
        in_specs=(
            P("fsdp", "ctx", None),
            P("fsdp", "ctx", None),
            P(),
            P(),
            P("fsdp", None),
            P("fsdp", None),
            P("fsdp", None),
            P("fsdp", None),
        ),
        out_specs=(
            P("fsdp", "ctx", None),
            P("fsdp", "ctx", None),
            P(("ctx", "fsdp"), None),
            P(("ctx", "fsdp"), None),
            P(("ctx", "fsdp"), None),
            P(("ctx", "fsdp"), None),
            P(("ctx", "fsdp")),
            P(("ctx", "fsdp")),
        ),
        check_vma=False,
    )
```

```python
import functools
import math

import jax
import jax.numpy as jnp
from jax import lax
from jax.experimental import pallas as pl
from jax.experimental.pallas import tpu as pltpu
from jax.sharding import PartitionSpec as P

HEAD_DIM = 64


EPSILON = 1e-05
ROPE_BASE = 160000.0


def normalize(tensor):
    centred = tensor - jnp.mean(tensor, axis=-1, keepdims=True)
    inv_std = lax.rsqrt(jnp.mean(centred * centred, axis=-1, keepdims=True) + EPSILON)
    return (centred * inv_std, inv_std)


def norm_back(grad_norm, normed, inv_std):
    return inv_std * (
        grad_norm
        - jnp.mean(grad_norm, axis=-1, keepdims=True)
        - normed * jnp.mean(grad_norm * normed, axis=-1, keepdims=True)
    )


def gelu_pair(tensor):
    cumul = 0.5 * (1.0 + jax.scipy.special.erf(tensor * 0.7071067811865476))
    density = jnp.exp(-0.5 * tensor * tensor) * 0.3989422804014327
    return (tensor * cumul, cumul + tensor * density)


def rope_tables(offset, length, head_size):
    positions = (offset + jnp.arange(length, dtype=jnp.int32)).astype(jnp.float32)
    inverse = ROPE_BASE ** (
        -jnp.arange(0, head_size, 2, dtype=jnp.int32).astype(jnp.float32) / head_size
    )
    angles = positions[:, None] * inverse[None, :]
    angles = jnp.concatenate([angles, angles], axis=-1)
    return (jnp.cos(angles)[:, None, :], jnp.sin(angles)[:, None, :])


def rotate(tensor, cos_table, sine_table):
    middle = tensor.shape[-1] // 2
    turned = jnp.concatenate([-tensor[..., middle:], tensor[..., :middle]], axis=-1)
    return tensor * cos_table + turned * sine_table


def rotate_back(gradient, cos_table, sine_table):
    middle = gradient.shape[-1] // 2
    scaled = gradient * sine_table
    turned = jnp.concatenate([scaled[..., middle:], -scaled[..., :middle]], axis=-1)
    return gradient * cos_table + turned


def rows_product(left, right):
    return lax.dot_general(
        left, right, (((1,), (1,)), ((), ())), preferred_element_type=jnp.float32
    )


def rows_contract(left, right):
    return lax.dot_general(
        left, right, (((0,), (0,)), ((), ())), preferred_element_type=jnp.float32
    )


def gathered_layer(
    tokens, cotangent, gain_attn, gain_mlp, qkv_weight, out_weight, in_weight, down_weight
):
    f32 = jnp.float32
    bf16 = jnp.bfloat16
    qkv_full, out_full, in_full, down_full = (
        lax.all_gather(qkv_weight, "fsdp", axis=0, tiled=True),
        lax.all_gather(out_weight, "fsdp", axis=0, tiled=True),
        lax.all_gather(in_weight, "fsdp", axis=0, tiled=True),
        lax.all_gather(down_weight, "fsdp", axis=0, tiled=True),
    )
    tok_rows = tokens.shape[1]
    width = tokens.shape[2]
    hidden = down_full.shape[1]
    head_size = HEAD_DIM
    head_count = width // head_size
    scale = head_size ** (-0.5)
    offset = lax.axis_index("ctx") * tok_rows
    cos_table, sine_table = rope_tables(offset, tok_rows, head_size)
    resid = tokens[0].astype(f32)
    normed_a, inv_a = normalize(resid)
    act_a = (normed_a * gain_attn).astype(bf16)
    packed = rows_product(act_a, qkv_full)
    query_heads = rotate(
        packed[:, :width].reshape(tok_rows, head_count, head_size), cos_table, sine_table
    ).astype(bf16)
    key_heads = rotate(
        packed[:, width : 2 * width].reshape(tok_rows, head_count, head_size), cos_table, sine_table
    ).astype(bf16)
    value_send = packed[:, 2 * width :].astype(bf16)
    key_send = key_heads.reshape(tok_rows, width)
    value_heads = value_send.reshape(tok_rows, head_count, head_size)
    start_state = (
        jnp.zeros((tok_rows, head_count, head_size), f32),
        jnp.full((head_count, tok_rows), -1e30, f32),
        jnp.zeros((head_count, tok_rows), f32),
    )
    key_piece = lax.all_gather(key_send, "ctx", axis=0, tiled=True)
    value_piece = lax.all_gather(value_send, "ctx", axis=0, tiled=True)
    length = key_piece.shape[0]
    step_len = math.gcd(length, 1024)

    def attend_block(block_num, running):
        weighted, row_max, row_sum = running
        key_blk = lax.dynamic_slice_in_dim(key_piece, block_num * step_len, step_len, 0).reshape(
            step_len, head_count, head_size
        )
        value_blk = lax.dynamic_slice_in_dim(
            value_piece, block_num * step_len, step_len, 0
        ).reshape(step_len, head_count, head_size)
        scores = (
            jnp.einsum("qhd,khd->hqk", query_heads, key_blk, preferred_element_type=f32) * scale
        )
        new_max = jnp.maximum(row_max, jnp.max(scores, axis=-1))
        shrink = jnp.exp(row_max - new_max)
        weights = jnp.exp(scores - new_max[..., None])
        row_sum = row_sum * shrink + jnp.sum(weights, axis=-1)
        weighted = weighted * shrink.T[:, :, None] + jnp.einsum(
            "hqk,khd->qhd", weights.astype(bf16), value_blk, preferred_element_type=f32
        )
        return (weighted, new_max, row_sum)

    weighted, row_max, row_sum = lax.fori_loop(0, length // step_len, attend_block, start_state)
    log_sum = row_max + jnp.log(row_sum)
    mixed = (weighted / row_sum.T[:, :, None]).reshape(tok_rows, width).astype(bf16)
    middle = resid + rows_product(mixed, out_full)
    normed_m, inv_m = normalize(middle)
    act_m = (normed_m * gain_mlp).astype(bf16)
    inner = rows_product(act_m, in_full)
    gelu_val, gelu_slope = gelu_pair(inner[:, :hidden])
    gated = (gelu_val * inner[:, hidden:]).astype(bf16)
    output = middle + rows_product(gated, down_full)
    cot_rows = cotangent[0]
    grad_down = rows_contract(cot_rows, gated)
    grad_gated = jnp.dot(cot_rows, down_full, preferred_element_type=f32)
    grad_inner = jnp.concatenate(
        [grad_gated * inner[:, hidden:] * gelu_slope, grad_gated * gelu_val], axis=1
    ).astype(bf16)
    grad_in = rows_contract(grad_inner, act_m)
    grad_act_m = jnp.dot(grad_inner, in_full, preferred_element_type=f32)
    grad_gain_m = jnp.sum(grad_act_m * normed_m, axis=0)
    grad_middle = cot_rows.astype(f32) + norm_back(grad_act_m * gain_mlp, normed_m, inv_m)
    grad_mid_bf = grad_middle.astype(bf16)
    grad_out = rows_contract(grad_mid_bf, mixed)
    grad_mixed = jnp.dot(grad_mid_bf, out_full, preferred_element_type=f32).astype(bf16)
    grad_heads = grad_mixed.reshape(tok_rows, head_count, head_size)
    delta_rows = jnp.sum(
        grad_heads.astype(f32) * mixed.reshape(tok_rows, head_count, head_size).astype(f32), axis=-1
    )
    delta = delta_rows.T
    zeros_heads = jnp.zeros((tok_rows, head_count, head_size), f32)
    query_key_piece = lax.all_gather(key_send, "ctx", axis=0, tiled=True)
    query_value_piece = lax.all_gather(value_send, "ctx", axis=0, tiled=True)
    length = query_key_piece.shape[0]
    query_step_len = math.gcd(length, 1024)

    def query_grad_block(block_num, grad_query):
        key_blk = lax.dynamic_slice_in_dim(
            query_key_piece, block_num * query_step_len, query_step_len, 0
        ).reshape(query_step_len, head_count, head_size)
        value_blk = lax.dynamic_slice_in_dim(
            query_value_piece, block_num * query_step_len, query_step_len, 0
        ).reshape(query_step_len, head_count, head_size)
        scores = (
            jnp.einsum("qhd,khd->hqk", query_heads, key_blk, preferred_element_type=f32) * scale
        )
        probs = jnp.exp(scores - log_sum[..., None])
        grad_probs = jnp.einsum("qhd,khd->hqk", grad_heads, value_blk, preferred_element_type=f32)
        grad_scores = (probs * (grad_probs - delta[..., None])).astype(bf16)
        return (
            grad_query
            + jnp.einsum("hqk,khd->qhd", grad_scores, key_blk, preferred_element_type=f32) * scale
        )

    grad_query = lax.fori_loop(0, length // query_step_len, query_grad_block, zeros_heads)
    query_send = query_heads.reshape(tok_rows, width).astype(f32)
    grad_send = grad_mixed.astype(f32)
    query_piece = lax.all_gather(query_send, "ctx", axis=0, tiled=True)
    grad_piece = lax.all_gather(grad_send, "ctx", axis=0, tiled=True)
    log_piece = lax.all_gather(log_sum.T, "ctx", axis=0, tiled=True)
    delta_piece = lax.all_gather(delta_rows, "ctx", axis=0, tiled=True)
    length = query_piece.shape[0]
    key_step_len = math.gcd(length, 1024)

    def key_grad_block(block_num, running):
        grad_keys, grad_values = running
        query_blk = (
            lax.dynamic_slice_in_dim(query_piece, block_num * key_step_len, key_step_len, 0)
            .astype(bf16)
            .reshape(key_step_len, head_count, head_size)
        )
        grad_blk = (
            lax.dynamic_slice_in_dim(grad_piece, block_num * key_step_len, key_step_len, 0)
            .astype(bf16)
            .reshape(key_step_len, head_count, head_size)
        )
        log_blk = lax.dynamic_slice_in_dim(log_piece, block_num * key_step_len, key_step_len, 0).T
        delta_blk = lax.dynamic_slice_in_dim(
            delta_piece, block_num * key_step_len, key_step_len, 0
        ).T
        scores = (
            jnp.einsum("qhd,khd->hqk", query_blk, key_heads, preferred_element_type=f32) * scale
        )
        probs = jnp.exp(scores - log_blk[..., None])
        grad_values = grad_values + jnp.einsum(
            "hqk,qhd->khd", probs.astype(bf16), grad_blk, preferred_element_type=f32
        )
        grad_probs = jnp.einsum("qhd,khd->hqk", grad_blk, value_heads, preferred_element_type=f32)
        grad_scores = (probs * (grad_probs - delta_blk[..., None])).astype(bf16)
        grad_keys = (
            grad_keys
            + jnp.einsum("hqk,qhd->khd", grad_scores, query_blk, preferred_element_type=f32) * scale
        )
        return (grad_keys, grad_values)

    grad_keys, grad_values = lax.fori_loop(
        0, length // key_step_len, key_grad_block, (zeros_heads, zeros_heads)
    )
    grad_query = rotate_back(grad_query, cos_table, sine_table)
    grad_keys = rotate_back(grad_keys, cos_table, sine_table)
    grad_packed = jnp.concatenate(
        [
            grad_query.reshape(tok_rows, width),
            grad_keys.reshape(tok_rows, width),
            grad_values.reshape(tok_rows, width),
        ],
        axis=1,
    ).astype(bf16)
    grad_qkv = rows_contract(grad_packed, act_a)
    grad_act_a = jnp.dot(grad_packed, qkv_full, preferred_element_type=f32)
    grad_gain_a = jnp.sum(grad_act_a * normed_a, axis=0)
    grad_input = grad_middle + norm_back(grad_act_a * gain_attn, normed_a, inv_a)
    owned = (
        lax.psum_scatter(grad_qkv, ("ctx", "fsdp"), scatter_dimension=0, tiled=True),
        lax.psum_scatter(grad_out, ("ctx", "fsdp"), scatter_dimension=0, tiled=True),
        lax.psum_scatter(grad_in, ("ctx", "fsdp"), scatter_dimension=0, tiled=True),
        lax.psum_scatter(grad_down, ("ctx", "fsdp"), scatter_dimension=0, tiled=True),
        lax.psum_scatter(grad_gain_a, ("ctx", "fsdp"), scatter_dimension=0, tiled=True),
        lax.psum_scatter(grad_gain_m, ("ctx", "fsdp"), scatter_dimension=0, tiled=True),
    )
    return (
        output[None],
        grad_input[None],
        owned[0],
        owned[1],
        owned[2],
        owned[3],
        owned[4],
        owned[5],
    )


MESH = pl.DeviceIdType.MESH
VMEM_LIMIT = 60 * 1024 * 1024


def matmul(left, right, left_dim, right_dim):
    return lax.dot_general(
        left, right, (((left_dim,), (right_dim,)), ((), ())), preferred_element_type=jnp.float32
    )


class Place:
    def __init__(self, count):
        self.count, self.line = count, count // 4
        self.me, self.pair = lax.axis_index("ctx"), lax.axis_index("fsdp")
        self.owner = self.me * 2 + self.pair
        self.z, self.x, self.core = self.me // 4, self.me // 2 % 2, self.me % 2

    def slot(self, z, x, core):
        return z * 4 + x * 2 + core

    def far(self, step):
        last = self.line - 1
        low = 2 * self.z < self.line
        own = jnp.where(low, self.z, last - self.z)
        at = jnp.where(
            step < last - own, last - step, jnp.where(step == last, own, step - (last - own))
        )
        return jnp.where(low, at, last - at)

    def near(self, step):
        return self.far(self.line - 1 - step)

    def meet(self, everyone=False):
        barrier = pltpu.get_barrier_semaphore()

        @pl.loop(1, self.count)
        def _(shift):
            pl.semaphore_signal(
                barrier, inc=1, device_id={"ctx": (self.me + shift) % self.count}, device_id_type=MESH
            )

        if everyone:
            @pl.loop(0, self.count)
            def _(to):
                pl.semaphore_signal(
                    barrier, inc=1, device_id={"ctx": to, "fsdp": 1 - self.pair}, device_id_type=MESH
                )

            pl.semaphore_wait(barrier, 2 * self.count - 1)
        else:
            pl.semaphore_signal(barrier, inc=1, device_id={"fsdp": 1 - self.pair}, device_id_type=MESH)
            pl.semaphore_wait(barrier, self.count)

    def over_pair(self, src, dst, send, recv):
        return pltpu.make_async_remote_copy(
            src_ref=src, dst_ref=dst, send_sem=send, recv_sem=recv,
            device_id={"fsdp": 1 - self.pair}, device_id_type=MESH,
        )

    def to_owner(self, src, dst, send, recv, owner):
        return pltpu.make_async_remote_copy(
            src_ref=src, dst_ref=dst, send_sem=send, recv_sem=recv,
            device_id={"ctx": owner // 2, "fsdp": owner % 2}, device_id_type=MESH,
        )

    def copy(self, src, dst, send, recv, to):
        return pltpu.make_async_remote_copy(
            src_ref=src, dst_ref=dst, send_sem=send, recv_sem=recv,
            device_id={"ctx": to}, device_id_type=MESH,
        )


class Gather:
    def __init__(self, place, buf, sems):
        self.p, self.buf = place, buf
        self.up_s, self.up_r, self.dn_s, self.dn_r, self.x_s, self.x_r, self.c_s, self.c_r = sems

    @staticmethod
    def sems(line):
        return [pltpu.SemaphoreType.DMA((line,))] * 6 + [pltpu.SemaphoreType.DMA((2 * line,))] * 2

    def over(self, z, x, core, send, recv, to):
        at = self.buf.at[self.p.slot(z, x, core)]
        return self.p.copy(at, at, send, recv, to)

    def up(self, z):
        p = self.p
        return self.over(z, p.x, p.core, self.up_s.at[z], self.up_r.at[z], (p.me + 4) % p.count)

    def down(self, z):
        p = self.p
        return self.over(z, p.x, p.core, self.dn_s.at[z], self.dn_r.at[z], (p.me + p.count - 4) % p.count)

    def across(self, z):
        p = self.p
        return self.over(z, p.x, p.core, self.x_s.at[z], self.x_r.at[z], p.slot(p.z, 1 - p.x, p.core))

    def beside(self, z, x):
        p = self.p
        at = z * 2 + x
        return self.over(z, x, p.core, self.c_s.at[at], self.c_r.at[at], p.slot(p.z, p.x, 1 - p.core))

    def arrive(self, z):
        p = self.p

        @pl.when(z < p.z)
        def _():
            self.up(z).wait_recv()

        @pl.when(z > p.z)
        def _():
            self.down(z).wait_recv()

        @pl.when((z <= p.z) & (p.z < p.line - 1))
        def _():
            self.up(z).start()

        @pl.when((z >= p.z) & (p.z > 0))
        def _():
            self.down(z).start()

        self.across(z).start()
        self.beside(z, p.x).start()

    def arrive_across(self, z):
        self.across(z).wait_recv()
        self.beside(z, 1 - self.p.x).start()

    def part(self, turn, use=None):
        p = self.p
        step, part = turn // 4, turn % 4
        z = jnp.where(part == 0, p.near(step), p.near(step - 1))

        @pl.when(jnp.where(part == 0, step < p.line, step > 0))
        def _():
            @pl.when(part == 0)
            def _():
                self.arrive(z)

            @pl.when(part == 1)
            def _():
                self.arrive_across(z)

            x = jnp.where(part % 2 == 0, p.x, 1 - p.x)

            @pl.when(part >= 2)
            def _():
                self.beside(z, x).wait_recv()

            if use is not None:
                use(z, x, jnp.where(part < 2, p.core, 1 - p.core))

    def sent(self):
        p = self.p

        @pl.loop(0, p.line)
        def _(z):
            @pl.when((z <= p.z) & (p.z < p.line - 1))
            def _():
                self.up(z).wait_send()

            @pl.when((z >= p.z) & (p.z > 0))
            def _():
                self.down(z).wait_send()

            self.across(z).wait_send()
            self.beside(z, 0).wait_send()
            self.beside(z, 1).wait_send()


class Halve:
    def __init__(self, place, whole, got, sums, sems):
        self.p, self.whole, self.got, self.sums = place, whole, got, sums
        self.c_s, self.c_r = sems

    @staticmethod
    def sems(line):
        return [pltpu.SemaphoreType.DMA((2 * line,))] * 2

    def beside(self, z, x):
        p, at = self.p, z * 2 + x
        return p.copy(
            self.whole.at[p.slot(z, x, 1 - p.core)], self.got.at[at], self.c_s.at[at], self.c_r.at[at],
            p.slot(p.z, p.x, 1 - p.core),
        )

    def add(self, z):
        p = self.p
        for x in range(2):
            at = z * 2 + x
            self.beside(z, x).wait_recv()
            self.sums[at] = (
                self.whole[p.slot(z, x, p.core)].astype(jnp.float32) + self.got[at].astype(jnp.float32)
            ).astype(self.sums.dtype)

    def sent(self):
        @pl.loop(0, 2 * self.p.line)
        def _(at):
            self.beside(at // 2, at % 2).wait_send()


class Quad:
    def __init__(self, place, buf, sems):
        self.p, self.buf = place, buf
        self.s, self.r = sems

    @staticmethod
    def sems():
        return [pltpu.SemaphoreType.DMA((3,))] * 2

    def over(self, x, to, at):
        piece = self.buf.at[x * 2 + self.p.core]
        return self.p.copy(piece, piece, self.s.at[at], self.r.at[at], to)

    def across(self):
        p = self.p
        return self.over(p.x, p.slot(p.z, 1 - p.x, p.core), 0)

    def beside(self):
        p = self.p
        return self.over(p.x, p.slot(p.z, p.x, 1 - p.core), 1)

    def beside_next(self):
        p = self.p
        return self.over(1 - p.x, p.slot(p.z, p.x, 1 - p.core), 2)

    def start(self):
        self.across().start()
        self.beside().start()

    def relay(self):
        self.across().wait_recv()
        self.beside_next().start()

    def sent(self):
        self.across().wait_send()
        self.beside().wait_send()
        self.beside_next().wait_send()


class QuadSum:
    def __init__(self, place, whole, bufs, sems):
        self.p, self.whole = place, whole
        self.got, self.sums, self.far = bufs
        self.s, self.r = sems

    @staticmethod
    def sems():
        return [pltpu.SemaphoreType.DMA((3,))] * 2

    @staticmethod
    def bufs(block):
        return [pltpu.VMEM((2,) + block, jnp.bfloat16)] * 2 + [pltpu.VMEM(block, jnp.bfloat16)]

    def beside(self, x):
        p = self.p
        return p.copy(
            self.whole.at[x * 2 + 1 - p.core], self.got.at[x], self.s.at[x], self.r.at[x],
            p.slot(p.z, p.x, 1 - p.core),
        )

    def across(self):
        p = self.p
        return p.copy(
            self.sums.at[1 - p.x], self.far, self.s.at[2], self.r.at[2], p.slot(p.z, 1 - p.x, p.core)
        )

    def add(self, x):
        f32 = jnp.float32
        self.beside(x).wait_recv()
        self.sums[x] = (
            self.whole[x * 2 + self.p.core].astype(f32) + self.got[x].astype(f32)
        ).astype(self.sums.dtype)

    def finish(self, out):
        f32 = jnp.float32
        self.across().wait_recv()
        out[...] = self.sums[self.p.x].astype(f32) + self.far[...].astype(f32)

    def sent(self):
        self.beside(0).wait_send()
        self.beside(1).wait_send()
        self.across().wait_send()


class Settle:
    def __init__(self, place, sums, bufs, sems, pairwise=False):
        self.p, self.sums, self.pairwise = place, sums, pairwise
        self.got, self.total, self.low, self.high = bufs
        self.x_s, self.x_r, self.up_s, self.up_r, self.dn_s, self.dn_r = sems

    @staticmethod
    def sems(line):
        return [pltpu.SemaphoreType.DMA((line,))] * 6

    @staticmethod
    def bufs(line, block):
        return [pltpu.VMEM((line,) + block, jnp.bfloat16)] * 4

    def kept(self, z):
        p = self.p
        return p.pair * p.line + z if self.pairwise else z * 2 + p.x

    def across(self, z):
        p = self.p
        if self.pairwise:
            return p.over_pair(
                self.sums.at[(1 - p.pair) * p.line + z], self.got.at[z], self.x_s.at[z], self.x_r.at[z]
            )
        return p.copy(
            self.sums.at[z * 2 + 1 - p.x], self.got.at[z], self.x_s.at[z], self.x_r.at[z],
            p.slot(p.z, 1 - p.x, p.core),
        )

    def up(self, z):
        p = self.p
        return p.copy(self.total.at[z], self.low.at[z], self.up_s.at[z], self.up_r.at[z], (p.me + 4) % p.count)

    def down(self, z):
        p = self.p
        return p.copy(
            self.total.at[z], self.high.at[z], self.dn_s.at[z], self.dn_r.at[z], (p.me + p.count - 4) % p.count
        )

    def pass_on(self, z):
        p, f32 = self.p, jnp.float32
        self.across(z).wait_recv()
        self.total[z] = (
            self.sums[self.kept(z)].astype(f32) + self.got[z].astype(f32)
        ).astype(self.total.dtype)

        @pl.when(z > p.z)
        def _():
            @pl.when(p.z > 0)
            def _():
                self.up(z).wait_recv()
                self.total[z] = (self.total[z].astype(f32) + self.low[z].astype(f32)).astype(self.total.dtype)

            self.up(z).start()

        @pl.when(z < p.z)
        def _():
            @pl.when(p.z < p.line - 1)
            def _():
                self.down(z).wait_recv()
                self.total[z] = (self.total[z].astype(f32) + self.high[z].astype(f32)).astype(self.total.dtype)

            self.down(z).start()

    def finish(self, out):
        p, f32 = self.p, jnp.float32
        @pl.when(p.z > 0)
        def _():
            self.up(p.z).wait_recv()

        @pl.when(p.z < p.line - 1)
        def _():
            self.down(p.z).wait_recv()

        total = self.total[p.z].astype(f32)
        total += jnp.where(p.z > 0, self.low[p.z].astype(f32), 0.0)
        total += jnp.where(p.z < p.line - 1, self.high[p.z].astype(f32), 0.0)
        out[...] = total.astype(out.dtype)

    def sent(self):
        p = self.p

        @pl.loop(0, p.line)
        def _(z):
            self.across(z).wait_send()

            @pl.when(z > p.z)
            def _():
                self.up(z).wait_send()

            @pl.when(z < p.z)
            def _():
                self.down(z).wait_send()


class Exchange:
    def __init__(self, place, src, dst, sems):
        self.p, self.src, self.dst = place, src, dst
        self.s, self.r = sems

    @staticmethod
    def sems(count):
        return [pltpu.SemaphoreType.DMA((count,))] * 2

    def to(self, j):
        return self.p.copy(self.src.at[j], self.dst.at[self.p.me], self.s.at[j], self.r.at[self.p.me], j)

    def send(self, j):
        @pl.when(j != self.p.me)
        def _():
            self.to(j).start()

        @pl.when(j == self.p.me)
        def _():
            self.dst[j] = self.src[j]

    def arrived(self):
        p = self.p

        @pl.loop(1, p.count)
        def _(shift):
            j = (p.me + shift) % p.count
            p.copy(self.src.at[j], self.dst.at[j], self.s.at[j], self.r.at[j], j).wait_recv()

    def sent(self):
        p = self.p

        @pl.loop(1, p.count)
        def _(shift):
            self.to((p.me + shift) % p.count).wait_send()


class Spread:
    def __init__(self, place, src, dst, sems):
        self.p, self.src, self.dst = place, src, dst
        self.s, self.r = sems

    @staticmethod
    def sems(count):
        return [pltpu.SemaphoreType.DMA((2 * count,))] * 2

    def to(self, j):
        p = self.p
        return p.to_owner(self.src.at[j], self.dst.at[p.owner], self.s.at[j], self.r.at[p.owner], j)

    def send(self):
        p = self.p
        self.dst[p.owner] = self.src[p.owner]

        @pl.loop(1, 2 * p.count)
        def _(shift):
            self.to((p.owner + shift) % (2 * p.count)).start()

    def arrived(self):
        p = self.p

        @pl.loop(1, 2 * p.count)
        def _(shift):
            j = (p.owner + shift) % (2 * p.count)
            p.to_owner(self.src.at[j], self.dst.at[j], self.s.at[j], self.r.at[j], j).wait_recv()

    def sent(self):
        p = self.p

        @pl.loop(1, 2 * p.count)
        def _(shift):
            self.to((p.owner + shift) % (2 * p.count)).wait_send()


class Deliver:
    def __init__(self, place, src, dst, sems):
        self.p, self.src, self.dst = place, src, dst
        self.s, self.r = sems

    def away(self, piece, owner, slot):
        return self.p.to_owner(self.src.at[piece], self.dst.at[slot], self.s.at[piece], self.r.at[slot], owner)

    def send(self, piece, owner, slot):
        @pl.when(owner != self.p.owner)
        def _():
            self.away(piece, owner, slot).start()

        @pl.when(owner == self.p.owner)
        def _():
            self.dst[slot] = self.src[piece]

    def sent(self, piece, owner, slot):
        @pl.when(owner != self.p.owner)
        def _():
            self.away(piece, owner, slot).wait_send()

    def arrived(self, slot, source):
        p = self.p

        @pl.when(source != p.owner)
        def _():
            p.to_owner(self.src.at[0], self.dst.at[slot], self.s.at[0], self.r.at[slot], source).wait_recv()


def rotate_rows(value, cos, sine):
    half = value.shape[0] // 2
    first, second = value[:half], value[half:]
    return jnp.concatenate([first * cos - second * sine, second * cos + first * sine], axis=0)


def rotate_rows_back(grad, cos, sine):
    half = grad.shape[0] // 2
    first, second = grad[:half], grad[half:]
    return jnp.concatenate([first * cos + second * sine, second * cos - first * sine], axis=0)


def attend_kernel(
    count, tokens, cot, gain_attn, gain_mlp, qkv_weight, in_weight, down_mine, out_mine,
    normed_a, inv_a, normed_m, inv_m, middle, act_m, cos, sine, act_all, cot_all, query_t, keys_t, keys, values, mixed_own, log_sum, mixed, weight, in_other, down_other, out_pair,
    values_t, load_sem, part_sem, part_got, piece_sem, piece_got, *sems
):
    f32, bf16 = jnp.float32, jnp.bfloat16
    p = Place(count)
    rows, width = tokens.shape
    head = keys_t.shape[0]
    n = 8
    first = Gather(p, act_all, sems[:n])
    second = Quad(p, cot_all, sems[n : n + 2])
    trade = Exchange(p, mixed_own, mixed, sems[n + 2 :])
    half = out_mine.shape[0] // 2
    part_half = pl.ds(pl.multiple_of(p.core * half, half), half)
    loads = [(cot, cot_all.at[p.x * 2 + p.core]), (out_mine, out_pair.at[p.pair])]
    loads = [pltpu.make_async_copy(src, dst, load_sem.at[i]) for i, (src, dst) in enumerate(loads)]
    for load in loads:
        load.start()

    def part_rows(part):
        start = part * width + p.me * head
        holder = start // qkv_weight.shape[0]
        at = pl.ds(pl.multiple_of(start - holder * qkv_weight.shape[0], head), head)
        return holder == p.pair, qkv_weight.at[at]

    def part_copies(part):
        here, src = part_rows(part)
        return (
            here,
            pltpu.make_async_copy(src, weight.at[part], load_sem.at[3 + part]),
            p.over_pair(src, weight.at[part], part_sem.at[part], part_got.at[part]),
        )

    units, columns = in_other.shape[0], in_other.shape[1] // 2
    in_rows = pl.ds(pl.multiple_of((p.x * 2 + p.core) * units, 16), units)
    in_cols = pl.ds(pl.multiple_of(p.z % 2 * columns, columns), columns)
    in_here = in_other.at[:, in_cols]
    swaps = [
        p.over_pair(out_mine.at[part_half], out_pair.at[p.pair, part_half], piece_sem.at[0], piece_got.at[0]),
        p.over_pair(in_weight.at[in_rows, in_cols], in_here, piece_sem.at[1], piece_got.at[1]),
        p.over_pair(down_mine, down_other, piece_sem.at[2], piece_got.at[2]),
    ]
    next_z = p.me + 4 - p.z % 2 * 8
    in_share = p.copy(in_here, in_here, piece_sem.at[4], piece_got.at[4], next_z)
    out_rest = out_pair.at[1 - p.pair, part_half]
    share = p.copy(out_rest, out_rest, piece_sem.at[3], piece_got.at[3], p.slot(p.z, p.x, 1 - p.core))
    for part in range(3):
        here, own, away = part_copies(part)

        @pl.when(here)
        def _():
            own.start()

    p.meet()
    for part in range(3):
        here, own, away = part_copies(part)

        @pl.when(here)
        def _():
            away.start()

    for at in (1, 0, 2):
        swaps[at].start()
    resid = tokens[...].astype(f32)
    normed, inv = normalize(resid)
    normed_a[...], inv_a[...] = normed, inv
    act_all[p.me] = (normed * gain_attn[...]).astype(bf16)
    for load in loads:
        load.wait()

    first.part(0)
    position = lax.broadcasted_iota(jnp.int32, cos.shape, 1).astype(f32)
    entry = lax.broadcasted_iota(jnp.int32, (cos.shape[0], 1), 0).astype(f32)
    angles = position * jnp.exp(entry * (-2.0 * math.log(ROPE_BASE) / head))
    cos[...], sine[...] = jnp.cos(angles), jnp.sin(angles)
    for part in range(3):
        here, own, away = part_copies(part)

        @pl.when(here)
        def _():
            own.wait()

        @pl.when(jnp.logical_not(here))
        def _():
            away.wait_recv()

    head_weight = weight[...].reshape(3 * head, width)

    def project(z, x, core):
        at = p.slot(z, x, core)
        lanes = pl.ds(pl.multiple_of(at * rows, rows), rows)
        packed = matmul(head_weight, act_all[at], 1, 1)
        c, s = cos[:, lanes], sine[:, lanes]
        query, key = packed[:head], packed[head : 2 * head]
        query_t[:, lanes] = rotate_rows(query, c, s).astype(bf16)
        key = rotate_rows(key, c, s)
        keys_t[:, lanes] = key.astype(bf16)
        values_t[:, lanes] = packed[2 * head :].astype(bf16)
        keys[lanes, :] = key.T.astype(bf16)
        values[lanes, :] = packed[2 * head :].T.astype(bf16)

    project(p.z, p.x, p.core)

    @pl.loop(4, 4 * p.line + 4)
    def _(at):
        first.part(at, project)

    second.start()
    swaps[1].wait_recv()
    in_share.start()
    wide = 2 * rows
    blocks = count // 2
    scale = head ** (-0.5)

    def attend(i):
        block = (p.me // 2 + i) % blocks
        lanes = pl.ds(pl.multiple_of(block * wide, wide), wide)
        scores = matmul(keys[...], query_t[:, lanes], 1, 0) * scale
        top = jnp.max(scores, axis=0, keepdims=True)
        weights = jnp.exp(scores - top)
        total = jnp.sum(weights, axis=0, keepdims=True)
        log_sum[:, lanes] = top + jnp.log(total)
        out = (matmul(values_t[...], weights.astype(bf16), 1, 0) / total).astype(bf16)
        mixed_own[2 * block] = out[:, :rows]
        mixed_own[2 * block + 1] = out[:, rows:]
        trade.send(2 * block)
        trade.send(2 * block + 1)

    @pl.loop(0, blocks // 2)
    def _(i):
        attend(i)

    second.relay()
    swaps[0].wait_recv()
    share.start()

    @pl.loop(blocks // 2, blocks)
    def _(i):
        attend(i)

    trade.arrived()
    share.wait_recv()
    flat = mixed[...].reshape(width, rows)
    total = tokens[...].astype(f32) + matmul(flat, out_pair[...].reshape(width, width), 0, 1)
    middle[...] = total
    normed, inv = normalize(total)
    normed_m[...], inv_m[...] = normed, inv
    act_m[...] = (normed * gain_mlp[...]).astype(bf16)
    second.beside().wait_recv()
    second.beside_next().wait_recv()
    swaps[2].wait_recv()
    first.sent()
    second.sent()
    trade.sent()
    for part in range(3):
        here, own, away = part_copies(part)

        @pl.when(here)
        def _():
            away.wait_send()

    for swap in swaps:
        swap.wait_send()
    share.wait_send()
    in_share.wait()


def feed_kernel(
    count, act, cot_all, in_weight, in_other, down_mine, down_other, gain, out_pair, normed, inv, middle,
    output, grad_middle, grad_mid, grad_mixed, in_grad, down_grad,
    grad_act, out_total, weight, down, act_all, gated, inner_grad, grad_part, out_part, load_sem, *rest
):
    f32, bf16 = jnp.float32, jnp.bfloat16
    p = Place(count)
    rows, group = act.shape[0], down.shape[1]
    gather = Quad(p, act_all, rest[:2])
    grad_sum = QuadSum(p, grad_part, rest[2:5], rest[8:10])
    out_sum = QuadSum(p, out_part, rest[5:8], rest[10:12])
    units, half = in_other.shape[0], down_other.shape[0]
    in_rows = pl.ds(pl.multiple_of((p.x * 2 + p.core) * units, 16), units)
    own_at = pl.ds(pl.multiple_of(p.pair * group, group), units)
    other_at = pl.ds(pl.multiple_of((1 - p.pair) * group, group), units)
    load = pltpu.make_async_copy(act, act_all.at[p.x * 2 + p.core], load_sem.at[0])
    weights = [
        pltpu.make_async_copy(in_weight.at[in_rows], weight.at[own_at], load_sem.at[1]),
        pltpu.make_async_copy(in_other, weight.at[other_at], load_sem.at[2]),
    ]
    load.start()
    for copy in weights:
        copy.start()
    p.meet()
    load.wait()
    gather.start()
    down[...] = jnp.zeros_like(down)
    down[pl.ds(pl.multiple_of(p.pair * half, half), half), :units] = down_mine[...]
    down[pl.ds(pl.multiple_of((1 - p.pair) * half, half), half), :units] = down_other[...]
    for at in range(2):
        weight[at * group + units : (at + 1) * group, :] = jnp.zeros((group - units, weight.shape[1]), bf16)
    for copy in weights:
        copy.wait()
    gather.beside().wait_recv()

    @pl.loop(0, 2)
    def _(step):
        x = jnp.where(step == 0, p.x, 1 - p.x)

        @pl.when(step == 1)
        def _():
            gather.relay()
            gather.beside_next().wait_recv()

        acts = jnp.concatenate([act_all[2 * x], act_all[2 * x + 1]], axis=0)
        cots = jnp.concatenate([cot_all[2 * x], cot_all[2 * x + 1]], axis=0)
        inner = matmul(acts, weight[...], 1, 1)
        grad_gated = matmul(cots, down[...], 1, 0)
        value, gate = inner[:, :group], inner[:, group:]
        gelu_val, gelu_slope = gelu_pair(value)
        token = pl.ds(pl.multiple_of(x * 2 * rows, 2 * rows), 2 * rows)
        out = (gelu_val * gate).astype(bf16)
        gated[token, :] = out
        grads = jnp.concatenate(
            [grad_gated * gate * gelu_slope, grad_gated * gelu_val], axis=1
        ).astype(bf16)
        inner_grad[token, :] = grads
        part = matmul(grads, weight[...], 1, 0).astype(bf16)
        grad_part[2 * x], grad_part[2 * x + 1] = part[:rows], part[rows:]
        grad_sum.beside(x).start()
        part = matmul(out, down[...], 1, 1).astype(bf16)
        out_part[2 * x], out_part[2 * x + 1] = part[:rows], part[rows:]
        out_sum.beside(x).start()

    grad_sum.add(1 - p.x)
    grad_sum.across().start()
    grad_sum.add(p.x)
    out_sum.add(1 - p.x)
    out_sum.across().start()
    out_sum.add(p.x)
    acts = act_all[...].reshape(4 * rows, act.shape[1])
    cots = cot_all[...].reshape(4 * rows, act.shape[1])
    quarter = units // 4
    gain_row = jnp.zeros((1, act.shape[1]), f32)
    for at in range(2):
        piece = matmul(inner_grad[:, at * group : (at + 1) * group], acts, 0, 0)
        gain_row += jnp.sum(piece * weight[at * group : (at + 1) * group, :].astype(f32), axis=0, keepdims=True)
        for k in range(4):
            in_grad[k % 2 * p.line + at * 2 + k // 2] = piece[k * quarter : (k + 1) * quarter].astype(bf16)
    piece = matmul(cots, gated[...], 0, 0)
    lane = lax.broadcasted_iota(jnp.int32, piece.shape, 1)
    gain_row = gain_row / gain[...]
    column = jnp.broadcast_to(gain_row, (8, gain_row.shape[1])).T[:, :1]
    piece = jnp.where(lane == units, column, piece).astype(bf16)
    unit = act.shape[1] // (2 * count)
    for z in range(p.line):
        for r in range(4):
            for y in range(2):
                start = ((z * 4 + r) * 2 + y) * unit
                down_grad[y * p.line + z, r] = piece[start : start + unit]
    grad_sum.finish(grad_act)
    cot = cot_all[p.x * 2 + p.core].astype(f32)
    grad = cot + norm_back(grad_act[...] * gain[...], normed[...], inv[...])
    grad_middle[...] = grad
    grad_mid[...] = grad.astype(bf16)
    width = act.shape[1]
    back = matmul(grad_mid[...], out_pair[...].reshape(width, width), 1, 0)
    grad_mixed[...] = back.T.astype(bf16).reshape(grad_mixed.shape)
    out_sum.finish(out_total)
    output[...] = middle[...] + out_total[...]
    gather.sent()
    grad_sum.sent()
    out_sum.sent()


def attend_back_kernel(
    count, grad_mixed, grad_mid, mixed, query_t, keys_t, keys, values, mixed_own, log_sum,
    act_all, weight, cos, sine, in_grad, down_grad, gain, grad_middle, normed, inv,
    grad_input, qkv_out, out_out, in_out, down_out, gain_m_out, gain_a_out,
    grad_act, grad_own, grad_keys, grad_values, grad_packed, grad_part, grad_got, grad_sums, grad_weight,
    pair_part, pair_core, pair_sums, pair_got, proj_sums, in_sum, in_got, down_sum, down_got,
    qkv_part, qkv_got, gain_part, gain_got,
    pair_s, pair_r, in_s, in_r, down_s, down_r, qkv_s, qkv_r, *rest
):
    f32, bf16 = jnp.float32, jnp.bfloat16
    p = Place(count)
    rows, head = grad_mixed.shape[2], keys_t.shape[0]
    width, unit = count * head, head // 2
    bufs, proj_bufs, in_bufs, down_bufs, sems = rest[:4], rest[4:8], rest[8:12], rest[12:16], rest[16:]
    trade = Exchange(p, grad_mixed, grad_own, sems[:2])
    halve = Halve(p, grad_part, grad_got, grad_sums, sems[2:4])
    settle = Settle(p, grad_sums, bufs, sems[4:10])
    halve_proj = Halve(p, pair_part, pair_core, pair_sums, sems[10:12])
    settle_proj = Settle(p, proj_sums, proj_bufs, sems[12:18])
    settle_in = Settle(p, in_grad, in_bufs, sems[18:24], True)
    settle_down = Settle(p, down_grad, down_bufs, sems[24:30], True)
    spread_gain = Spread(p, gain_part, gain_got, sems[30:32])
    give_in = Deliver(p, in_sum, in_got, (in_s, in_r))
    give_down = Deliver(p, down_sum, down_got, (down_s, down_r))
    give_qkv = Deliver(p, qkv_part, qkv_got, (qkv_s, qkv_r))

    def swap(at):
        return p.over_pair(pair_sums.at[at, 1 - p.pair], pair_got.at[at], pair_s.at[at], pair_r.at[at])

    p.meet(True)

    @pl.loop(0, count)
    def _(shift):
        trade.send((p.me + shift) % count)

    settle_in.across(p.far(0)).start()
    settle_down.across(p.far(0)).start()
    flat = mixed[...].reshape(width, rows)

    @pl.loop(0, count // 2)
    def _(i):
        lanes = pl.ds(pl.multiple_of(i * 4 * unit, 4 * unit), 4 * unit)
        piece = matmul(grad_mid[:, lanes], flat, 0, 1).astype(bf16)
        for at in range(4):
            pair_part[2 * i + at // 2, at % 2] = piece[at * unit : (at + 1) * unit]

    @pl.loop(0, 2 * p.line)
    def _(at):
        halve_proj.beside(at // 2, at % 2).start()

    @pl.loop(0, p.line)
    def _(step):
        z = p.far(step)
        halve_proj.add(z)
        swap(2 * z).start()
        swap(2 * z + 1).start()

    @pl.loop(1, p.line)
    def _(step):
        settle_in.across(p.far(step)).start()
        settle_down.across(p.far(step)).start()

    grad_keys[...] = jnp.zeros_like(grad_keys)
    grad_values[...] = jnp.zeros_like(grad_values)
    trade.arrived()
    wide = 2 * rows
    scale = head ** (-0.5)

    def back(i):
        lanes = pl.ds(pl.multiple_of(i * wide, wide), wide)
        query = query_t[:, lanes]
        grad = jnp.concatenate([grad_own[2 * i], grad_own[2 * i + 1]], axis=1)
        own = jnp.concatenate([mixed_own[2 * i], mixed_own[2 * i + 1]], axis=1)
        delta = jnp.sum(grad.astype(f32) * own.astype(f32), axis=0, keepdims=True)
        scores = matmul(keys[...], query, 1, 0) * scale
        probs = jnp.exp(scores - log_sum[:, lanes])
        grad_values[...] += matmul(probs.astype(bf16), grad, 1, 1)
        grad_probs = matmul(values[...], grad, 1, 0)
        grad_scores = (probs * (grad_probs - delta)).astype(bf16)
        grad_keys[...] += matmul(grad_scores, query, 1, 1)
        grad_query = matmul(keys_t[...], grad_scores, 1, 0) * scale
        back_query = rotate_rows_back(grad_query, cos[:, lanes], sine[:, lanes])
        grad_packed[:head, lanes] = back_query.astype(bf16)

    @pl.loop(0, count // 2)
    def _(i):
        back(i)

    grad_key = grad_keys[...].T * scale
    grad_packed[head : 2 * head, :] = rotate_rows_back(grad_key, cos[...], sine[...]).astype(bf16)
    grad_packed[2 * head :, :] = grad_values[...].T.astype(bf16)

    @pl.loop(0, p.line)
    def _(step):
        z = p.far(step)
        for at in range(4):
            lanes = pl.ds(pl.multiple_of((z * 4 + at) * rows, rows), rows)
            grad_part[z * 4 + at] = matmul(grad_packed[:, lanes], weight[...], 0, 0).astype(bf16)
        halve.beside(z, 0).start()
        halve.beside(z, 1).start()

    @pl.loop(0, p.line)
    def _(step):
        z = p.far(step)
        halve.add(z)
        settle.across(z).start()

    @pl.loop(0, p.line)
    def _(step):
        z = p.far(step)
        for x in range(2):
            at = 2 * z + x
            swap(at).wait_recv()
            proj_sums[at] = (pair_sums[at, p.pair].astype(f32) + pair_got[at].astype(f32)).astype(bf16)
        settle_proj.across(z).start()

    settle_in.pass_on(p.far(0))
    settle_down.pass_on(p.far(0))

    def grad_chunk(step):
        lanes = pl.ds(pl.multiple_of(step * 4 * rows, 4 * rows), 4 * rows)
        acts = jnp.concatenate([act_all[4 * step + i] for i in range(4)], axis=0)
        return matmul(grad_packed[:, lanes], acts, 1, 0)

    grad_weight[...] = grad_chunk(0)

    @pl.loop(1, p.line)
    def _(step):
        grad_weight[...] += grad_chunk(step)

    for at in range(6):
        qkv_part[at] = grad_weight[at * unit : (at + 1) * unit, :].astype(bf16)
    gain_row = jnp.sum(grad_weight[...] * weight[...].astype(f32), axis=0, keepdims=True) / gain[...]
    for at in range(2 * count):
        chunk = at * unit // 128 * 128
        gain_part[at] = gain_row[:, chunk : chunk + 128]

    def unit_of(at):
        return (at // 2) * 2 * count + 2 * p.me + at % 2

    for at in range(6):
        give_qkv.send(at, unit_of(at) // 3, unit_of(at) % 3 * 2 + p.pair)
    spread_gain.send()

    @pl.loop(0, p.line)
    def _(step):
        z = p.far(step)
        settle.pass_on(z)
        settle_proj.pass_on(z)

        @pl.when(step == 1)
        def _():
            settle_in.pass_on(z)
            settle_down.pass_on(z)

    @pl.loop(2, p.line)
    def _(step):
        settle_in.pass_on(p.far(step))
        settle_down.pass_on(p.far(step))

    units = in_out.shape[0]
    r = p.x * 2 + p.core
    piece_owner = p.z // 2 * count + r * 4 + p.z % 2 * 2 + p.pair
    settle_in.finish(in_sum.at[0])
    give_in.send(0, piece_owner, 0)
    settle_down.finish(down_sum)
    for at in range(4):
        give_down.send(at, (p.z * 4 + at) * 2 + p.pair, r)
    for slot in range(3):
        source = (3 * p.owner + slot) % (2 * count) // 2 * 2
        for side in range(2):
            give_qkv.arrived(2 * slot + side, source + side)
        qkv_out[slot * unit : (slot + 1) * unit, :] = qkv_got[2 * slot].astype(f32) + qkv_got[2 * slot + 1].astype(f32)
    spread_gain.arrived()
    gain_a = gain_got[0]
    for at in range(1, 2 * count):
        gain_a += gain_got[at]
    chunks = 128 // unit
    gain_a_out[...] = sum(
        jnp.where(p.owner % chunks == at, gain_a[:, at * unit : (at + 1) * unit], 0.0) for at in range(chunks)
    )
    settle_proj.finish(out_out)
    settle.finish(grad_act)
    grad_input[...] = grad_middle[...] + norm_back(grad_act[...] * gain[...], normed[...], inv[...])
    half, r_of, k_of = p.owner // count, p.owner % count // 4, p.owner % 4
    source_in = ((half * 2 + k_of // 2) * 4 + r_of) * 2 + k_of % 2
    give_in.arrived(0, source_in)
    in_out[...] = in_got[0].astype(f32)
    gain_m = jnp.zeros((unit, 1), f32)
    group = 4 * units
    for at in range(4):
        give_down.arrived(at, (p.z * 4 + at) * 2 + p.pair)
        block = down_got[at].astype(f32)
        down_out[:, at * group : (at + 1) * group] = block[:, :group]
        gain_m += block[:, group : group + 1]
    gain_m_out[...] = jnp.broadcast_to(gain_m, (unit, 128)).T[:1]
    trade.sent()
    halve.sent()
    settle.sent()
    halve_proj.sent()
    settle_proj.sent()
    settle_in.sent()
    settle_down.sent()
    spread_gain.sent()

    @pl.loop(0, 2 * p.line)
    def _(at):
        swap(at).wait_send()

    give_in.sent(0, piece_owner, 0)
    for at in range(4):
        give_down.sent(at, (p.z * 4 + at) * 2 + p.pair, r)
    for at in range(6):
        give_qkv.sent(at, unit_of(at) // 3, unit_of(at) % 3 * 2 + p.pair)


def run_kernel(body, outs, scratch, collective, flops, args, outside=(), outs_outside=()):
    vmem, anywhere = pl.BlockSpec(memory_space=pltpu.VMEM), pl.BlockSpec(memory_space=pl.ANY)
    return pl.pallas_call(
        body,
        out_shape=outs,
        in_specs=[anywhere if i in outside else vmem for i in range(len(args))],
        out_specs=[anywhere if i in outs_outside else vmem for i in range(len(outs))],
        scratch_shapes=scratch,
        compiler_params=pltpu.CompilerParams(
            collective_id=collective, has_side_effects=True, vmem_limit_bytes=VMEM_LIMIT
        ),
        cost_estimate=pl.CostEstimate(flops=flops, bytes_accessed=20_000_000, transcendentals=0),
        name=body.func.__name__,
    )(*args)


def shaped(shape, kind):
    return jax.ShapeDtypeStruct(shape, kind)


def attend(count, head, tokens, cot, gain_attn, gain_mlp, qkv_weight, in_weight, down_mine, out_mine):
    bf16, f32 = jnp.bfloat16, jnp.float32
    rows, width = tokens.shape
    length, line = rows * count, count // 4
    blocks = shaped((count, rows, width), bf16)
    tall, flat = shaped((head, length), bf16), shaped((length, head), bf16)
    heads = shaped((count, head, rows), bf16)
    block, column, table = shaped((rows, width), f32), shaped((rows, 1), f32), shaped((head // 2, length), f32)
    pairs = [shaped((in_weight.shape[0] // 4, width), bf16), shaped(down_mine.shape, bf16), shaped((2,) + out_mine.shape, bf16)]
    three, six = pltpu.SemaphoreType.DMA((3,)), pltpu.SemaphoreType.DMA((6,))
    return run_kernel(
        functools.partial(attend_kernel, count),
        [block, column, block, column, block, shaped((rows, width), bf16), table, table,
         blocks, shaped((4, rows, width), bf16), tall, tall, flat, flat, heads, shaped((1, length), f32), heads,
         shaped((3, head, width), bf16)] + pairs,
        [pltpu.VMEM((head, length), bf16), pltpu.SemaphoreType.DMA((6,))] + [three, three, six, six]
        + Gather.sems(line) + Quad.sems() + Exchange.sems(count),
        0, 10_000_000_000, [tokens, cot, gain_attn, gain_mlp, qkv_weight, in_weight, down_mine, out_mine], (4, 5, 6, 7),
        (18, 19),
    )


def feed(count, group, act, cot_all, in_weight, in_other, down_mine, down_other, gain, out_pair, normed, inv, middle):
    bf16, f32 = jnp.bfloat16, jnp.float32
    rows, width = act.shape
    block = (rows, width)
    units, line, unit = in_other.shape[0], count // 4, width // (2 * count)
    whole = pltpu.VMEM((4,) + block, bf16)
    return run_kernel(
        functools.partial(feed_kernel, count),
        [shaped(block, f32), shaped(block, f32), shaped(block, bf16), shaped((count, width // count, rows), bf16),
         shaped((2 * line, units // 4, width), bf16), shaped((2 * line, 4, unit, group), bf16)],
        [pltpu.VMEM(block, f32), pltpu.VMEM(block, f32), pltpu.VMEM((2 * group, width), bf16), pltpu.VMEM((width, group), bf16),
         whole, pltpu.VMEM((4 * rows, group), bf16), pltpu.VMEM((4 * rows, 2 * group), bf16), whole, whole,
         pltpu.SemaphoreType.DMA((3,))]
        + Quad.sems() + QuadSum.bufs(block) * 2 + QuadSum.sems() * 2,
        1, 20_000_000_000, [act, cot_all, in_weight, in_other, down_mine, down_other, gain, out_pair, normed, inv, middle], (2, 3),
    )


def attend_back(count, grad_mixed, grad_mid, mixed, kept, act_all, weight, cos, sine, in_grad, down_grad, gain, grad_middle, normed, inv):
    bf16, f32 = jnp.bfloat16, jnp.float32
    rows, width = act_all.shape[1:]
    head, length, line = weight.shape[0] // 3, rows * count, count // 4
    block, unit, units = (rows, width), head // 2, in_grad.shape[1]
    down_block = down_grad.shape[1:]
    piece = (unit, width)

    def held(*shape):
        return pltpu.VMEM(shape, bf16)

    whole, half = held(count, *block), held(2 * line, *block)
    flat = pltpu.VMEM((length, head), f32)
    one, four, six, many = [pltpu.SemaphoreType.DMA((n,)) for n in (1, 4, 6, 2 * line)]
    return run_kernel(
        functools.partial(attend_back_kernel, count),
        [shaped(block, f32), shaped((3 * unit, width), f32), shaped(piece, f32),
         shaped((units, width), f32), shaped((unit, units * count), f32), shaped((1, unit), f32), shaped((1, unit), f32)],
        [pltpu.VMEM(block, f32), held(count, head, rows), flat, flat, held(3 * head, length), whole, half, half,
         pltpu.VMEM((3 * head, width), f32),
         held(count, 2, *piece), held(2 * line, 2, *piece), held(2 * line, 2, *piece), held(2 * line, *piece),
         held(2 * line, *piece), held(1, units, width), held(1, units, width), held(*down_block), held(*down_block),
         held(6, *piece), held(6, *piece), pltpu.VMEM((2 * count, 1, 128), f32), pltpu.VMEM((2 * count, 1, 128), f32),
         many, many, one, one, four, four, six, six]
        + Settle.bufs(line, block) + Settle.bufs(line, piece)
        + Settle.bufs(line, (units, width)) + Settle.bufs(line, down_block)
        + Exchange.sems(count) + (Halve.sems(line) + Settle.sems(line)) * 2
        + Settle.sems(line) * 2 + Spread.sems(count),
        2, 20_000_000_000,
        [grad_mixed, grad_mid, mixed, *kept, act_all, weight, cos, sine, in_grad, down_grad, gain,
         grad_middle, normed, inv],
    )


def publish_kernel(*refs):
    half = len(refs) // 2
    for src, dst in zip(refs[:half], refs[half:]):
        dst[...] = src[...]


def publish(arrays):
    vmem = pl.BlockSpec(memory_space=pltpu.VMEM)
    return pl.pallas_call(
        publish_kernel,
        out_shape=[shaped(array.shape, array.dtype) for array in arrays],
        in_specs=[vmem] * len(arrays),
        out_specs=[vmem] * len(arrays),
        compiler_params=pltpu.CompilerParams(vmem_limit_bytes=VMEM_LIMIT),
    )(*arrays)


def tensor_layer(
    tokens, cotangent, gain_attn, gain_mlp, qkv_weight, out_weight, in_weight, down_weight
):
    count = lax.axis_size("ctx")
    index = lax.axis_index("ctx")
    width = tokens.shape[2]
    head_size = width // count
    group = in_weight.shape[0] // 4
    padded = (group // 128 + 1) * 128

    down_mine = lax.dynamic_slice_in_dim(down_weight, lax.rem(index, 4) * group, group, 1)
    (
        normed_a, inv_a, normed_m, inv_m, middle, act_m, cos, sine, act_all, cot_all, *kept,
        mixed, qkv_head, in_other, down_other, out_pair,
    ) = attend(
        count, head_size, tokens[0], cotangent[0], gain_attn[None], gain_mlp[None],
        qkv_weight, in_weight, down_mine, out_weight,
    )
    output, grad_middle, grad_mid, grad_mixed, in_grad, down_grad = feed(
        count, padded, act_m, cot_all, in_weight, in_other, down_mine, down_other, gain_mlp[None],
        out_pair, normed_m, inv_m, middle,
    )
    grad_input, grad_qkv, grad_out, grad_in, grad_down, grad_gain_m, grad_gain_a = attend_back(
        count, grad_mixed, grad_mid, mixed, kept, act_all, qkv_head.reshape(3 * head_size, width), cos, sine,
        in_grad, down_grad, gain_attn[None], grad_middle, normed_a, inv_a,
    )
    output, grad_input, grad_qkv, grad_out, grad_in, grad_down, grad_gain_a, grad_gain_m = publish(
        [output, grad_input, grad_qkv, grad_out, grad_in, grad_down, grad_gain_a, grad_gain_m]
    )
    return (output[None], grad_input[None], grad_qkv, grad_out, grad_in, grad_down, grad_gain_a[0], grad_gain_m[0])


def solution(mesh):

    def layer(*arrays):
        one_head_each = arrays[0].shape[2] == HEAD_DIM * mesh.shape["ctx"]
        if one_head_each and mesh.shape["fsdp"] == 2 and mesh.shape["ctx"] % 4 == 0:
            return tensor_layer(*arrays)
        return gathered_layer(*arrays)

    return jax.shard_map(
        layer,
        mesh=mesh,
        in_specs=(
            P("fsdp", "ctx", None),
            P("fsdp", "ctx", None),
            P(),
            P(),
            P("fsdp", None),
            P("fsdp", None),
            P("fsdp", None),
            P("fsdp", None),
        ),
        out_specs=(
            P("fsdp", "ctx", None),
            P("fsdp", "ctx", None),
            P(("ctx", "fsdp"), None),
            P(("ctx", "fsdp"), None),
            P(("ctx", "fsdp"), None),
            P(("ctx", "fsdp"), None),
            P(("ctx", "fsdp")),
            P(("ctx", "fsdp")),
        ),
        check_vma=False,
    )
```

```python
import functools
import math

import jax
import jax.numpy as jnp
from jax import lax
from jax.experimental import pallas as pl
from jax.experimental.pallas import tpu as pltpu
from jax.sharding import PartitionSpec as P

HEAD_DIM = 64


EPSILON = 1e-05
ROPE_BASE = 160000.0


def normalize(tensor):
    centred = tensor - jnp.mean(tensor, axis=-1, keepdims=True)
    inv_std = lax.rsqrt(jnp.mean(centred * centred, axis=-1, keepdims=True) + EPSILON)
    return (centred * inv_std, inv_std)


def norm_back(grad_norm, normed, inv_std):
    return inv_std * (
        grad_norm
        - jnp.mean(grad_norm, axis=-1, keepdims=True)
        - normed * jnp.mean(grad_norm * normed, axis=-1, keepdims=True)
    )


def gelu_pair(tensor):
    cumul = 0.5 * (1.0 + jax.scipy.special.erf(tensor * 0.7071067811865476))
    density = jnp.exp(-0.5 * tensor * tensor) * 0.3989422804014327
    return (tensor * cumul, cumul + tensor * density)


def rope_tables(offset, length, head_size):
    positions = (offset + jnp.arange(length, dtype=jnp.int32)).astype(jnp.float32)
    inverse = ROPE_BASE ** (
        -jnp.arange(0, head_size, 2, dtype=jnp.int32).astype(jnp.float32) / head_size
    )
    angles = positions[:, None] * inverse[None, :]
    angles = jnp.concatenate([angles, angles], axis=-1)
    return (jnp.cos(angles)[:, None, :], jnp.sin(angles)[:, None, :])


def rotate(tensor, cos_table, sine_table):
    middle = tensor.shape[-1] // 2
    turned = jnp.concatenate([-tensor[..., middle:], tensor[..., :middle]], axis=-1)
    return tensor * cos_table + turned * sine_table


def rotate_back(gradient, cos_table, sine_table):
    middle = gradient.shape[-1] // 2
    scaled = gradient * sine_table
    turned = jnp.concatenate([scaled[..., middle:], -scaled[..., :middle]], axis=-1)
    return gradient * cos_table + turned


def rows_product(left, right):
    return lax.dot_general(
        left, right, (((1,), (1,)), ((), ())), preferred_element_type=jnp.float32
    )


def rows_contract(left, right):
    return lax.dot_general(
        left, right, (((0,), (0,)), ((), ())), preferred_element_type=jnp.float32
    )


def gathered_layer(
    tokens, cotangent, gain_attn, gain_mlp, qkv_weight, out_weight, in_weight, down_weight
):
    f32 = jnp.float32
    bf16 = jnp.bfloat16
    qkv_full, out_full, in_full, down_full = (
        lax.all_gather(qkv_weight, "fsdp", axis=0, tiled=True),
        lax.all_gather(out_weight, "fsdp", axis=0, tiled=True),
        lax.all_gather(in_weight, "fsdp", axis=0, tiled=True),
        lax.all_gather(down_weight, "fsdp", axis=0, tiled=True),
    )
    tok_rows = tokens.shape[1]
    width = tokens.shape[2]
    hidden = down_full.shape[1]
    head_size = HEAD_DIM
    head_count = width // head_size
    scale = head_size ** (-0.5)
    offset = lax.axis_index("ctx") * tok_rows
    cos_table, sine_table = rope_tables(offset, tok_rows, head_size)
    resid = tokens[0].astype(f32)
    normed_a, inv_a = normalize(resid)
    act_a = (normed_a * gain_attn).astype(bf16)
    packed = rows_product(act_a, qkv_full)
    query_heads = rotate(
        packed[:, :width].reshape(tok_rows, head_count, head_size), cos_table, sine_table
    ).astype(bf16)
    key_heads = rotate(
        packed[:, width : 2 * width].reshape(tok_rows, head_count, head_size), cos_table, sine_table
    ).astype(bf16)
    value_send = packed[:, 2 * width :].astype(bf16)
    key_send = key_heads.reshape(tok_rows, width)
    value_heads = value_send.reshape(tok_rows, head_count, head_size)
    start_state = (
        jnp.zeros((tok_rows, head_count, head_size), f32),
        jnp.full((head_count, tok_rows), -1e30, f32),
        jnp.zeros((head_count, tok_rows), f32),
    )
    key_piece = lax.all_gather(key_send, "ctx", axis=0, tiled=True)
    value_piece = lax.all_gather(value_send, "ctx", axis=0, tiled=True)
    length = key_piece.shape[0]
    step_len = math.gcd(length, 1024)

    def attend_block(block_num, running):
        weighted, row_max, row_sum = running
        key_blk = lax.dynamic_slice_in_dim(key_piece, block_num * step_len, step_len, 0).reshape(
            step_len, head_count, head_size
        )
        value_blk = lax.dynamic_slice_in_dim(
            value_piece, block_num * step_len, step_len, 0
        ).reshape(step_len, head_count, head_size)
        scores = (
            jnp.einsum("qhd,khd->hqk", query_heads, key_blk, preferred_element_type=f32) * scale
        )
        new_max = jnp.maximum(row_max, jnp.max(scores, axis=-1))
        shrink = jnp.exp(row_max - new_max)
        weights = jnp.exp(scores - new_max[..., None])
        row_sum = row_sum * shrink + jnp.sum(weights, axis=-1)
        weighted = weighted * shrink.T[:, :, None] + jnp.einsum(
            "hqk,khd->qhd", weights.astype(bf16), value_blk, preferred_element_type=f32
        )
        return (weighted, new_max, row_sum)

    weighted, row_max, row_sum = lax.fori_loop(0, length // step_len, attend_block, start_state)
    log_sum = row_max + jnp.log(row_sum)
    mixed = (weighted / row_sum.T[:, :, None]).reshape(tok_rows, width).astype(bf16)
    middle = resid + rows_product(mixed, out_full)
    normed_m, inv_m = normalize(middle)
    act_m = (normed_m * gain_mlp).astype(bf16)
    inner = rows_product(act_m, in_full)
    gelu_val, gelu_slope = gelu_pair(inner[:, :hidden])
    gated = (gelu_val * inner[:, hidden:]).astype(bf16)
    output = middle + rows_product(gated, down_full)
    cot_rows = cotangent[0]
    grad_down = rows_contract(cot_rows, gated)
    grad_gated = jnp.dot(cot_rows, down_full, preferred_element_type=f32)
    grad_inner = jnp.concatenate(
        [grad_gated * inner[:, hidden:] * gelu_slope, grad_gated * gelu_val], axis=1
    ).astype(bf16)
    grad_in = rows_contract(grad_inner, act_m)
    grad_act_m = jnp.dot(grad_inner, in_full, preferred_element_type=f32)
    grad_gain_m = jnp.sum(grad_act_m * normed_m, axis=0)
    grad_middle = cot_rows.astype(f32) + norm_back(grad_act_m * gain_mlp, normed_m, inv_m)
    grad_mid_bf = grad_middle.astype(bf16)
    grad_out = rows_contract(grad_mid_bf, mixed)
    grad_mixed = jnp.dot(grad_mid_bf, out_full, preferred_element_type=f32).astype(bf16)
    grad_heads = grad_mixed.reshape(tok_rows, head_count, head_size)
    delta_rows = jnp.sum(
        grad_heads.astype(f32) * mixed.reshape(tok_rows, head_count, head_size).astype(f32), axis=-1
    )
    delta = delta_rows.T
    zeros_heads = jnp.zeros((tok_rows, head_count, head_size), f32)
    query_key_piece = lax.all_gather(key_send, "ctx", axis=0, tiled=True)
    query_value_piece = lax.all_gather(value_send, "ctx", axis=0, tiled=True)
    length = query_key_piece.shape[0]
    query_step_len = math.gcd(length, 1024)

    def query_grad_block(block_num, grad_query):
        key_blk = lax.dynamic_slice_in_dim(
            query_key_piece, block_num * query_step_len, query_step_len, 0
        ).reshape(query_step_len, head_count, head_size)
        value_blk = lax.dynamic_slice_in_dim(
            query_value_piece, block_num * query_step_len, query_step_len, 0
        ).reshape(query_step_len, head_count, head_size)
        scores = (
            jnp.einsum("qhd,khd->hqk", query_heads, key_blk, preferred_element_type=f32) * scale
        )
        probs = jnp.exp(scores - log_sum[..., None])
        grad_probs = jnp.einsum("qhd,khd->hqk", grad_heads, value_blk, preferred_element_type=f32)
        grad_scores = (probs * (grad_probs - delta[..., None])).astype(bf16)
        return (
            grad_query
            + jnp.einsum("hqk,khd->qhd", grad_scores, key_blk, preferred_element_type=f32) * scale
        )

    grad_query = lax.fori_loop(0, length // query_step_len, query_grad_block, zeros_heads)
    query_send = query_heads.reshape(tok_rows, width).astype(f32)
    grad_send = grad_mixed.astype(f32)
    query_piece = lax.all_gather(query_send, "ctx", axis=0, tiled=True)
    grad_piece = lax.all_gather(grad_send, "ctx", axis=0, tiled=True)
    log_piece = lax.all_gather(log_sum.T, "ctx", axis=0, tiled=True)
    delta_piece = lax.all_gather(delta_rows, "ctx", axis=0, tiled=True)
    length = query_piece.shape[0]
    key_step_len = math.gcd(length, 1024)

    def key_grad_block(block_num, running):
        grad_keys, grad_values = running
        query_blk = (
            lax.dynamic_slice_in_dim(query_piece, block_num * key_step_len, key_step_len, 0)
            .astype(bf16)
            .reshape(key_step_len, head_count, head_size)
        )
        grad_blk = (
            lax.dynamic_slice_in_dim(grad_piece, block_num * key_step_len, key_step_len, 0)
            .astype(bf16)
            .reshape(key_step_len, head_count, head_size)
        )
        log_blk = lax.dynamic_slice_in_dim(log_piece, block_num * key_step_len, key_step_len, 0).T
        delta_blk = lax.dynamic_slice_in_dim(
            delta_piece, block_num * key_step_len, key_step_len, 0
        ).T
        scores = (
            jnp.einsum("qhd,khd->hqk", query_blk, key_heads, preferred_element_type=f32) * scale
        )
        probs = jnp.exp(scores - log_blk[..., None])
        grad_values = grad_values + jnp.einsum(
            "hqk,qhd->khd", probs.astype(bf16), grad_blk, preferred_element_type=f32
        )
        grad_probs = jnp.einsum("qhd,khd->hqk", grad_blk, value_heads, preferred_element_type=f32)
        grad_scores = (probs * (grad_probs - delta_blk[..., None])).astype(bf16)
        grad_keys = (
            grad_keys
            + jnp.einsum("hqk,qhd->khd", grad_scores, query_blk, preferred_element_type=f32) * scale
        )
        return (grad_keys, grad_values)

    grad_keys, grad_values = lax.fori_loop(
        0, length // key_step_len, key_grad_block, (zeros_heads, zeros_heads)
    )
    grad_query = rotate_back(grad_query, cos_table, sine_table)
    grad_keys = rotate_back(grad_keys, cos_table, sine_table)
    grad_packed = jnp.concatenate(
        [
            grad_query.reshape(tok_rows, width),
            grad_keys.reshape(tok_rows, width),
            grad_values.reshape(tok_rows, width),
        ],
        axis=1,
    ).astype(bf16)
    grad_qkv = rows_contract(grad_packed, act_a)
    grad_act_a = jnp.dot(grad_packed, qkv_full, preferred_element_type=f32)
    grad_gain_a = jnp.sum(grad_act_a * normed_a, axis=0)
    grad_input = grad_middle + norm_back(grad_act_a * gain_attn, normed_a, inv_a)
    owned = (
        lax.psum_scatter(grad_qkv, ("ctx", "fsdp"), scatter_dimension=0, tiled=True),
        lax.psum_scatter(grad_out, ("ctx", "fsdp"), scatter_dimension=0, tiled=True),
        lax.psum_scatter(grad_in, ("ctx", "fsdp"), scatter_dimension=0, tiled=True),
        lax.psum_scatter(grad_down, ("ctx", "fsdp"), scatter_dimension=0, tiled=True),
        lax.psum_scatter(grad_gain_a, ("ctx", "fsdp"), scatter_dimension=0, tiled=True),
        lax.psum_scatter(grad_gain_m, ("ctx", "fsdp"), scatter_dimension=0, tiled=True),
    )
    return (
        output[None],
        grad_input[None],
        owned[0],
        owned[1],
        owned[2],
        owned[3],
        owned[4],
        owned[5],
    )


MESH = pl.DeviceIdType.MESH
VMEM_LIMIT = 60 * 1024 * 1024


def matmul(left, right, left_dim, right_dim):
    return lax.dot_general(
        left, right, (((left_dim,), (right_dim,)), ((), ())), preferred_element_type=jnp.float32
    )


class Place:
    def __init__(self, count):
        self.count, self.line = count, count // 4
        self.me, self.pair = lax.axis_index("ctx"), lax.axis_index("fsdp")
        self.owner = self.me * 2 + self.pair
        self.z, self.x, self.core = self.me // 4, self.me // 2 % 2, self.me % 2

    def slot(self, z, x, core):
        return z * 4 + x * 2 + core

    def far(self, step):
        last = self.line - 1
        low = 2 * self.z < self.line
        own = jnp.where(low, self.z, last - self.z)
        at = jnp.where(
            step < last - own, last - step, jnp.where(step == last, own, step - (last - own))
        )
        return jnp.where(low, at, last - at)

    def near(self, step):
        return self.far(self.line - 1 - step)

    def meet(self, everyone=False):
        barrier = pltpu.get_barrier_semaphore()

        @pl.loop(1, self.count)
        def _(shift):
            pl.semaphore_signal(
                barrier, inc=1, device_id={"ctx": (self.me + shift) % self.count}, device_id_type=MESH
            )

        if everyone:
            @pl.loop(0, self.count)
            def _(to):
                pl.semaphore_signal(
                    barrier, inc=1, device_id={"ctx": to, "fsdp": 1 - self.pair}, device_id_type=MESH
                )

            pl.semaphore_wait(barrier, 2 * self.count - 1)
        else:
            pl.semaphore_signal(barrier, inc=1, device_id={"fsdp": 1 - self.pair}, device_id_type=MESH)
            pl.semaphore_wait(barrier, self.count)

    def over_pair(self, src, dst, send, recv):
        return pltpu.make_async_remote_copy(
            src_ref=src, dst_ref=dst, send_sem=send, recv_sem=recv,
            device_id={"fsdp": 1 - self.pair}, device_id_type=MESH,
        )

    def to_owner(self, src, dst, send, recv, owner):
        return pltpu.make_async_remote_copy(
            src_ref=src, dst_ref=dst, send_sem=send, recv_sem=recv,
            device_id={"ctx": owner // 2, "fsdp": owner % 2}, device_id_type=MESH,
        )

    def copy(self, src, dst, send, recv, to):
        return pltpu.make_async_remote_copy(
            src_ref=src, dst_ref=dst, send_sem=send, recv_sem=recv,
            device_id={"ctx": to}, device_id_type=MESH,
        )


class Gather:
    def __init__(self, place, buf, sems):
        self.p, self.buf = place, buf
        self.up_s, self.up_r, self.dn_s, self.dn_r, self.x_s, self.x_r, self.c_s, self.c_r = sems

    @staticmethod
    def sems(line):
        return [pltpu.SemaphoreType.DMA((line,))] * 6 + [pltpu.SemaphoreType.DMA((2 * line,))] * 2

    def over(self, z, x, core, send, recv, to):
        at = self.buf.at[self.p.slot(z, x, core)]
        return self.p.copy(at, at, send, recv, to)

    def up(self, z):
        p = self.p
        return self.over(z, p.x, p.core, self.up_s.at[z], self.up_r.at[z], (p.me + 4) % p.count)

    def down(self, z):
        p = self.p
        return self.over(z, p.x, p.core, self.dn_s.at[z], self.dn_r.at[z], (p.me + p.count - 4) % p.count)

    def across(self, z):
        p = self.p
        return self.over(z, p.x, p.core, self.x_s.at[z], self.x_r.at[z], p.slot(p.z, 1 - p.x, p.core))

    def beside(self, z, x):
        p = self.p
        at = z * 2 + x
        return self.over(z, x, p.core, self.c_s.at[at], self.c_r.at[at], p.slot(p.z, p.x, 1 - p.core))

    def arrive(self, z):
        p = self.p

        @pl.when(z < p.z)
        def _():
            self.up(z).wait_recv()

        @pl.when(z > p.z)
        def _():
            self.down(z).wait_recv()

        @pl.when((z <= p.z) & (p.z < p.line - 1))
        def _():
            self.up(z).start()

        @pl.when((z >= p.z) & (p.z > 0))
        def _():
            self.down(z).start()

        self.across(z).start()
        self.beside(z, p.x).start()

    def arrive_across(self, z):
        self.across(z).wait_recv()
        self.beside(z, 1 - self.p.x).start()

    def part(self, turn, use=None):
        p = self.p
        step, part = turn // 4, turn % 4
        z = jnp.where(part == 0, p.near(step), p.near(step - 1))

        @pl.when(jnp.where(part == 0, step < p.line, step > 0))
        def _():
            @pl.when(part == 0)
            def _():
                self.arrive(z)

            @pl.when(part == 1)
            def _():
                self.arrive_across(z)

            x = jnp.where(part % 2 == 0, p.x, 1 - p.x)

            @pl.when(part >= 2)
            def _():
                self.beside(z, x).wait_recv()

            if use is not None:
                use(z, x, jnp.where(part < 2, p.core, 1 - p.core))

    def sent(self):
        p = self.p

        @pl.loop(0, p.line)
        def _(z):
            @pl.when((z <= p.z) & (p.z < p.line - 1))
            def _():
                self.up(z).wait_send()

            @pl.when((z >= p.z) & (p.z > 0))
            def _():
                self.down(z).wait_send()

            self.across(z).wait_send()
            self.beside(z, 0).wait_send()
            self.beside(z, 1).wait_send()


class Halve:
    def __init__(self, place, whole, got, sums, sems):
        self.p, self.whole, self.got, self.sums = place, whole, got, sums
        self.c_s, self.c_r = sems

    @staticmethod
    def sems(line):
        return [pltpu.SemaphoreType.DMA((2 * line,))] * 2

    def beside(self, z, x):
        p, at = self.p, z * 2 + x
        return p.copy(
            self.whole.at[p.slot(z, x, 1 - p.core)], self.got.at[at], self.c_s.at[at], self.c_r.at[at],
            p.slot(p.z, p.x, 1 - p.core),
        )

    def add(self, z):
        p = self.p
        for x in range(2):
            at = z * 2 + x
            self.beside(z, x).wait_recv()
            self.sums[at] = (
                self.whole[p.slot(z, x, p.core)].astype(jnp.float32) + self.got[at].astype(jnp.float32)
            ).astype(self.sums.dtype)

    def sent(self):
        @pl.loop(0, 2 * self.p.line)
        def _(at):
            self.beside(at // 2, at % 2).wait_send()


class Quad:
    def __init__(self, place, buf, sems):
        self.p, self.buf = place, buf
        self.s, self.r = sems

    @staticmethod
    def sems():
        return [pltpu.SemaphoreType.DMA((3,))] * 2

    def over(self, x, to, at):
        piece = self.buf.at[x * 2 + self.p.core]
        return self.p.copy(piece, piece, self.s.at[at], self.r.at[at], to)

    def across(self):
        p = self.p
        return self.over(p.x, p.slot(p.z, 1 - p.x, p.core), 0)

    def beside(self):
        p = self.p
        return self.over(p.x, p.slot(p.z, p.x, 1 - p.core), 1)

    def beside_next(self):
        p = self.p
        return self.over(1 - p.x, p.slot(p.z, p.x, 1 - p.core), 2)

    def start(self):
        self.across().start()
        self.beside().start()

    def relay(self):
        self.across().wait_recv()
        self.beside_next().start()

    def sent(self):
        self.across().wait_send()
        self.beside().wait_send()
        self.beside_next().wait_send()


class QuadSum:
    def __init__(self, place, whole, bufs, sems):
        self.p, self.whole = place, whole
        self.got, self.sums, self.far = bufs
        self.s, self.r = sems

    @staticmethod
    def sems():
        return [pltpu.SemaphoreType.DMA((3,))] * 2

    @staticmethod
    def bufs(block):
        return [pltpu.VMEM((2,) + block, jnp.bfloat16)] * 2 + [pltpu.VMEM(block, jnp.bfloat16)]

    def beside(self, x):
        p = self.p
        return p.copy(
            self.whole.at[x * 2 + 1 - p.core], self.got.at[x], self.s.at[x], self.r.at[x],
            p.slot(p.z, p.x, 1 - p.core),
        )

    def across(self):
        p = self.p
        return p.copy(
            self.sums.at[1 - p.x], self.far, self.s.at[2], self.r.at[2], p.slot(p.z, 1 - p.x, p.core)
        )

    def add(self, x):
        f32 = jnp.float32
        self.beside(x).wait_recv()
        self.sums[x] = (
            self.whole[x * 2 + self.p.core].astype(f32) + self.got[x].astype(f32)
        ).astype(self.sums.dtype)

    def finish(self, out):
        f32 = jnp.float32
        self.across().wait_recv()
        out[...] = self.sums[self.p.x].astype(f32) + self.far[...].astype(f32)

    def sent(self):
        self.beside(0).wait_send()
        self.beside(1).wait_send()
        self.across().wait_send()


class Settle:
    def __init__(self, place, sums, bufs, sems, pairwise=False):
        self.p, self.sums, self.pairwise = place, sums, pairwise
        self.got, self.total, self.low, self.high = bufs
        self.x_s, self.x_r, self.up_s, self.up_r, self.dn_s, self.dn_r = sems

    @staticmethod
    def sems(line):
        return [pltpu.SemaphoreType.DMA((line,))] * 6

    @staticmethod
    def bufs(line, block):
        return [pltpu.VMEM((line,) + block, jnp.bfloat16)] * 4

    def kept(self, z):
        p = self.p
        return p.pair * p.line + z if self.pairwise else z * 2 + p.x

    def across(self, z):
        p = self.p
        if self.pairwise:
            return p.over_pair(
                self.sums.at[(1 - p.pair) * p.line + z], self.got.at[z], self.x_s.at[z], self.x_r.at[z]
            )
        return p.copy(
            self.sums.at[z * 2 + 1 - p.x], self.got.at[z], self.x_s.at[z], self.x_r.at[z],
            p.slot(p.z, 1 - p.x, p.core),
        )

    def up(self, z):
        p = self.p
        return p.copy(self.total.at[z], self.low.at[z], self.up_s.at[z], self.up_r.at[z], (p.me + 4) % p.count)

    def down(self, z):
        p = self.p
        return p.copy(
            self.total.at[z], self.high.at[z], self.dn_s.at[z], self.dn_r.at[z], (p.me + p.count - 4) % p.count
        )

    def pass_on(self, z):
        p, f32 = self.p, jnp.float32
        self.across(z).wait_recv()
        self.total[z] = (
            self.sums[self.kept(z)].astype(f32) + self.got[z].astype(f32)
        ).astype(self.total.dtype)

        @pl.when(z > p.z)
        def _():
            @pl.when(p.z > 0)
            def _():
                self.up(z).wait_recv()
                self.total[z] = (self.total[z].astype(f32) + self.low[z].astype(f32)).astype(self.total.dtype)

            self.up(z).start()

        @pl.when(z < p.z)
        def _():
            @pl.when(p.z < p.line - 1)
            def _():
                self.down(z).wait_recv()
                self.total[z] = (self.total[z].astype(f32) + self.high[z].astype(f32)).astype(self.total.dtype)

            self.down(z).start()

    def finish(self, out):
        p, f32 = self.p, jnp.float32
        @pl.when(p.z > 0)
        def _():
            self.up(p.z).wait_recv()

        @pl.when(p.z < p.line - 1)
        def _():
            self.down(p.z).wait_recv()

        total = self.total[p.z].astype(f32)
        total += jnp.where(p.z > 0, self.low[p.z].astype(f32), 0.0)
        total += jnp.where(p.z < p.line - 1, self.high[p.z].astype(f32), 0.0)
        out[...] = total.astype(out.dtype)

    def sent(self):
        p = self.p

        @pl.loop(0, p.line)
        def _(z):
            self.across(z).wait_send()

            @pl.when(z > p.z)
            def _():
                self.up(z).wait_send()

            @pl.when(z < p.z)
            def _():
                self.down(z).wait_send()


class Exchange:
    def __init__(self, place, src, dst, sems):
        self.p, self.src, self.dst = place, src, dst
        self.s, self.r = sems

    @staticmethod
    def sems(count):
        return [pltpu.SemaphoreType.DMA((count,))] * 2

    def to(self, j):
        return self.p.copy(self.src.at[j], self.dst.at[self.p.me], self.s.at[j], self.r.at[self.p.me], j)

    def send(self, j):
        @pl.when(j != self.p.me)
        def _():
            self.to(j).start()

        @pl.when(j == self.p.me)
        def _():
            self.dst[j] = self.src[j]

    def arrived(self):
        p = self.p

        @pl.loop(1, p.count)
        def _(shift):
            j = (p.me + shift) % p.count
            p.copy(self.src.at[j], self.dst.at[j], self.s.at[j], self.r.at[j], j).wait_recv()

    def sent(self):
        p = self.p

        @pl.loop(1, p.count)
        def _(shift):
            self.to((p.me + shift) % p.count).wait_send()


class Spread:
    def __init__(self, place, src, dst, sems):
        self.p, self.src, self.dst = place, src, dst
        self.s, self.r = sems

    @staticmethod
    def sems(count):
        return [pltpu.SemaphoreType.DMA((2 * count,))] * 2

    def to(self, j):
        p = self.p
        return p.to_owner(self.src.at[j], self.dst.at[p.owner], self.s.at[j], self.r.at[p.owner], j)

    def send(self):
        p = self.p
        self.dst[p.owner] = self.src[p.owner]

        @pl.loop(1, 2 * p.count)
        def _(shift):
            self.to((p.owner + shift) % (2 * p.count)).start()

    def arrived(self):
        p = self.p

        @pl.loop(1, 2 * p.count)
        def _(shift):
            j = (p.owner + shift) % (2 * p.count)
            p.to_owner(self.src.at[j], self.dst.at[j], self.s.at[j], self.r.at[j], j).wait_recv()

    def sent(self):
        p = self.p

        @pl.loop(1, 2 * p.count)
        def _(shift):
            self.to((p.owner + shift) % (2 * p.count)).wait_send()


class Deliver:
    def __init__(self, place, src, dst, sems):
        self.p, self.src, self.dst = place, src, dst
        self.s, self.r = sems

    def away(self, piece, owner, slot):
        return self.p.to_owner(self.src.at[piece], self.dst.at[slot], self.s.at[piece], self.r.at[slot], owner)

    def send(self, piece, owner, slot):
        @pl.when(owner != self.p.owner)
        def _():
            self.away(piece, owner, slot).start()

        @pl.when(owner == self.p.owner)
        def _():
            self.dst[slot] = self.src[piece]

    def sent(self, piece, owner, slot):
        @pl.when(owner != self.p.owner)
        def _():
            self.away(piece, owner, slot).wait_send()

    def arrived(self, slot, source):
        p = self.p

        @pl.when(source != p.owner)
        def _():
            p.to_owner(self.src.at[0], self.dst.at[slot], self.s.at[0], self.r.at[slot], source).wait_recv()


def rotate_rows(value, cos, sine):
    half = value.shape[0] // 2
    first, second = value[:half], value[half:]
    return jnp.concatenate([first * cos - second * sine, second * cos + first * sine], axis=0)


def rotate_rows_back(grad, cos, sine):
    half = grad.shape[0] // 2
    first, second = grad[:half], grad[half:]
    return jnp.concatenate([first * cos + second * sine, second * cos - first * sine], axis=0)


def attend_kernel(
    count, tokens, cot, gain_attn, gain_mlp, qkv_weight, in_weight, down_mine, out_mine,
    normed_a, inv_a, normed_m, inv_m, middle, act_m, cos, sine, act_out, cot_all, query_t, keys_t, keys, values, mixed_own, log_sum, mixed, weight, in_other, down_other, out_pair,
    act_all, values_t, load_sem, part_sem, part_got, piece_sem, piece_got, *sems
):
    f32, bf16 = jnp.float32, jnp.bfloat16
    p = Place(count)
    rows, width = tokens.shape
    head = keys_t.shape[0]
    n = 8
    first = Gather(p, act_all, sems[:n])
    second = Quad(p, cot_all, sems[n : n + 2])
    trade = Exchange(p, mixed_own, mixed, sems[n + 2 :])
    half = out_mine.shape[0] // 2
    part_half = pl.ds(pl.multiple_of(p.core * half, half), half)
    loads = [(cot, cot_all.at[p.x * 2 + p.core]), (out_mine, out_pair.at[p.pair])]
    loads = [pltpu.make_async_copy(src, dst, load_sem.at[i]) for i, (src, dst) in enumerate(loads)]
    for load in loads:
        load.start()

    def part_rows(part):
        start = part * width + p.me * head
        holder = start // qkv_weight.shape[0]
        at = pl.ds(pl.multiple_of(start - holder * qkv_weight.shape[0], head), head)
        return holder == p.pair, qkv_weight.at[at]

    def part_copies(part):
        here, src = part_rows(part)
        return (
            here,
            pltpu.make_async_copy(src, weight.at[part], load_sem.at[3 + part]),
            p.over_pair(src, weight.at[part], part_sem.at[part], part_got.at[part]),
        )

    units, columns = in_other.shape[0], in_other.shape[1] // 2
    in_rows = pl.ds(pl.multiple_of((p.x * 2 + p.core) * units, 16), units)
    in_cols = pl.ds(pl.multiple_of(p.z % 2 * columns, columns), columns)
    in_here = in_other.at[:, in_cols]
    swaps = [
        p.over_pair(out_mine.at[part_half], out_pair.at[p.pair, part_half], piece_sem.at[0], piece_got.at[0]),
        p.over_pair(in_weight.at[in_rows, in_cols], in_here, piece_sem.at[1], piece_got.at[1]),
        p.over_pair(down_mine, down_other, piece_sem.at[2], piece_got.at[2]),
    ]
    next_z = p.me + 4 - p.z % 2 * 8
    in_share = p.copy(in_here, in_here, piece_sem.at[4], piece_got.at[4], next_z)
    out_rest = out_pair.at[1 - p.pair, part_half]
    share = p.copy(out_rest, out_rest, piece_sem.at[3], piece_got.at[3], p.slot(p.z, p.x, 1 - p.core))
    for part in range(3):
        here, own, away = part_copies(part)

        @pl.when(here)
        def _():
            own.start()

    p.meet()
    for part in range(3):
        here, own, away = part_copies(part)

        @pl.when(here)
        def _():
            away.start()

    for at in (1, 0, 2):
        swaps[at].start()
    resid = tokens[...].astype(f32)
    normed, inv = normalize(resid)
    normed_a[...], inv_a[...] = normed, inv
    act_all[p.me] = (normed * gain_attn[...]).astype(bf16)
    for load in loads:
        load.wait()

    first.part(0)
    position = lax.broadcasted_iota(jnp.int32, cos.shape, 1).astype(f32)
    entry = lax.broadcasted_iota(jnp.int32, (cos.shape[0], 1), 0).astype(f32)
    angles = position * jnp.exp(entry * (-2.0 * math.log(ROPE_BASE) / head))
    cos[...], sine[...] = jnp.cos(angles), jnp.sin(angles)
    for part in range(3):
        here, own, away = part_copies(part)

        @pl.when(here)
        def _():
            own.wait()

        @pl.when(jnp.logical_not(here))
        def _():
            away.wait_recv()

    head_weight = weight[...].reshape(3 * head, width)

    def project(z, x, core):
        at = p.slot(z, x, core)
        lanes = pl.ds(pl.multiple_of(at * rows, rows), rows)
        packed = matmul(head_weight, act_all[at], 1, 1)
        c, s = cos[:, lanes], sine[:, lanes]
        query, key = packed[:head], packed[head : 2 * head]
        query_t[:, lanes] = rotate_rows(query, c, s).astype(bf16)
        key = rotate_rows(key, c, s)
        keys_t[:, lanes] = key.astype(bf16)
        values_t[:, lanes] = packed[2 * head :].astype(bf16)
        keys[lanes, :] = key.T.astype(bf16)
        values[lanes, :] = packed[2 * head :].T.astype(bf16)

    project(p.z, p.x, p.core)

    @pl.loop(4, 4 * p.line + 4)
    def _(at):
        first.part(at, project)

    keep_act = pltpu.make_async_copy(act_all, act_out, load_sem.at[2])
    keep_act.start()
    second.start()
    swaps[1].wait_recv()
    in_share.start()
    wide = 2 * rows
    blocks = count // 2
    scale = head ** (-0.5)

    def attend(i):
        block = (p.me // 2 + i) % blocks
        lanes = pl.ds(pl.multiple_of(block * wide, wide), wide)
        scores = matmul(keys[...], query_t[:, lanes], 1, 0) * scale
        top = jnp.max(scores, axis=0, keepdims=True)
        weights = jnp.exp(scores - top)
        total = jnp.sum(weights, axis=0, keepdims=True)
        log_sum[:, lanes] = top + jnp.log(total)
        out = (matmul(values_t[...], weights.astype(bf16), 1, 0) / total).astype(bf16)
        mixed_own[2 * block] = out[:, :rows]
        mixed_own[2 * block + 1] = out[:, rows:]
        trade.send(2 * block)
        trade.send(2 * block + 1)

    @pl.loop(0, blocks // 2)
    def _(i):
        attend(i)

    second.relay()
    swaps[0].wait_recv()
    share.start()

    @pl.loop(blocks // 2, blocks)
    def _(i):
        attend(i)

    trade.arrived()
    share.wait_recv()
    flat = mixed[...].reshape(width, rows)
    total = tokens[...].astype(f32) + matmul(flat, out_pair[...].reshape(width, width), 0, 1)
    middle[...] = total
    normed, inv = normalize(total)
    normed_m[...], inv_m[...] = normed, inv
    act_m[...] = (normed * gain_mlp[...]).astype(bf16)
    second.beside().wait_recv()
    second.beside_next().wait_recv()
    swaps[2].wait_recv()
    first.sent()
    second.sent()
    trade.sent()
    for part in range(3):
        here, own, away = part_copies(part)

        @pl.when(here)
        def _():
            away.wait_send()

    for swap in swaps:
        swap.wait_send()
    share.wait_send()
    in_share.wait()
    keep_act.wait()


def feed_kernel(
    count, act, cot_all, in_weight, in_other, down_mine, down_other, gain, out_pair, normed, inv, middle,
    output, grad_middle, grad_mid, grad_mixed, in_grad, down_grad,
    grad_act, out_total, weight, down, act_all, gated, inner_grad, grad_part, out_part, load_sem, *rest
):
    f32, bf16 = jnp.float32, jnp.bfloat16
    p = Place(count)
    rows, group = act.shape[0], down.shape[1]
    gather = Quad(p, act_all, rest[:2])
    grad_sum = QuadSum(p, grad_part, rest[2:5], rest[8:10])
    out_sum = QuadSum(p, out_part, rest[5:8], rest[10:12])
    units, half = in_other.shape[0], down_other.shape[0]
    in_rows = pl.ds(pl.multiple_of((p.x * 2 + p.core) * units, 16), units)
    own_at = pl.ds(pl.multiple_of(p.pair * group, group), units)
    other_at = pl.ds(pl.multiple_of((1 - p.pair) * group, group), units)
    load = pltpu.make_async_copy(act, act_all.at[p.x * 2 + p.core], load_sem.at[0])
    weights = [
        pltpu.make_async_copy(in_weight.at[in_rows], weight.at[own_at], load_sem.at[1]),
        pltpu.make_async_copy(in_other, weight.at[other_at], load_sem.at[2]),
    ]
    load.start()
    for copy in weights:
        copy.start()
    p.meet()
    load.wait()
    gather.start()
    down[...] = jnp.zeros_like(down)
    down[pl.ds(pl.multiple_of(p.pair * half, half), half), :units] = down_mine[...]
    down[pl.ds(pl.multiple_of((1 - p.pair) * half, half), half), :units] = down_other[...]
    for at in range(2):
        weight[at * group + units : (at + 1) * group, :] = jnp.zeros((group - units, weight.shape[1]), bf16)
    for copy in weights:
        copy.wait()
    gather.beside().wait_recv()

    @pl.loop(0, 2)
    def _(step):
        x = jnp.where(step == 0, p.x, 1 - p.x)

        @pl.when(step == 1)
        def _():
            gather.relay()
            gather.beside_next().wait_recv()

        acts = jnp.concatenate([act_all[2 * x], act_all[2 * x + 1]], axis=0)
        cots = jnp.concatenate([cot_all[2 * x], cot_all[2 * x + 1]], axis=0)
        inner = matmul(acts, weight[...], 1, 1)
        grad_gated = matmul(cots, down[...], 1, 0)
        value, gate = inner[:, :group], inner[:, group:]
        gelu_val, gelu_slope = gelu_pair(value)
        token = pl.ds(pl.multiple_of(x * 2 * rows, 2 * rows), 2 * rows)
        out = (gelu_val * gate).astype(bf16)
        gated[token, :] = out
        grads = jnp.concatenate(
            [grad_gated * gate * gelu_slope, grad_gated * gelu_val], axis=1
        ).astype(bf16)
        inner_grad[token, :] = grads
        part = matmul(grads, weight[...], 1, 0).astype(bf16)
        grad_part[2 * x], grad_part[2 * x + 1] = part[:rows], part[rows:]
        grad_sum.beside(x).start()
        part = matmul(out, down[...], 1, 1).astype(bf16)
        out_part[2 * x], out_part[2 * x + 1] = part[:rows], part[rows:]
        out_sum.beside(x).start()

    grad_sum.add(1 - p.x)
    grad_sum.across().start()
    grad_sum.add(p.x)
    out_sum.add(1 - p.x)
    out_sum.across().start()
    out_sum.add(p.x)
    acts = act_all[...].reshape(4 * rows, act.shape[1])
    cots = cot_all[...].reshape(4 * rows, act.shape[1])
    quarter = units // 4
    gain_row = jnp.zeros((1, act.shape[1]), f32)
    for at in range(2):
        piece = matmul(inner_grad[:, at * group : (at + 1) * group], acts, 0, 0)
        gain_row += jnp.sum(piece * weight[at * group : (at + 1) * group, :].astype(f32), axis=0, keepdims=True)
        for k in range(4):
            in_grad[k % 2 * p.line + at * 2 + k // 2] = piece[k * quarter : (k + 1) * quarter].astype(bf16)
    piece = matmul(cots, gated[...], 0, 0)
    lane = lax.broadcasted_iota(jnp.int32, piece.shape, 1)
    gain_row = gain_row / gain[...]
    column = jnp.broadcast_to(gain_row, (8, gain_row.shape[1])).T[:, :1]
    piece = jnp.where(lane == units, column, piece).astype(bf16)
    unit = act.shape[1] // (2 * count)
    for z in range(p.line):
        for r in range(4):
            for y in range(2):
                start = ((z * 4 + r) * 2 + y) * unit
                down_grad[y * p.line + z, r] = piece[start : start + unit]
    grad_sum.finish(grad_act)
    cot = cot_all[p.x * 2 + p.core].astype(f32)
    grad = cot + norm_back(grad_act[...] * gain[...], normed[...], inv[...])
    grad_middle[...] = grad
    grad_mid[...] = grad.astype(bf16)
    width = act.shape[1]
    back = matmul(grad_mid[...], out_pair[...].reshape(width, width), 1, 0)
    grad_mixed[...] = back.T.astype(bf16).reshape(grad_mixed.shape)
    out_sum.finish(out_total)
    output[...] = middle[...] + out_total[...]
    gather.sent()
    grad_sum.sent()
    out_sum.sent()


def attend_back_kernel(
    count, grad_mixed, grad_mid, mixed, query_t, keys_t, keys, values, mixed_own, log_sum,
    act_in, weight, cos, sine, in_grad, down_grad, gain, grad_middle, normed, inv,
    grad_input, qkv_out, out_out, in_out, down_out, gain_m_out, gain_a_out,
    act_all, act_sem, grad_act, grad_own, grad_keys, grad_values, grad_packed, grad_part, grad_got, grad_sums, grad_weight,
    pair_part, pair_core, pair_sums, pair_got, proj_sums, in_sum, in_got, down_sum, down_got,
    qkv_part, qkv_got, gain_part, gain_got,
    pair_s, pair_r, in_s, in_r, down_s, down_r, qkv_s, qkv_r, *rest
):
    f32, bf16 = jnp.float32, jnp.bfloat16
    p = Place(count)
    rows, head = grad_mixed.shape[2], keys_t.shape[0]
    width, unit = count * head, head // 2
    bufs, proj_bufs, in_bufs, down_bufs, sems = rest[:4], rest[4:8], rest[8:12], rest[12:16], rest[16:]
    trade = Exchange(p, grad_mixed, grad_own, sems[:2])
    halve = Halve(p, grad_part, grad_got, grad_sums, sems[2:4])
    settle = Settle(p, grad_sums, bufs, sems[4:10])
    halve_proj = Halve(p, pair_part, pair_core, pair_sums, sems[10:12])
    settle_proj = Settle(p, proj_sums, proj_bufs, sems[12:18])
    settle_in = Settle(p, in_grad, in_bufs, sems[18:24], True)
    settle_down = Settle(p, down_grad, down_bufs, sems[24:30], True)
    spread_gain = Spread(p, gain_part, gain_got, sems[30:32])
    give_in = Deliver(p, in_sum, in_got, (in_s, in_r))
    give_down = Deliver(p, down_sum, down_got, (down_s, down_r))
    give_qkv = Deliver(p, qkv_part, qkv_got, (qkv_s, qkv_r))

    def swap(at):
        return p.over_pair(pair_sums.at[at, 1 - p.pair], pair_got.at[at], pair_s.at[at], pair_r.at[at])

    load_act = pltpu.make_async_copy(act_in, act_all, act_sem)
    load_act.start()
    p.meet(True)

    @pl.loop(0, count)
    def _(shift):
        trade.send((p.me + shift) % count)

    @pl.loop(0, p.line)
    def _(step):
        settle_in.across(p.far(step)).start()
        settle_down.across(p.far(step)).start()

    flat = mixed[...].reshape(width, rows)

    @pl.loop(0, count // 2)
    def _(i):
        lanes = pl.ds(pl.multiple_of(i * 4 * unit, 4 * unit), 4 * unit)
        piece = matmul(grad_mid[:, lanes], flat, 0, 1).astype(bf16)
        for at in range(4):
            pair_part[2 * i + at // 2, at % 2] = piece[at * unit : (at + 1) * unit]

    @pl.loop(0, 2 * p.line)
    def _(at):
        halve_proj.beside(at // 2, at % 2).start()

    @pl.loop(0, p.line)
    def _(step):
        z = p.far(step)
        halve_proj.add(z)
        swap(2 * z).start()
        swap(2 * z + 1).start()

    grad_keys[...] = jnp.zeros_like(grad_keys)
    grad_values[...] = jnp.zeros_like(grad_values)
    trade.arrived()
    wide = 2 * rows
    scale = head ** (-0.5)

    def back(i):
        lanes = pl.ds(pl.multiple_of(i * wide, wide), wide)
        query = query_t[:, lanes]
        grad = jnp.concatenate([grad_own[2 * i], grad_own[2 * i + 1]], axis=1)
        own = jnp.concatenate([mixed_own[2 * i], mixed_own[2 * i + 1]], axis=1)
        delta = jnp.sum(grad.astype(f32) * own.astype(f32), axis=0, keepdims=True)
        scores = matmul(keys[...], query, 1, 0) * scale
        probs = jnp.exp(scores - log_sum[:, lanes])
        grad_values[...] += matmul(probs.astype(bf16), grad, 1, 1)
        grad_probs = matmul(values[...], grad, 1, 0)
        grad_scores = (probs * (grad_probs - delta)).astype(bf16)
        grad_keys[...] += matmul(grad_scores, query, 1, 1)
        grad_query = matmul(keys_t[...], grad_scores, 1, 0) * scale
        back_query = rotate_rows_back(grad_query, cos[:, lanes], sine[:, lanes])
        grad_packed[:head, lanes] = back_query.astype(bf16)

    @pl.loop(0, count // 2)
    def _(i):
        back(i)

        @pl.when(i == count // 4)
        def _():
            settle_in.pass_on(p.far(0))
            settle_down.pass_on(p.far(0))

    grad_key = grad_keys[...].T * scale
    grad_packed[head : 2 * head, :] = rotate_rows_back(grad_key, cos[...], sine[...]).astype(bf16)
    grad_packed[2 * head :, :] = grad_values[...].T.astype(bf16)

    @pl.loop(0, p.line)
    def _(step):
        z = p.far(step)
        for at in range(4):
            lanes = pl.ds(pl.multiple_of((z * 4 + at) * rows, rows), rows)
            grad_part[z * 4 + at] = matmul(grad_packed[:, lanes], weight[...], 0, 0).astype(bf16)
        halve.beside(z, 0).start()
        halve.beside(z, 1).start()

    @pl.loop(0, p.line)
    def _(step):
        z = p.far(step)
        halve.add(z)
        settle.across(z).start()

    def grad_chunk(step):
        lanes = pl.ds(pl.multiple_of(step * 4 * rows, 4 * rows), 4 * rows)
        acts = jnp.concatenate([act_all[4 * step + i] for i in range(4)], axis=0)
        return matmul(grad_packed[:, lanes], acts, 1, 0)

    load_act.wait()
    grad_weight[...] = grad_chunk(0)

    @pl.loop(1, p.line)
    def _(step):
        grad_weight[...] += grad_chunk(step)

    for at in range(6):
        qkv_part[at] = grad_weight[at * unit : (at + 1) * unit, :].astype(bf16)
    gain_row = jnp.sum(grad_weight[...] * weight[...].astype(f32), axis=0, keepdims=True) / gain[...]
    for at in range(2 * count):
        chunk = at * unit // 128 * 128
        gain_part[at] = gain_row[:, chunk : chunk + 128]

    def unit_of(at):
        return (at // 2) * 2 * count + 2 * p.me + at % 2

    for at in range(6):
        give_qkv.send(at, unit_of(at) // 3, unit_of(at) % 3 * 2 + p.pair)
    spread_gain.send()

    @pl.loop(0, p.line)
    def _(step):
        z = p.far(step)
        settle.pass_on(z)

        @pl.when(step > 0)
        def _():
            settle_in.pass_on(z)
            settle_down.pass_on(z)

    @pl.loop(0, p.line)
    def _(step):
        z = p.far(step)
        for x in range(2):
            at = 2 * z + x
            swap(at).wait_recv()
            proj_sums[at] = (pair_sums[at, p.pair].astype(f32) + pair_got[at].astype(f32)).astype(bf16)
        settle_proj.across(z).start()

    @pl.loop(0, p.line)
    def _(step):
        settle_proj.pass_on(p.far(step))

    units = in_out.shape[0]
    r = p.x * 2 + p.core
    piece_owner = p.z // 2 * count + r * 4 + p.z % 2 * 2 + p.pair
    settle_in.finish(in_sum.at[0])
    give_in.send(0, piece_owner, 0)
    settle_down.finish(down_sum)
    for at in range(4):
        give_down.send(at, (p.z * 4 + at) * 2 + p.pair, r)
    for slot in range(3):
        source = (3 * p.owner + slot) % (2 * count) // 2 * 2
        for side in range(2):
            give_qkv.arrived(2 * slot + side, source + side)
        qkv_out[slot * unit : (slot + 1) * unit, :] = qkv_got[2 * slot].astype(f32) + qkv_got[2 * slot + 1].astype(f32)
    spread_gain.arrived()
    gain_a = gain_got[0]
    for at in range(1, 2 * count):
        gain_a += gain_got[at]
    chunks = 128 // unit
    gain_a_out[...] = sum(
        jnp.where(p.owner % chunks == at, gain_a[:, at * unit : (at + 1) * unit], 0.0) for at in range(chunks)
    )
    settle_proj.finish(out_out)
    settle.finish(grad_act)
    grad_input[...] = grad_middle[...] + norm_back(grad_act[...] * gain[...], normed[...], inv[...])
    half, r_of, k_of = p.owner // count, p.owner % count // 4, p.owner % 4
    source_in = ((half * 2 + k_of // 2) * 4 + r_of) * 2 + k_of % 2
    give_in.arrived(0, source_in)
    in_out[...] = in_got[0].astype(f32)
    gain_m = jnp.zeros((unit, 1), f32)
    group = 4 * units
    for at in range(4):
        give_down.arrived(at, (p.z * 4 + at) * 2 + p.pair)
        block = down_got[at].astype(f32)
        down_out[:, at * group : (at + 1) * group] = block[:, :group]
        gain_m += block[:, group : group + 1]
    gain_m_out[...] = jnp.broadcast_to(gain_m, (unit, 128)).T[:1]
    trade.sent()
    halve.sent()
    settle.sent()
    halve_proj.sent()
    settle_proj.sent()
    settle_in.sent()
    settle_down.sent()
    spread_gain.sent()

    @pl.loop(0, 2 * p.line)
    def _(at):
        swap(at).wait_send()

    give_in.sent(0, piece_owner, 0)
    for at in range(4):
        give_down.sent(at, (p.z * 4 + at) * 2 + p.pair, r)
    for at in range(6):
        give_qkv.sent(at, unit_of(at) // 3, unit_of(at) % 3 * 2 + p.pair)


def run_kernel(body, outs, scratch, collective, flops, args, outside=(), outs_outside=()):
    vmem, anywhere = pl.BlockSpec(memory_space=pltpu.VMEM), pl.BlockSpec(memory_space=pl.ANY)
    return pl.pallas_call(
        body,
        out_shape=outs,
        in_specs=[anywhere if i in outside else vmem for i in range(len(args))],
        out_specs=[anywhere if i in outs_outside else vmem for i in range(len(outs))],
        scratch_shapes=scratch,
        compiler_params=pltpu.CompilerParams(
            collective_id=collective, has_side_effects=True, vmem_limit_bytes=VMEM_LIMIT
        ),
        cost_estimate=pl.CostEstimate(flops=flops, bytes_accessed=20_000_000, transcendentals=0),
        name=body.func.__name__,
    )(*args)


def shaped(shape, kind):
    return jax.ShapeDtypeStruct(shape, kind)


def attend(count, head, tokens, cot, gain_attn, gain_mlp, qkv_weight, in_weight, down_mine, out_mine):
    bf16, f32 = jnp.bfloat16, jnp.float32
    rows, width = tokens.shape
    length, line = rows * count, count // 4
    blocks = shaped((count, rows, width), bf16)
    tall, flat = shaped((head, length), bf16), shaped((length, head), bf16)
    heads = shaped((count, head, rows), bf16)
    block, column, table = shaped((rows, width), f32), shaped((rows, 1), f32), shaped((head // 2, length), f32)
    pairs = [shaped((in_weight.shape[0] // 4, width), bf16), shaped(down_mine.shape, bf16), shaped((2,) + out_mine.shape, bf16)]
    three, six = pltpu.SemaphoreType.DMA((3,)), pltpu.SemaphoreType.DMA((6,))
    return run_kernel(
        functools.partial(attend_kernel, count),
        [block, column, block, column, block, shaped((rows, width), bf16), table, table,
         blocks, shaped((4, rows, width), bf16), tall, tall, flat, flat, heads, shaped((1, length), f32), heads,
         shaped((3, head, width), bf16)] + pairs,
        [pltpu.VMEM(blocks.shape, bf16), pltpu.VMEM((head, length), bf16), pltpu.SemaphoreType.DMA((6,))] + [three, three, six, six]
        + Gather.sems(line) + Quad.sems() + Exchange.sems(count),
        0, 10_000_000_000, [tokens, cot, gain_attn, gain_mlp, qkv_weight, in_weight, down_mine, out_mine], (4, 5, 6, 7),
        (8, 18, 19),
    )


def feed(count, group, act, cot_all, in_weight, in_other, down_mine, down_other, gain, out_pair, normed, inv, middle):
    bf16, f32 = jnp.bfloat16, jnp.float32
    rows, width = act.shape
    block = (rows, width)
    units, line, unit = in_other.shape[0], count // 4, width // (2 * count)
    whole = pltpu.VMEM((4,) + block, bf16)
    return run_kernel(
        functools.partial(feed_kernel, count),
        [shaped(block, f32), shaped(block, f32), shaped(block, bf16), shaped((count, width // count, rows), bf16),
         shaped((2 * line, units // 4, width), bf16), shaped((2 * line, 4, unit, group), bf16)],
        [pltpu.VMEM(block, f32), pltpu.VMEM(block, f32), pltpu.VMEM((2 * group, width), bf16), pltpu.VMEM((width, group), bf16),
         whole, pltpu.VMEM((4 * rows, group), bf16), pltpu.VMEM((4 * rows, 2 * group), bf16), whole, whole,
         pltpu.SemaphoreType.DMA((3,))]
        + Quad.sems() + QuadSum.bufs(block) * 2 + QuadSum.sems() * 2,
        1, 20_000_000_000, [act, cot_all, in_weight, in_other, down_mine, down_other, gain, out_pair, normed, inv, middle], (2, 3),
    )


def attend_back(count, grad_mixed, grad_mid, mixed, kept, act_all, weight, cos, sine, in_grad, down_grad, gain, grad_middle, normed, inv):
    bf16, f32 = jnp.bfloat16, jnp.float32
    rows, width = act_all.shape[1:]
    head, length, line = weight.shape[0] // 3, rows * count, count // 4
    block, unit, units = (rows, width), head // 2, in_grad.shape[1]
    down_block = down_grad.shape[1:]
    piece = (unit, width)

    def held(*shape):
        return pltpu.VMEM(shape, bf16)

    whole, half = held(count, *block), held(2 * line, *block)
    flat = pltpu.VMEM((length, head), f32)
    one, four, six, many = [pltpu.SemaphoreType.DMA((n,)) for n in (1, 4, 6, 2 * line)]
    return run_kernel(
        functools.partial(attend_back_kernel, count),
        [shaped(block, f32), shaped((3 * unit, width), f32), shaped(piece, f32),
         shaped((units, width), f32), shaped((unit, units * count), f32), shaped((1, unit), f32), shaped((1, unit), f32)],
        [whole, pltpu.SemaphoreType.DMA, pltpu.VMEM(block, f32), held(count, head, rows), flat, flat, held(3 * head, length), whole, half, half,
         pltpu.VMEM((3 * head, width), f32),
         held(count, 2, *piece), held(2 * line, 2, *piece), held(2 * line, 2, *piece), held(2 * line, *piece),
         held(2 * line, *piece), held(1, units, width), held(1, units, width), held(*down_block), held(*down_block),
         held(6, *piece), held(6, *piece), pltpu.VMEM((2 * count, 1, 128), f32), pltpu.VMEM((2 * count, 1, 128), f32),
         many, many, one, one, four, four, six, six]
        + Settle.bufs(line, block) + Settle.bufs(line, piece)
        + Settle.bufs(line, (units, width)) + Settle.bufs(line, down_block)
        + Exchange.sems(count) + (Halve.sems(line) + Settle.sems(line)) * 2
        + Settle.sems(line) * 2 + Spread.sems(count),
        2, 20_000_000_000,
        [grad_mixed, grad_mid, mixed, *kept, act_all, weight, cos, sine, in_grad, down_grad, gain,
         grad_middle, normed, inv], (3 + len(kept),),
    )


def publish_kernel(*refs):
    half = len(refs) // 2
    for src, dst in zip(refs[:half], refs[half:]):
        dst[...] = src[...]


def publish(arrays):
    vmem = pl.BlockSpec(memory_space=pltpu.VMEM)
    return pl.pallas_call(
        publish_kernel,
        out_shape=[shaped(array.shape, array.dtype) for array in arrays],
        in_specs=[vmem] * len(arrays),
        out_specs=[vmem] * len(arrays),
        compiler_params=pltpu.CompilerParams(vmem_limit_bytes=VMEM_LIMIT),
    )(*arrays)


def tensor_layer(
    tokens, cotangent, gain_attn, gain_mlp, qkv_weight, out_weight, in_weight, down_weight
):
    count = lax.axis_size("ctx")
    index = lax.axis_index("ctx")
    width = tokens.shape[2]
    head_size = width // count
    group = in_weight.shape[0] // 4
    padded = (group // 128 + 1) * 128

    down_mine = lax.dynamic_slice_in_dim(down_weight, lax.rem(index, 4) * group, group, 1)
    (
        normed_a, inv_a, normed_m, inv_m, middle, act_m, cos, sine, act_all, cot_all, *kept,
        mixed, qkv_head, in_other, down_other, out_pair,
    ) = attend(
        count, head_size, tokens[0], cotangent[0], gain_attn[None], gain_mlp[None],
        qkv_weight, in_weight, down_mine, out_weight,
    )
    output, grad_middle, grad_mid, grad_mixed, in_grad, down_grad = feed(
        count, padded, act_m, cot_all, in_weight, in_other, down_mine, down_other, gain_mlp[None],
        out_pair, normed_m, inv_m, middle,
    )
    grad_input, grad_qkv, grad_out, grad_in, grad_down, grad_gain_m, grad_gain_a = attend_back(
        count, grad_mixed, grad_mid, mixed, kept, act_all, qkv_head.reshape(3 * head_size, width), cos, sine,
        in_grad, down_grad, gain_attn[None], grad_middle, normed_a, inv_a,
    )
    output, grad_input, grad_qkv, grad_out, grad_in, grad_down, grad_gain_a, grad_gain_m = publish(
        [output, grad_input, grad_qkv, grad_out, grad_in, grad_down, grad_gain_a, grad_gain_m]
    )
    return (output[None], grad_input[None], grad_qkv, grad_out, grad_in, grad_down, grad_gain_a[0], grad_gain_m[0])


def solution(mesh):

    def layer(*arrays):
        one_head_each = arrays[0].shape[2] == HEAD_DIM * mesh.shape["ctx"]
        if one_head_each and mesh.shape["fsdp"] == 2 and mesh.shape["ctx"] % 4 == 0:
            return tensor_layer(*arrays)
        return gathered_layer(*arrays)

    return jax.shard_map(
        layer,
        mesh=mesh,
        in_specs=(
            P("fsdp", "ctx", None),
            P("fsdp", "ctx", None),
            P(),
            P(),
            P("fsdp", None),
            P("fsdp", None),
            P("fsdp", None),
            P("fsdp", None),
        ),
        out_specs=(
            P("fsdp", "ctx", None),
            P("fsdp", "ctx", None),
            P(("ctx", "fsdp"), None),
            P(("ctx", "fsdp"), None),
            P(("ctx", "fsdp"), None),
            P(("ctx", "fsdp"), None),
            P(("ctx", "fsdp")),
            P(("ctx", "fsdp")),
        ),
        check_vma=False,
    )
```

```python
import functools
import math

import jax
import jax.numpy as jnp
from jax import lax
from jax.experimental import pallas as pl
from jax.experimental.pallas import tpu as pltpu
from jax.sharding import PartitionSpec as P

HEAD_DIM = 64


EPSILON = 1e-05
ROPE_BASE = 160000.0


def normalize(tensor):
    centred = tensor - jnp.mean(tensor, axis=-1, keepdims=True)
    inv_std = lax.rsqrt(jnp.mean(centred * centred, axis=-1, keepdims=True) + EPSILON)
    return (centred * inv_std, inv_std)


def norm_back(grad_norm, normed, inv_std):
    return inv_std * (
        grad_norm
        - jnp.mean(grad_norm, axis=-1, keepdims=True)
        - normed * jnp.mean(grad_norm * normed, axis=-1, keepdims=True)
    )


def gelu_pair(tensor):
    cumul = 0.5 * (1.0 + jax.scipy.special.erf(tensor * 0.7071067811865476))
    density = jnp.exp(-0.5 * tensor * tensor) * 0.3989422804014327
    return (tensor * cumul, cumul + tensor * density)


def rope_tables(offset, length, head_size):
    positions = (offset + jnp.arange(length, dtype=jnp.int32)).astype(jnp.float32)
    inverse = ROPE_BASE ** (
        -jnp.arange(0, head_size, 2, dtype=jnp.int32).astype(jnp.float32) / head_size
    )
    angles = positions[:, None] * inverse[None, :]
    angles = jnp.concatenate([angles, angles], axis=-1)
    return (jnp.cos(angles)[:, None, :], jnp.sin(angles)[:, None, :])


def rotate(tensor, cos_table, sine_table):
    middle = tensor.shape[-1] // 2
    turned = jnp.concatenate([-tensor[..., middle:], tensor[..., :middle]], axis=-1)
    return tensor * cos_table + turned * sine_table


def rotate_back(gradient, cos_table, sine_table):
    middle = gradient.shape[-1] // 2
    scaled = gradient * sine_table
    turned = jnp.concatenate([scaled[..., middle:], -scaled[..., :middle]], axis=-1)
    return gradient * cos_table + turned


def rows_product(left, right):
    return lax.dot_general(
        left, right, (((1,), (1,)), ((), ())), preferred_element_type=jnp.float32
    )


def rows_contract(left, right):
    return lax.dot_general(
        left, right, (((0,), (0,)), ((), ())), preferred_element_type=jnp.float32
    )


def gathered_layer(
    tokens, cotangent, gain_attn, gain_mlp, qkv_weight, out_weight, in_weight, down_weight
):
    f32 = jnp.float32
    bf16 = jnp.bfloat16
    qkv_full, out_full, in_full, down_full = (
        lax.all_gather(qkv_weight, "fsdp", axis=0, tiled=True),
        lax.all_gather(out_weight, "fsdp", axis=0, tiled=True),
        lax.all_gather(in_weight, "fsdp", axis=0, tiled=True),
        lax.all_gather(down_weight, "fsdp", axis=0, tiled=True),
    )
    tok_rows = tokens.shape[1]
    width = tokens.shape[2]
    hidden = down_full.shape[1]
    head_size = HEAD_DIM
    head_count = width // head_size
    scale = head_size ** (-0.5)
    offset = lax.axis_index("ctx") * tok_rows
    cos_table, sine_table = rope_tables(offset, tok_rows, head_size)
    resid = tokens[0].astype(f32)
    normed_a, inv_a = normalize(resid)
    act_a = (normed_a * gain_attn).astype(bf16)
    packed = rows_product(act_a, qkv_full)
    query_heads = rotate(
        packed[:, :width].reshape(tok_rows, head_count, head_size), cos_table, sine_table
    ).astype(bf16)
    key_heads = rotate(
        packed[:, width : 2 * width].reshape(tok_rows, head_count, head_size), cos_table, sine_table
    ).astype(bf16)
    value_send = packed[:, 2 * width :].astype(bf16)
    key_send = key_heads.reshape(tok_rows, width)
    value_heads = value_send.reshape(tok_rows, head_count, head_size)
    start_state = (
        jnp.zeros((tok_rows, head_count, head_size), f32),
        jnp.full((head_count, tok_rows), -1e30, f32),
        jnp.zeros((head_count, tok_rows), f32),
    )
    key_piece = lax.all_gather(key_send, "ctx", axis=0, tiled=True)
    value_piece = lax.all_gather(value_send, "ctx", axis=0, tiled=True)
    length = key_piece.shape[0]
    step_len = math.gcd(length, 1024)

    def attend_block(block_num, running):
        weighted, row_max, row_sum = running
        key_blk = lax.dynamic_slice_in_dim(key_piece, block_num * step_len, step_len, 0).reshape(
            step_len, head_count, head_size
        )
        value_blk = lax.dynamic_slice_in_dim(
            value_piece, block_num * step_len, step_len, 0
        ).reshape(step_len, head_count, head_size)
        scores = (
            jnp.einsum("qhd,khd->hqk", query_heads, key_blk, preferred_element_type=f32) * scale
        )
        new_max = jnp.maximum(row_max, jnp.max(scores, axis=-1))
        shrink = jnp.exp(row_max - new_max)
        weights = jnp.exp(scores - new_max[..., None])
        row_sum = row_sum * shrink + jnp.sum(weights, axis=-1)
        weighted = weighted * shrink.T[:, :, None] + jnp.einsum(
            "hqk,khd->qhd", weights.astype(bf16), value_blk, preferred_element_type=f32
        )
        return (weighted, new_max, row_sum)

    weighted, row_max, row_sum = lax.fori_loop(0, length // step_len, attend_block, start_state)
    log_sum = row_max + jnp.log(row_sum)
    mixed = (weighted / row_sum.T[:, :, None]).reshape(tok_rows, width).astype(bf16)
    middle = resid + rows_product(mixed, out_full)
    normed_m, inv_m = normalize(middle)
    act_m = (normed_m * gain_mlp).astype(bf16)
    inner = rows_product(act_m, in_full)
    gelu_val, gelu_slope = gelu_pair(inner[:, :hidden])
    gated = (gelu_val * inner[:, hidden:]).astype(bf16)
    output = middle + rows_product(gated, down_full)
    cot_rows = cotangent[0]
    grad_down = rows_contract(cot_rows, gated)
    grad_gated = jnp.dot(cot_rows, down_full, preferred_element_type=f32)
    grad_inner = jnp.concatenate(
        [grad_gated * inner[:, hidden:] * gelu_slope, grad_gated * gelu_val], axis=1
    ).astype(bf16)
    grad_in = rows_contract(grad_inner, act_m)
    grad_act_m = jnp.dot(grad_inner, in_full, preferred_element_type=f32)
    grad_gain_m = jnp.sum(grad_act_m * normed_m, axis=0)
    grad_middle = cot_rows.astype(f32) + norm_back(grad_act_m * gain_mlp, normed_m, inv_m)
    grad_mid_bf = grad_middle.astype(bf16)
    grad_out = rows_contract(grad_mid_bf, mixed)
    grad_mixed = jnp.dot(grad_mid_bf, out_full, preferred_element_type=f32).astype(bf16)
    grad_heads = grad_mixed.reshape(tok_rows, head_count, head_size)
    delta_rows = jnp.sum(
        grad_heads.astype(f32) * mixed.reshape(tok_rows, head_count, head_size).astype(f32), axis=-1
    )
    delta = delta_rows.T
    zeros_heads = jnp.zeros((tok_rows, head_count, head_size), f32)
    query_key_piece = lax.all_gather(key_send, "ctx", axis=0, tiled=True)
    query_value_piece = lax.all_gather(value_send, "ctx", axis=0, tiled=True)
    length = query_key_piece.shape[0]
    query_step_len = math.gcd(length, 1024)

    def query_grad_block(block_num, grad_query):
        key_blk = lax.dynamic_slice_in_dim(
            query_key_piece, block_num * query_step_len, query_step_len, 0
        ).reshape(query_step_len, head_count, head_size)
        value_blk = lax.dynamic_slice_in_dim(
            query_value_piece, block_num * query_step_len, query_step_len, 0
        ).reshape(query_step_len, head_count, head_size)
        scores = (
            jnp.einsum("qhd,khd->hqk", query_heads, key_blk, preferred_element_type=f32) * scale
        )
        probs = jnp.exp(scores - log_sum[..., None])
        grad_probs = jnp.einsum("qhd,khd->hqk", grad_heads, value_blk, preferred_element_type=f32)
        grad_scores = (probs * (grad_probs - delta[..., None])).astype(bf16)
        return (
            grad_query
            + jnp.einsum("hqk,khd->qhd", grad_scores, key_blk, preferred_element_type=f32) * scale
        )

    grad_query = lax.fori_loop(0, length // query_step_len, query_grad_block, zeros_heads)
    query_send = query_heads.reshape(tok_rows, width).astype(f32)
    grad_send = grad_mixed.astype(f32)
    query_piece = lax.all_gather(query_send, "ctx", axis=0, tiled=True)
    grad_piece = lax.all_gather(grad_send, "ctx", axis=0, tiled=True)
    log_piece = lax.all_gather(log_sum.T, "ctx", axis=0, tiled=True)
    delta_piece = lax.all_gather(delta_rows, "ctx", axis=0, tiled=True)
    length = query_piece.shape[0]
    key_step_len = math.gcd(length, 1024)

    def key_grad_block(block_num, running):
        grad_keys, grad_values = running
        query_blk = (
            lax.dynamic_slice_in_dim(query_piece, block_num * key_step_len, key_step_len, 0)
            .astype(bf16)
            .reshape(key_step_len, head_count, head_size)
        )
        grad_blk = (
            lax.dynamic_slice_in_dim(grad_piece, block_num * key_step_len, key_step_len, 0)
            .astype(bf16)
            .reshape(key_step_len, head_count, head_size)
        )
        log_blk = lax.dynamic_slice_in_dim(log_piece, block_num * key_step_len, key_step_len, 0).T
        delta_blk = lax.dynamic_slice_in_dim(
            delta_piece, block_num * key_step_len, key_step_len, 0
        ).T
        scores = (
            jnp.einsum("qhd,khd->hqk", query_blk, key_heads, preferred_element_type=f32) * scale
        )
        probs = jnp.exp(scores - log_blk[..., None])
        grad_values = grad_values + jnp.einsum(
            "hqk,qhd->khd", probs.astype(bf16), grad_blk, preferred_element_type=f32
        )
        grad_probs = jnp.einsum("qhd,khd->hqk", grad_blk, value_heads, preferred_element_type=f32)
        grad_scores = (probs * (grad_probs - delta_blk[..., None])).astype(bf16)
        grad_keys = (
            grad_keys
            + jnp.einsum("hqk,qhd->khd", grad_scores, query_blk, preferred_element_type=f32) * scale
        )
        return (grad_keys, grad_values)

    grad_keys, grad_values = lax.fori_loop(
        0, length // key_step_len, key_grad_block, (zeros_heads, zeros_heads)
    )
    grad_query = rotate_back(grad_query, cos_table, sine_table)
    grad_keys = rotate_back(grad_keys, cos_table, sine_table)
    grad_packed = jnp.concatenate(
        [
            grad_query.reshape(tok_rows, width),
            grad_keys.reshape(tok_rows, width),
            grad_values.reshape(tok_rows, width),
        ],
        axis=1,
    ).astype(bf16)
    grad_qkv = rows_contract(grad_packed, act_a)
    grad_act_a = jnp.dot(grad_packed, qkv_full, preferred_element_type=f32)
    grad_gain_a = jnp.sum(grad_act_a * normed_a, axis=0)
    grad_input = grad_middle + norm_back(grad_act_a * gain_attn, normed_a, inv_a)
    owned = (
        lax.psum_scatter(grad_qkv, ("ctx", "fsdp"), scatter_dimension=0, tiled=True),
        lax.psum_scatter(grad_out, ("ctx", "fsdp"), scatter_dimension=0, tiled=True),
        lax.psum_scatter(grad_in, ("ctx", "fsdp"), scatter_dimension=0, tiled=True),
        lax.psum_scatter(grad_down, ("ctx", "fsdp"), scatter_dimension=0, tiled=True),
        lax.psum_scatter(grad_gain_a, ("ctx", "fsdp"), scatter_dimension=0, tiled=True),
        lax.psum_scatter(grad_gain_m, ("ctx", "fsdp"), scatter_dimension=0, tiled=True),
    )
    return (
        output[None],
        grad_input[None],
        owned[0],
        owned[1],
        owned[2],
        owned[3],
        owned[4],
        owned[5],
    )


MESH = pl.DeviceIdType.MESH
VMEM_LIMIT = 60 * 1024 * 1024


def matmul(left, right, left_dim, right_dim):
    return lax.dot_general(
        left, right, (((left_dim,), (right_dim,)), ((), ())), preferred_element_type=jnp.float32
    )


class Place:
    def __init__(self, count):
        self.count, self.line = count, count // 4
        self.me, self.pair = lax.axis_index("ctx"), lax.axis_index("fsdp")
        self.owner = self.me * 2 + self.pair
        self.z, self.x, self.core = self.me // 4, self.me // 2 % 2, self.me % 2

    def slot(self, z, x, core):
        return z * 4 + x * 2 + core

    def far(self, step):
        last = self.line - 1
        low = 2 * self.z < self.line
        own = jnp.where(low, self.z, last - self.z)
        at = jnp.where(
            step < last - own, last - step, jnp.where(step == last, own, step - (last - own))
        )
        return jnp.where(low, at, last - at)

    def near(self, step):
        return self.far(self.line - 1 - step)

    def meet(self, everyone=False):
        barrier = pltpu.get_barrier_semaphore()

        @pl.loop(1, self.count)
        def _(shift):
            pl.semaphore_signal(
                barrier, inc=1, device_id={"ctx": (self.me + shift) % self.count}, device_id_type=MESH
            )

        if everyone:
            @pl.loop(0, self.count)
            def _(to):
                pl.semaphore_signal(
                    barrier, inc=1, device_id={"ctx": to, "fsdp": 1 - self.pair}, device_id_type=MESH
                )

            pl.semaphore_wait(barrier, 2 * self.count - 1)
        else:
            pl.semaphore_signal(barrier, inc=1, device_id={"fsdp": 1 - self.pair}, device_id_type=MESH)
            pl.semaphore_wait(barrier, self.count)

    def over_pair(self, src, dst, send, recv):
        return pltpu.make_async_remote_copy(
            src_ref=src, dst_ref=dst, send_sem=send, recv_sem=recv,
            device_id={"fsdp": 1 - self.pair}, device_id_type=MESH,
        )

    def to_owner(self, src, dst, send, recv, owner):
        return pltpu.make_async_remote_copy(
            src_ref=src, dst_ref=dst, send_sem=send, recv_sem=recv,
            device_id={"ctx": owner // 2, "fsdp": owner % 2}, device_id_type=MESH,
        )

    def copy(self, src, dst, send, recv, to):
        return pltpu.make_async_remote_copy(
            src_ref=src, dst_ref=dst, send_sem=send, recv_sem=recv,
            device_id={"ctx": to}, device_id_type=MESH,
        )


class Gather:
    def __init__(self, place, buf, sems):
        self.p, self.buf = place, buf
        self.up_s, self.up_r, self.dn_s, self.dn_r, self.x_s, self.x_r, self.c_s, self.c_r = sems

    @staticmethod
    def sems(line):
        return [pltpu.SemaphoreType.DMA((line,))] * 6 + [pltpu.SemaphoreType.DMA((2 * line,))] * 2

    def over(self, z, x, core, send, recv, to):
        at = self.buf.at[self.p.slot(z, x, core)]
        return self.p.copy(at, at, send, recv, to)

    def up(self, z):
        p = self.p
        return self.over(z, p.x, p.core, self.up_s.at[z], self.up_r.at[z], (p.me + 4) % p.count)

    def down(self, z):
        p = self.p
        return self.over(z, p.x, p.core, self.dn_s.at[z], self.dn_r.at[z], (p.me + p.count - 4) % p.count)

    def across(self, z):
        p = self.p
        return self.over(z, p.x, p.core, self.x_s.at[z], self.x_r.at[z], p.slot(p.z, 1 - p.x, p.core))

    def beside(self, z, x):
        p = self.p
        at = z * 2 + x
        return self.over(z, x, p.core, self.c_s.at[at], self.c_r.at[at], p.slot(p.z, p.x, 1 - p.core))

    def arrive(self, z):
        p = self.p

        @pl.when(z < p.z)
        def _():
            self.up(z).wait_recv()

        @pl.when(z > p.z)
        def _():
            self.down(z).wait_recv()

        @pl.when((z <= p.z) & (p.z < p.line - 1))
        def _():
            self.up(z).start()

        @pl.when((z >= p.z) & (p.z > 0))
        def _():
            self.down(z).start()

        self.across(z).start()
        self.beside(z, p.x).start()

    def arrive_across(self, z):
        self.across(z).wait_recv()
        self.beside(z, 1 - self.p.x).start()

    def part(self, turn, use=None):
        p = self.p
        step, part = turn // 4, turn % 4
        z = jnp.where(part == 0, p.near(step), p.near(step - 1))

        @pl.when(jnp.where(part == 0, step < p.line, step > 0))
        def _():
            @pl.when(part == 0)
            def _():
                self.arrive(z)

            @pl.when(part == 1)
            def _():
                self.arrive_across(z)

            x = jnp.where(part % 2 == 0, p.x, 1 - p.x)

            @pl.when(part >= 2)
            def _():
                self.beside(z, x).wait_recv()

            if use is not None:
                use(z, x, jnp.where(part < 2, p.core, 1 - p.core))

    def sent(self):
        p = self.p

        @pl.loop(0, p.line)
        def _(z):
            @pl.when((z <= p.z) & (p.z < p.line - 1))
            def _():
                self.up(z).wait_send()

            @pl.when((z >= p.z) & (p.z > 0))
            def _():
                self.down(z).wait_send()

            self.across(z).wait_send()
            self.beside(z, 0).wait_send()
            self.beside(z, 1).wait_send()


class Halve:
    def __init__(self, place, whole, got, sums, sems):
        self.p, self.whole, self.got, self.sums = place, whole, got, sums
        self.c_s, self.c_r = sems

    @staticmethod
    def sems(line):
        return [pltpu.SemaphoreType.DMA((2 * line,))] * 2

    def beside(self, z, x):
        p, at = self.p, z * 2 + x
        return p.copy(
            self.whole.at[p.slot(z, x, 1 - p.core)], self.got.at[at], self.c_s.at[at], self.c_r.at[at],
            p.slot(p.z, p.x, 1 - p.core),
        )

    def add(self, z):
        p = self.p
        for x in range(2):
            at = z * 2 + x
            self.beside(z, x).wait_recv()
            self.sums[at] = (
                self.whole[p.slot(z, x, p.core)].astype(jnp.float32) + self.got[at].astype(jnp.float32)
            ).astype(self.sums.dtype)

    def sent(self):
        @pl.loop(0, 2 * self.p.line)
        def _(at):
            self.beside(at // 2, at % 2).wait_send()


class Quad:
    def __init__(self, place, buf, sems):
        self.p, self.buf = place, buf
        self.s, self.r = sems

    @staticmethod
    def sems():
        return [pltpu.SemaphoreType.DMA((3,))] * 2

    def over(self, x, to, at):
        piece = self.buf.at[x * 2 + self.p.core]
        return self.p.copy(piece, piece, self.s.at[at], self.r.at[at], to)

    def across(self):
        p = self.p
        return self.over(p.x, p.slot(p.z, 1 - p.x, p.core), 0)

    def beside(self):
        p = self.p
        return self.over(p.x, p.slot(p.z, p.x, 1 - p.core), 1)

    def beside_next(self):
        p = self.p
        return self.over(1 - p.x, p.slot(p.z, p.x, 1 - p.core), 2)

    def start(self):
        self.across().start()
        self.beside().start()

    def relay(self):
        self.across().wait_recv()
        self.beside_next().start()

    def sent(self):
        self.across().wait_send()
        self.beside().wait_send()
        self.beside_next().wait_send()


class QuadSum:
    def __init__(self, place, whole, bufs, sems):
        self.p, self.whole = place, whole
        self.got, self.sums, self.far = bufs
        self.s, self.r = sems

    @staticmethod
    def sems():
        return [pltpu.SemaphoreType.DMA((3,))] * 2

    @staticmethod
    def bufs(block):
        return [pltpu.VMEM((2,) + block, jnp.bfloat16)] * 2 + [pltpu.VMEM(block, jnp.bfloat16)]

    def beside(self, x):
        p = self.p
        return p.copy(
            self.whole.at[x * 2 + 1 - p.core], self.got.at[x], self.s.at[x], self.r.at[x],
            p.slot(p.z, p.x, 1 - p.core),
        )

    def across(self):
        p = self.p
        return p.copy(
            self.sums.at[1 - p.x], self.far, self.s.at[2], self.r.at[2], p.slot(p.z, 1 - p.x, p.core)
        )

    def add(self, x):
        f32 = jnp.float32
        self.beside(x).wait_recv()
        self.sums[x] = (
            self.whole[x * 2 + self.p.core].astype(f32) + self.got[x].astype(f32)
        ).astype(self.sums.dtype)

    def finish(self, out):
        f32 = jnp.float32
        self.across().wait_recv()
        out[...] = self.sums[self.p.x].astype(f32) + self.far[...].astype(f32)

    def sent(self):
        self.beside(0).wait_send()
        self.beside(1).wait_send()
        self.across().wait_send()


class Settle:
    def __init__(self, place, sums, bufs, sems, pairwise=False):
        self.p, self.sums, self.pairwise = place, sums, pairwise
        self.got, self.total, self.low, self.high = bufs
        self.x_s, self.x_r, self.up_s, self.up_r, self.dn_s, self.dn_r = sems

    @staticmethod
    def sems(line):
        return [pltpu.SemaphoreType.DMA((line,))] * 6

    @staticmethod
    def bufs(line, block):
        return [pltpu.VMEM((line,) + block, jnp.bfloat16)] * 4

    def kept(self, z):
        p = self.p
        return p.pair * p.line + z if self.pairwise else z * 2 + p.x

    def across(self, z):
        p = self.p
        if self.pairwise:
            return p.over_pair(
                self.sums.at[(1 - p.pair) * p.line + z], self.got.at[z], self.x_s.at[z], self.x_r.at[z]
            )
        return p.copy(
            self.sums.at[z * 2 + 1 - p.x], self.got.at[z], self.x_s.at[z], self.x_r.at[z],
            p.slot(p.z, 1 - p.x, p.core),
        )

    def up(self, z):
        p = self.p
        return p.copy(self.total.at[z], self.low.at[z], self.up_s.at[z], self.up_r.at[z], (p.me + 4) % p.count)

    def down(self, z):
        p = self.p
        return p.copy(
            self.total.at[z], self.high.at[z], self.dn_s.at[z], self.dn_r.at[z], (p.me + p.count - 4) % p.count
        )

    def pass_on(self, z):
        p, f32 = self.p, jnp.float32
        self.across(z).wait_recv()
        self.total[z] = (
            self.sums[self.kept(z)].astype(f32) + self.got[z].astype(f32)
        ).astype(self.total.dtype)

        @pl.when(z > p.z)
        def _():
            @pl.when(p.z > 0)
            def _():
                self.up(z).wait_recv()
                self.total[z] = (self.total[z].astype(f32) + self.low[z].astype(f32)).astype(self.total.dtype)

            self.up(z).start()

        @pl.when(z < p.z)
        def _():
            @pl.when(p.z < p.line - 1)
            def _():
                self.down(z).wait_recv()
                self.total[z] = (self.total[z].astype(f32) + self.high[z].astype(f32)).astype(self.total.dtype)

            self.down(z).start()

    def finish(self, out):
        p, f32 = self.p, jnp.float32
        @pl.when(p.z > 0)
        def _():
            self.up(p.z).wait_recv()

        @pl.when(p.z < p.line - 1)
        def _():
            self.down(p.z).wait_recv()

        total = self.total[p.z].astype(f32)
        total += jnp.where(p.z > 0, self.low[p.z].astype(f32), 0.0)
        total += jnp.where(p.z < p.line - 1, self.high[p.z].astype(f32), 0.0)
        out[...] = total.astype(out.dtype)

    def sent(self):
        p = self.p

        @pl.loop(0, p.line)
        def _(z):
            self.across(z).wait_send()

            @pl.when(z > p.z)
            def _():
                self.up(z).wait_send()

            @pl.when(z < p.z)
            def _():
                self.down(z).wait_send()


class Exchange:
    def __init__(self, place, src, dst, sems):
        self.p, self.src, self.dst = place, src, dst
        self.s, self.r = sems

    @staticmethod
    def sems(count):
        return [pltpu.SemaphoreType.DMA((count,))] * 2

    def to(self, j):
        return self.p.copy(self.src.at[j], self.dst.at[self.p.me], self.s.at[j], self.r.at[self.p.me], j)

    def send(self, j):
        @pl.when(j != self.p.me)
        def _():
            self.to(j).start()

        @pl.when(j == self.p.me)
        def _():
            self.dst[j] = self.src[j]

    def arrived(self):
        p = self.p

        @pl.loop(1, p.count)
        def _(shift):
            j = (p.me + shift) % p.count
            p.copy(self.src.at[j], self.dst.at[j], self.s.at[j], self.r.at[j], j).wait_recv()

    def sent(self):
        p = self.p

        @pl.loop(1, p.count)
        def _(shift):
            self.to((p.me + shift) % p.count).wait_send()


class Spread:
    def __init__(self, place, src, dst, sems):
        self.p, self.src, self.dst = place, src, dst
        self.s, self.r = sems

    @staticmethod
    def sems(count):
        return [pltpu.SemaphoreType.DMA((2 * count,))] * 2

    def to(self, j):
        p = self.p
        return p.to_owner(self.src.at[j], self.dst.at[p.owner], self.s.at[j], self.r.at[p.owner], j)

    def send(self):
        p = self.p
        self.dst[p.owner] = self.src[p.owner]

        @pl.loop(1, 2 * p.count)
        def _(shift):
            self.to((p.owner + shift) % (2 * p.count)).start()

    def arrived(self):
        p = self.p

        @pl.loop(1, 2 * p.count)
        def _(shift):
            j = (p.owner + shift) % (2 * p.count)
            p.to_owner(self.src.at[j], self.dst.at[j], self.s.at[j], self.r.at[j], j).wait_recv()

    def sent(self):
        p = self.p

        @pl.loop(1, 2 * p.count)
        def _(shift):
            self.to((p.owner + shift) % (2 * p.count)).wait_send()


class Deliver:
    def __init__(self, place, src, dst, sems):
        self.p, self.src, self.dst = place, src, dst
        self.s, self.r = sems

    def away(self, piece, owner, slot):
        return self.p.to_owner(self.src.at[piece], self.dst.at[slot], self.s.at[piece], self.r.at[slot], owner)

    def send(self, piece, owner, slot):
        @pl.when(owner != self.p.owner)
        def _():
            self.away(piece, owner, slot).start()

        @pl.when(owner == self.p.owner)
        def _():
            self.dst[slot] = self.src[piece]

    def sent(self, piece, owner, slot):
        @pl.when(owner != self.p.owner)
        def _():
            self.away(piece, owner, slot).wait_send()

    def arrived(self, slot, source):
        p = self.p

        @pl.when(source != p.owner)
        def _():
            p.to_owner(self.src.at[0], self.dst.at[slot], self.s.at[0], self.r.at[slot], source).wait_recv()


def rotate_rows(value, cos, sine):
    half = value.shape[0] // 2
    first, second = value[:half], value[half:]
    return jnp.concatenate([first * cos - second * sine, second * cos + first * sine], axis=0)


def rotate_rows_back(grad, cos, sine):
    half = grad.shape[0] // 2
    first, second = grad[:half], grad[half:]
    return jnp.concatenate([first * cos + second * sine, second * cos - first * sine], axis=0)


def attend_kernel(
    count, tokens, cot, gain_attn, gain_mlp, qkv_weight, in_weight, down_mine, out_mine,
    normed_a, inv_a, normed_m, inv_m, middle, act_m, cos, sine, act_out, cot_all, query_t, keys_t, keys, values, mixed_own, log_sum, mixed, weight, in_other, down_other, out_pair,
    act_all, values_t, load_sem, part_sem, part_got, piece_sem, piece_got, *sems
):
    f32, bf16 = jnp.float32, jnp.bfloat16
    p = Place(count)
    rows, width = tokens.shape
    head = keys_t.shape[0]
    n = 8
    first = Gather(p, act_all, sems[:n])
    second = Quad(p, cot_all, sems[n : n + 2])
    trade = Exchange(p, mixed_own, mixed, sems[n + 2 :])
    half = out_mine.shape[0] // 2
    part_half = pl.ds(pl.multiple_of(p.core * half, half), half)
    loads = [(cot, cot_all.at[p.x * 2 + p.core]), (out_mine, out_pair.at[p.pair])]
    loads = [pltpu.make_async_copy(src, dst, load_sem.at[i]) for i, (src, dst) in enumerate(loads)]
    for load in loads:
        load.start()

    def part_rows(part):
        start = part * width + p.me * head
        holder = start // qkv_weight.shape[0]
        at = pl.ds(pl.multiple_of(start - holder * qkv_weight.shape[0], head), head)
        return holder == p.pair, qkv_weight.at[at]

    def part_copies(part):
        here, src = part_rows(part)
        return (
            here,
            pltpu.make_async_copy(src, weight.at[part], load_sem.at[3 + part]),
            p.over_pair(src, weight.at[part], part_sem.at[part], part_got.at[part]),
        )

    units, columns = in_other.shape[0], in_other.shape[1] // 2
    in_rows = pl.ds(pl.multiple_of((p.x * 2 + p.core) * units, 16), units)
    in_cols = pl.ds(pl.multiple_of(p.z % 2 * columns, columns), columns)
    in_here = in_other.at[:, in_cols]
    swaps = [
        p.over_pair(out_mine.at[part_half], out_pair.at[p.pair, part_half], piece_sem.at[0], piece_got.at[0]),
        p.over_pair(in_weight.at[in_rows, in_cols], in_here, piece_sem.at[1], piece_got.at[1]),
        p.over_pair(down_mine, down_other, piece_sem.at[2], piece_got.at[2]),
    ]
    next_z = p.me + 4 - p.z % 2 * 8
    in_share = p.copy(in_here, in_here, piece_sem.at[4], piece_got.at[4], next_z)
    out_rest = out_pair.at[1 - p.pair, part_half]
    share = p.copy(out_rest, out_rest, piece_sem.at[3], piece_got.at[3], p.slot(p.z, p.x, 1 - p.core))
    for part in range(3):
        here, own, away = part_copies(part)

        @pl.when(here)
        def _():
            own.start()

    p.meet()
    for part in range(3):
        here, own, away = part_copies(part)

        @pl.when(here)
        def _():
            away.start()

    for at in (1, 0, 2):
        swaps[at].start()
    resid = tokens[...].astype(f32)
    normed, inv = normalize(resid)
    normed_a[...], inv_a[...] = normed, inv
    act_all[p.me] = (normed * gain_attn[...]).astype(bf16)
    for load in loads:
        load.wait()

    first.part(0)
    position = lax.broadcasted_iota(jnp.int32, cos.shape, 1).astype(f32)
    entry = lax.broadcasted_iota(jnp.int32, (cos.shape[0], 1), 0).astype(f32)
    angles = position * jnp.exp(entry * (-2.0 * math.log(ROPE_BASE) / head))
    cos[...], sine[...] = jnp.cos(angles), jnp.sin(angles)
    for part in range(3):
        here, own, away = part_copies(part)

        @pl.when(here)
        def _():
            own.wait()

        @pl.when(jnp.logical_not(here))
        def _():
            away.wait_recv()

    head_weight = weight[...].reshape(3 * head, width)

    def project(z, x, core):
        at = p.slot(z, x, core)
        lanes = pl.ds(pl.multiple_of(at * rows, rows), rows)
        packed = matmul(head_weight, act_all[at], 1, 1)
        c, s = cos[:, lanes], sine[:, lanes]
        query, key = packed[:head], packed[head : 2 * head]
        query_t[:, lanes] = rotate_rows(query, c, s).astype(bf16)
        key = rotate_rows(key, c, s)
        keys_t[:, lanes] = key.astype(bf16)
        values_t[:, lanes] = packed[2 * head :].astype(bf16)
        keys[lanes, :] = key.T.astype(bf16)
        values[lanes, :] = packed[2 * head :].T.astype(bf16)

    project(p.z, p.x, p.core)

    @pl.loop(4, 4 * p.line + 4)
    def _(at):
        first.part(at, project)

    keep_act = pltpu.make_async_copy(act_all, act_out, load_sem.at[2])
    keep_act.start()
    second.start()
    swaps[1].wait_recv()
    in_share.start()
    wide = 2 * rows
    blocks = count // 2
    scale = head ** (-0.5)

    def attend(i):
        block = (p.me // 2 + i) % blocks
        lanes = pl.ds(pl.multiple_of(block * wide, wide), wide)
        scores = matmul(keys[...], query_t[:, lanes], 1, 0) * scale
        top = jnp.max(scores, axis=0, keepdims=True)
        weights = jnp.exp(scores - top)
        total = jnp.sum(weights, axis=0, keepdims=True)
        log_sum[:, lanes] = top + jnp.log(total)
        out = (matmul(values_t[...], weights.astype(bf16), 1, 0) / total).astype(bf16)
        mixed_own[2 * block] = out[:, :rows]
        mixed_own[2 * block + 1] = out[:, rows:]
        trade.send(2 * block)
        trade.send(2 * block + 1)

    @pl.loop(0, blocks // 2)
    def _(i):
        attend(i)

    second.relay()
    swaps[0].wait_recv()
    share.start()

    @pl.loop(blocks // 2, blocks)
    def _(i):
        attend(i)

    trade.arrived()
    share.wait_recv()
    flat = mixed[...].reshape(width, rows)
    total = tokens[...].astype(f32) + matmul(flat, out_pair[...].reshape(width, width), 0, 1)
    middle[...] = total
    normed, inv = normalize(total)
    normed_m[...], inv_m[...] = normed, inv
    act_m[...] = (normed * gain_mlp[...]).astype(bf16)
    second.beside().wait_recv()
    second.beside_next().wait_recv()
    swaps[2].wait_recv()
    first.sent()
    second.sent()
    trade.sent()
    for part in range(3):
        here, own, away = part_copies(part)

        @pl.when(here)
        def _():
            away.wait_send()

    for swap in swaps:
        swap.wait_send()
    share.wait_send()
    in_share.wait()
    keep_act.wait()


def feed_kernel(
    count, act, cot_all, in_weight, in_other, down_mine, down_other, gain, out_in, normed, inv, middle,
    output, grad_middle, grad_mid, grad_mixed, in_grad, down_grad,
    out_pair, grad_act, out_total, weight, down, act_all, gated, inner_grad, grad_part, out_part, load_sem, *rest
):
    f32, bf16 = jnp.float32, jnp.bfloat16
    p = Place(count)
    rows, group = act.shape[0], down.shape[1]
    gather = Quad(p, act_all, rest[:2])
    grad_sum = QuadSum(p, grad_part, rest[2:5], rest[8:10])
    out_sum = QuadSum(p, out_part, rest[5:8], rest[10:12])
    units, half = in_other.shape[0], down_other.shape[0]
    in_rows = pl.ds(pl.multiple_of((p.x * 2 + p.core) * units, 16), units)
    own_at = pl.ds(pl.multiple_of(p.pair * group, group), units)
    other_at = pl.ds(pl.multiple_of((1 - p.pair) * group, group), units)
    load = pltpu.make_async_copy(act, act_all.at[p.x * 2 + p.core], load_sem.at[0])
    weights = [
        pltpu.make_async_copy(in_weight.at[in_rows], weight.at[own_at], load_sem.at[1]),
        pltpu.make_async_copy(in_other, weight.at[other_at], load_sem.at[2]),
    ]
    load.start()
    for copy in weights:
        copy.start()
    load_out = pltpu.make_async_copy(out_in, out_pair, load_sem.at[3])
    load_out.start()
    p.meet()
    load.wait()
    gather.start()
    down[...] = jnp.zeros_like(down)
    down[pl.ds(pl.multiple_of(p.pair * half, half), half), :units] = down_mine[...]
    down[pl.ds(pl.multiple_of((1 - p.pair) * half, half), half), :units] = down_other[...]
    for at in range(2):
        weight[at * group + units : (at + 1) * group, :] = jnp.zeros((group - units, weight.shape[1]), bf16)
    for copy in weights:
        copy.wait()
    gather.beside().wait_recv()

    @pl.loop(0, 2)
    def _(step):
        x = jnp.where(step == 0, p.x, 1 - p.x)

        @pl.when(step == 1)
        def _():
            gather.relay()
            gather.beside_next().wait_recv()

        acts = jnp.concatenate([act_all[2 * x], act_all[2 * x + 1]], axis=0)
        cots = jnp.concatenate([cot_all[2 * x], cot_all[2 * x + 1]], axis=0)
        inner = matmul(acts, weight[...], 1, 1)
        grad_gated = matmul(cots, down[...], 1, 0)
        value, gate = inner[:, :group], inner[:, group:]
        gelu_val, gelu_slope = gelu_pair(value)
        token = pl.ds(pl.multiple_of(x * 2 * rows, 2 * rows), 2 * rows)
        out = (gelu_val * gate).astype(bf16)
        gated[token, :] = out
        grads = jnp.concatenate(
            [grad_gated * gate * gelu_slope, grad_gated * gelu_val], axis=1
        ).astype(bf16)
        inner_grad[token, :] = grads
        part = matmul(grads, weight[...], 1, 0).astype(bf16)
        grad_part[2 * x], grad_part[2 * x + 1] = part[:rows], part[rows:]
        grad_sum.beside(x).start()
        part = matmul(out, down[...], 1, 1).astype(bf16)
        out_part[2 * x], out_part[2 * x + 1] = part[:rows], part[rows:]
        out_sum.beside(x).start()

    grad_sum.add(1 - p.x)
    grad_sum.across().start()
    grad_sum.add(p.x)
    out_sum.add(1 - p.x)
    out_sum.across().start()
    out_sum.add(p.x)
    acts = act_all[...].reshape(4 * rows, act.shape[1])
    cots = cot_all[...].reshape(4 * rows, act.shape[1])
    quarter = units // 4
    gain_row = jnp.zeros((1, act.shape[1]), f32)
    for at in range(2):
        piece = matmul(inner_grad[:, at * group : (at + 1) * group], acts, 0, 0)
        gain_row += jnp.sum(piece * weight[at * group : (at + 1) * group, :].astype(f32), axis=0, keepdims=True)
        for k in range(4):
            in_grad[k % 2 * p.line + at * 2 + k // 2] = piece[k * quarter : (k + 1) * quarter].astype(bf16)
    piece = matmul(cots, gated[...], 0, 0)
    lane = lax.broadcasted_iota(jnp.int32, piece.shape, 1)
    gain_row = gain_row / gain[...]
    column = jnp.broadcast_to(gain_row, (8, gain_row.shape[1])).T[:, :1]
    piece = jnp.where(lane == units, column, piece).astype(bf16)
    unit = act.shape[1] // (2 * count)
    for z in range(p.line):
        for r in range(4):
            for y in range(2):
                start = ((z * 4 + r) * 2 + y) * unit
                down_grad[y * p.line + z, r] = piece[start : start + unit]
    grad_sum.finish(grad_act)
    cot = cot_all[p.x * 2 + p.core].astype(f32)
    grad = cot + norm_back(grad_act[...] * gain[...], normed[...], inv[...])
    grad_middle[...] = grad
    grad_mid[...] = grad.astype(bf16)
    width = act.shape[1]
    load_out.wait()
    back = matmul(grad_mid[...], out_pair[...].reshape(width, width), 1, 0)
    grad_mixed[...] = back.T.astype(bf16).reshape(grad_mixed.shape)
    out_sum.finish(out_total)
    output[...] = middle[...] + out_total[...]
    gather.sent()
    grad_sum.sent()
    out_sum.sent()


def attend_back_kernel(
    count, grad_mixed, grad_mid, mixed, query_t, keys_t, keys, values, mixed_own, log_sum,
    act_in, weight, cos, sine, in_grad, down_grad, gain, grad_middle, normed, inv,
    grad_input, qkv_out, out_out, in_out, down_out, gain_m_out, gain_a_out,
    act_all, act_sem, grad_act, grad_own, grad_keys, grad_values, grad_packed, grad_part, grad_got, grad_sums, grad_weight,
    pair_part, pair_core, pair_sums, pair_got, proj_sums, in_sum, in_got, down_sum, down_got,
    qkv_part, qkv_got, gain_part, gain_got,
    pair_s, pair_r, in_s, in_r, down_s, down_r, qkv_s, qkv_r, *rest
):
    f32, bf16 = jnp.float32, jnp.bfloat16
    p = Place(count)
    rows, head = grad_mixed.shape[2], keys_t.shape[0]
    width, unit = count * head, head // 2
    bufs, proj_bufs, in_bufs, down_bufs, sems = rest[:4], rest[4:8], rest[8:12], rest[12:16], rest[16:]
    trade = Exchange(p, grad_mixed, grad_own, sems[:2])
    halve = Halve(p, grad_part, grad_got, grad_sums, sems[2:4])
    settle = Settle(p, grad_sums, bufs, sems[4:10])
    halve_proj = Halve(p, pair_part, pair_core, pair_sums, sems[10:12])
    settle_proj = Settle(p, proj_sums, proj_bufs, sems[12:18])
    settle_in = Settle(p, in_grad, in_bufs, sems[18:24], True)
    settle_down = Settle(p, down_grad, down_bufs, sems[24:30], True)
    spread_gain = Spread(p, gain_part, gain_got, sems[30:32])
    give_in = Deliver(p, in_sum, in_got, (in_s, in_r))
    give_down = Deliver(p, down_sum, down_got, (down_s, down_r))
    give_qkv = Deliver(p, qkv_part, qkv_got, (qkv_s, qkv_r))

    def swap(at):
        return p.over_pair(pair_sums.at[at, 1 - p.pair], pair_got.at[at], pair_s.at[at], pair_r.at[at])

    load_act = pltpu.make_async_copy(act_in, act_all, act_sem)
    load_act.start()
    p.meet(True)

    @pl.loop(0, count)
    def _(shift):
        trade.send((p.me + shift) % count)

    @pl.loop(0, p.line)
    def _(step):
        settle_in.across(p.far(step)).start()
        settle_down.across(p.far(step)).start()

    flat = mixed[...].reshape(width, rows)

    @pl.loop(0, count // 2)
    def _(i):
        lanes = pl.ds(pl.multiple_of(i * 4 * unit, 4 * unit), 4 * unit)
        piece = matmul(grad_mid[:, lanes], flat, 0, 1).astype(bf16)
        for at in range(4):
            pair_part[2 * i + at // 2, at % 2] = piece[at * unit : (at + 1) * unit]

    @pl.loop(0, 2 * p.line)
    def _(at):
        halve_proj.beside(at // 2, at % 2).start()

    @pl.loop(0, p.line)
    def _(step):
        z = p.far(step)
        halve_proj.add(z)
        swap(2 * z).start()
        swap(2 * z + 1).start()

    grad_keys[...] = jnp.zeros_like(grad_keys)
    grad_values[...] = jnp.zeros_like(grad_values)
    trade.arrived()
    wide = 2 * rows
    scale = head ** (-0.5)

    def back(i):
        lanes = pl.ds(pl.multiple_of(i * wide, wide), wide)
        query = query_t[:, lanes]
        grad = jnp.concatenate([grad_own[2 * i], grad_own[2 * i + 1]], axis=1)
        own = jnp.concatenate([mixed_own[2 * i], mixed_own[2 * i + 1]], axis=1)
        delta = jnp.sum(grad.astype(f32) * own.astype(f32), axis=0, keepdims=True)
        scores = matmul(keys[...], query, 1, 0) * scale
        probs = jnp.exp(scores - log_sum[:, lanes])
        grad_values[...] += matmul(probs.astype(bf16), grad, 1, 1)
        grad_probs = matmul(values[...], grad, 1, 0)
        grad_scores = (probs * (grad_probs - delta)).astype(bf16)
        grad_keys[...] += matmul(grad_scores, query, 1, 1)
        grad_query = matmul(keys_t[...], grad_scores, 1, 0) * scale
        back_query = rotate_rows_back(grad_query, cos[:, lanes], sine[:, lanes])
        grad_packed[:head, lanes] = back_query.astype(bf16)

    @pl.loop(0, count // 2)
    def _(i):
        back(i)

        @pl.when(i == count // 4)
        def _():
            settle_in.pass_on(p.far(0))
            settle_down.pass_on(p.far(0))

    grad_key = grad_keys[...].T * scale
    grad_packed[head : 2 * head, :] = rotate_rows_back(grad_key, cos[...], sine[...]).astype(bf16)
    grad_packed[2 * head :, :] = grad_values[...].T.astype(bf16)

    @pl.loop(0, p.line)
    def _(step):
        z = p.far(step)
        for at in range(4):
            lanes = pl.ds(pl.multiple_of((z * 4 + at) * rows, rows), rows)
            grad_part[z * 4 + at] = matmul(grad_packed[:, lanes], weight[...], 0, 0).astype(bf16)
        halve.beside(z, 0).start()
        halve.beside(z, 1).start()

    @pl.loop(0, p.line)
    def _(step):
        z = p.far(step)
        halve.add(z)
        settle.across(z).start()

    def grad_chunk(step):
        lanes = pl.ds(pl.multiple_of(step * 4 * rows, 4 * rows), 4 * rows)
        acts = jnp.concatenate([act_all[4 * step + i] for i in range(4)], axis=0)
        return matmul(grad_packed[:, lanes], acts, 1, 0)

    load_act.wait()
    grad_weight[...] = grad_chunk(0)

    @pl.loop(1, p.line)
    def _(step):
        grad_weight[...] += grad_chunk(step)

    for at in range(6):
        qkv_part[at] = grad_weight[at * unit : (at + 1) * unit, :].astype(bf16)
    gain_row = jnp.sum(grad_weight[...] * weight[...].astype(f32), axis=0, keepdims=True) / gain[...]
    for at in range(2 * count):
        chunk = at * unit // 128 * 128
        gain_part[at] = gain_row[:, chunk : chunk + 128]

    def unit_of(at):
        return (at // 2) * 2 * count + 2 * p.me + at % 2

    for at in range(6):
        give_qkv.send(at, unit_of(at) // 3, unit_of(at) % 3 * 2 + p.pair)
    spread_gain.send()

    @pl.loop(0, p.line)
    def _(step):
        z = p.far(step)
        settle.pass_on(z)

        @pl.when(step > 0)
        def _():
            settle_in.pass_on(z)
            settle_down.pass_on(z)

    @pl.loop(0, p.line)
    def _(step):
        z = p.far(step)
        for x in range(2):
            at = 2 * z + x
            swap(at).wait_recv()
            proj_sums[at] = (pair_sums[at, p.pair].astype(f32) + pair_got[at].astype(f32)).astype(bf16)
        settle_proj.across(z).start()

    @pl.loop(0, p.line)
    def _(step):
        settle_proj.pass_on(p.far(step))

    units = in_out.shape[0]
    r = p.x * 2 + p.core
    piece_owner = p.z // 2 * count + r * 4 + p.z % 2 * 2 + p.pair
    settle_in.finish(in_sum.at[0])
    give_in.send(0, piece_owner, 0)
    settle_down.finish(down_sum)
    for at in range(4):
        give_down.send(at, (p.z * 4 + at) * 2 + p.pair, r)
    for slot in range(3):
        source = (3 * p.owner + slot) % (2 * count) // 2 * 2
        for side in range(2):
            give_qkv.arrived(2 * slot + side, source + side)
        qkv_out[slot * unit : (slot + 1) * unit, :] = qkv_got[2 * slot].astype(f32) + qkv_got[2 * slot + 1].astype(f32)
    spread_gain.arrived()
    gain_a = gain_got[0]
    for at in range(1, 2 * count):
        gain_a += gain_got[at]
    chunks = 128 // unit
    gain_a_out[...] = sum(
        jnp.where(p.owner % chunks == at, gain_a[:, at * unit : (at + 1) * unit], 0.0) for at in range(chunks)
    )
    settle_proj.finish(out_out)
    settle.finish(grad_act)
    grad_input[...] = grad_middle[...] + norm_back(grad_act[...] * gain[...], normed[...], inv[...])
    half, r_of, k_of = p.owner // count, p.owner % count // 4, p.owner % 4
    source_in = ((half * 2 + k_of // 2) * 4 + r_of) * 2 + k_of % 2
    give_in.arrived(0, source_in)
    in_out[...] = in_got[0].astype(f32)
    gain_m = jnp.zeros((unit, 1), f32)
    group = 4 * units
    for at in range(4):
        give_down.arrived(at, (p.z * 4 + at) * 2 + p.pair)
        block = down_got[at].astype(f32)
        down_out[:, at * group : (at + 1) * group] = block[:, :group]
        gain_m += block[:, group : group + 1]
    gain_m_out[...] = jnp.broadcast_to(gain_m, (unit, 128)).T[:1]
    trade.sent()
    halve.sent()
    settle.sent()
    halve_proj.sent()
    settle_proj.sent()
    settle_in.sent()
    settle_down.sent()
    spread_gain.sent()

    @pl.loop(0, 2 * p.line)
    def _(at):
        swap(at).wait_send()

    give_in.sent(0, piece_owner, 0)
    for at in range(4):
        give_down.sent(at, (p.z * 4 + at) * 2 + p.pair, r)
    for at in range(6):
        give_qkv.sent(at, unit_of(at) // 3, unit_of(at) % 3 * 2 + p.pair)


def run_kernel(body, outs, scratch, collective, flops, args, outside=(), outs_outside=()):
    vmem, anywhere = pl.BlockSpec(memory_space=pltpu.VMEM), pl.BlockSpec(memory_space=pl.ANY)
    return pl.pallas_call(
        body,
        out_shape=outs,
        in_specs=[anywhere if i in outside else vmem for i in range(len(args))],
        out_specs=[anywhere if i in outs_outside else vmem for i in range(len(outs))],
        scratch_shapes=scratch,
        compiler_params=pltpu.CompilerParams(
            collective_id=collective, has_side_effects=True, vmem_limit_bytes=VMEM_LIMIT
        ),
        cost_estimate=pl.CostEstimate(flops=flops, bytes_accessed=20_000_000, transcendentals=0),
        name=body.func.__name__,
    )(*args)


def shaped(shape, kind):
    return jax.ShapeDtypeStruct(shape, kind)


def attend(count, head, tokens, cot, gain_attn, gain_mlp, qkv_weight, in_weight, down_mine, out_mine):
    bf16, f32 = jnp.bfloat16, jnp.float32
    rows, width = tokens.shape
    length, line = rows * count, count // 4
    blocks = shaped((count, rows, width), bf16)
    tall, flat = shaped((head, length), bf16), shaped((length, head), bf16)
    heads = shaped((count, head, rows), bf16)
    block, column, table = shaped((rows, width), f32), shaped((rows, 1), f32), shaped((head // 2, length), f32)
    pairs = [shaped((in_weight.shape[0] // 4, width), bf16), shaped(down_mine.shape, bf16), shaped((2,) + out_mine.shape, bf16)]
    three, six = pltpu.SemaphoreType.DMA((3,)), pltpu.SemaphoreType.DMA((6,))
    return run_kernel(
        functools.partial(attend_kernel, count),
        [block, column, block, column, block, shaped((rows, width), bf16), table, table,
         blocks, shaped((4, rows, width), bf16), tall, tall, flat, flat, heads, shaped((1, length), f32), heads,
         shaped((3, head, width), bf16)] + pairs,
        [pltpu.VMEM(blocks.shape, bf16), pltpu.VMEM((head, length), bf16), pltpu.SemaphoreType.DMA((6,))] + [three, three, six, six]
        + Gather.sems(line) + Quad.sems() + Exchange.sems(count),
        0, 10_000_000_000, [tokens, cot, gain_attn, gain_mlp, qkv_weight, in_weight, down_mine, out_mine], (4, 5, 6, 7),
        (8, 18, 19),
    )


def feed(count, group, act, cot_all, in_weight, in_other, down_mine, down_other, gain, out_pair, normed, inv, middle):
    bf16, f32 = jnp.bfloat16, jnp.float32
    rows, width = act.shape
    block = (rows, width)
    units, line, unit = in_other.shape[0], count // 4, width // (2 * count)
    whole = pltpu.VMEM((4,) + block, bf16)
    return run_kernel(
        functools.partial(feed_kernel, count),
        [shaped(block, f32), shaped(block, f32), shaped(block, bf16), shaped((count, width // count, rows), bf16),
         shaped((2 * line, units // 4, width), bf16), shaped((2 * line, 4, unit, group), bf16)],
        [pltpu.VMEM(out_pair.shape, bf16), pltpu.VMEM(block, f32), pltpu.VMEM(block, f32), pltpu.VMEM((2 * group, width), bf16), pltpu.VMEM((width, group), bf16),
         whole, pltpu.VMEM((4 * rows, group), bf16), pltpu.VMEM((4 * rows, 2 * group), bf16), whole, whole,
         pltpu.SemaphoreType.DMA((4,))]
        + Quad.sems() + QuadSum.bufs(block) * 2 + QuadSum.sems() * 2,
        1, 20_000_000_000, [act, cot_all, in_weight, in_other, down_mine, down_other, gain, out_pair, normed, inv, middle], (2, 3, 7),
    )


def attend_back(count, grad_mixed, grad_mid, mixed, kept, act_all, weight, cos, sine, in_grad, down_grad, gain, grad_middle, normed, inv):
    bf16, f32 = jnp.bfloat16, jnp.float32
    rows, width = act_all.shape[1:]
    head, length, line = weight.shape[0] // 3, rows * count, count // 4
    block, unit, units = (rows, width), head // 2, in_grad.shape[1]
    down_block = down_grad.shape[1:]
    piece = (unit, width)

    def held(*shape):
        return pltpu.VMEM(shape, bf16)

    whole, half = held(count, *block), held(2 * line, *block)
    flat = pltpu.VMEM((length, head), f32)
    one, four, six, many = [pltpu.SemaphoreType.DMA((n,)) for n in (1, 4, 6, 2 * line)]
    return run_kernel(
        functools.partial(attend_back_kernel, count),
        [shaped(block, f32), shaped((3 * unit, width), f32), shaped(piece, f32),
         shaped((units, width), f32), shaped((unit, units * count), f32), shaped((1, unit), f32), shaped((1, unit), f32)],
        [whole, pltpu.SemaphoreType.DMA, pltpu.VMEM(block, f32), held(count, head, rows), flat, flat, held(3 * head, length), whole, half, half,
         pltpu.VMEM((3 * head, width), f32),
         held(count, 2, *piece), held(2 * line, 2, *piece), held(2 * line, 2, *piece), held(2 * line, *piece),
         held(2 * line, *piece), held(1, units, width), held(1, units, width), held(*down_block), held(*down_block),
         held(6, *piece), held(6, *piece), pltpu.VMEM((2 * count, 1, 128), f32), pltpu.VMEM((2 * count, 1, 128), f32),
         many, many, one, one, four, four, six, six]
        + Settle.bufs(line, block) + Settle.bufs(line, piece)
        + Settle.bufs(line, (units, width)) + Settle.bufs(line, down_block)
        + Exchange.sems(count) + (Halve.sems(line) + Settle.sems(line)) * 2
        + Settle.sems(line) * 2 + Spread.sems(count),
        2, 20_000_000_000,
        [grad_mixed, grad_mid, mixed, *kept, act_all, weight, cos, sine, in_grad, down_grad, gain,
         grad_middle, normed, inv], (3 + len(kept),),
    )


def publish_kernel(*refs):
    half = len(refs) // 2
    for src, dst in zip(refs[:half], refs[half:]):
        dst[...] = src[...]


def publish(arrays):
    vmem = pl.BlockSpec(memory_space=pltpu.VMEM)
    return pl.pallas_call(
        publish_kernel,
        out_shape=[shaped(array.shape, array.dtype) for array in arrays],
        in_specs=[vmem] * len(arrays),
        out_specs=[vmem] * len(arrays),
        compiler_params=pltpu.CompilerParams(vmem_limit_bytes=VMEM_LIMIT),
    )(*arrays)


def tensor_layer(
    tokens, cotangent, gain_attn, gain_mlp, qkv_weight, out_weight, in_weight, down_weight
):
    count = lax.axis_size("ctx")
    index = lax.axis_index("ctx")
    width = tokens.shape[2]
    head_size = width // count
    group = in_weight.shape[0] // 4
    padded = (group // 128 + 1) * 128

    down_mine = lax.dynamic_slice_in_dim(down_weight, lax.rem(index, 4) * group, group, 1)
    (
        normed_a, inv_a, normed_m, inv_m, middle, act_m, cos, sine, act_all, cot_all, *kept,
        mixed, qkv_head, in_other, down_other, out_pair,
    ) = attend(
        count, head_size, tokens[0], cotangent[0], gain_attn[None], gain_mlp[None],
        qkv_weight, in_weight, down_mine, out_weight,
    )
    output, grad_middle, grad_mid, grad_mixed, in_grad, down_grad = feed(
        count, padded, act_m, cot_all, in_weight, in_other, down_mine, down_other, gain_mlp[None],
        out_pair, normed_m, inv_m, middle,
    )
    grad_input, grad_qkv, grad_out, grad_in, grad_down, grad_gain_m, grad_gain_a = attend_back(
        count, grad_mixed, grad_mid, mixed, kept, act_all, qkv_head.reshape(3 * head_size, width), cos, sine,
        in_grad, down_grad, gain_attn[None], grad_middle, normed_a, inv_a,
    )
    output, grad_input, grad_qkv, grad_out, grad_in, grad_down, grad_gain_a, grad_gain_m = publish(
        [output, grad_input, grad_qkv, grad_out, grad_in, grad_down, grad_gain_a, grad_gain_m]
    )
    return (output[None], grad_input[None], grad_qkv, grad_out, grad_in, grad_down, grad_gain_a[0], grad_gain_m[0])


def solution(mesh):

    def layer(*arrays):
        one_head_each = arrays[0].shape[2] == HEAD_DIM * mesh.shape["ctx"]
        if one_head_each and mesh.shape["fsdp"] == 2 and mesh.shape["ctx"] % 4 == 0:
            return tensor_layer(*arrays)
        return gathered_layer(*arrays)

    return jax.shard_map(
        layer,
        mesh=mesh,
        in_specs=(
            P("fsdp", "ctx", None),
            P("fsdp", "ctx", None),
            P(),
            P(),
            P("fsdp", None),
            P("fsdp", None),
            P("fsdp", None),
            P("fsdp", None),
        ),
        out_specs=(
            P("fsdp", "ctx", None),
            P("fsdp", "ctx", None),
            P(("ctx", "fsdp"), None),
            P(("ctx", "fsdp"), None),
            P(("ctx", "fsdp"), None),
            P(("ctx", "fsdp"), None),
            P(("ctx", "fsdp")),
            P(("ctx", "fsdp")),
        ),
        check_vma=False,
    )
```
